32 devices in a mesh: grp: 8 (over z, y), rep: 4 (over x, core).
Axes of the slice: x: 2, y: 2, z: 4, core: 2. Of those that a mesh axis runs over, the one named last changes fastest.
Arguments:
- queries: bfloat16 [16, 4, 32, 128], P('grp', 'rep'), may hold values from -3.2 to 3.2
- passages: bfloat16 [512, 4, 180, 128], P('grp', 'rep'), may hold values from -1.796875 to 1.796875
- lengths: int32 [512, 4], P('grp', 'rep'), may hold values from 16 to 180
- cand_ids: int32 [16, 4, 64], P('grp', 'rep'), may hold values from 0 to 511, as said below
- owner_map: int32 [4, 512], P('rep'), may hold values from 0 to 511, as said below
- teacher: float32 [16, 4, 64], P('grp', 'rep'), may hold values from -12 to 312
- weights: float32 [16, 4], P('grp', 'rep'), may hold values from 0.5 to 18
Outputs:
- loss: float32 [], replicated
- query_grad: float32 [16, 4, 32, 128], P('grp', 'rep')
- passage_grad: bfloat16 [512, 4, 180, 128], P('grp', 'rep')
The draws below stay inside these ranges and needn't reach their ends.
Inputs may be any that keep to these rules, and one draw needn't show every extreme that they name: `cand_ids`: within each replica, the 128 candidates of the queries of one grp index have storage rows of which at most 32 (counted with repeats) lie in any one aligned block of 64 rows; in every draw, in each replica, one block receives exactly 32 from every grp index. `owner_map`: each row is a permutation of 0 to 511.
All inputs are finite; a program needn't handle non-finite values.
Results may differ from the reference program's by a relative error of at most 0.0055.
Values may be sent and summed in bfloat16 or wider, within the bound.
No kernel may reach another device: no remote copies, remote signals or barrier semaphores. Data moves between devices by JAX's collectives and lax.ppermute only.
A program may use at most 128 MiB of HBM per device.

```python
import math
import jax
import jax.numpy as jnp
from jax import lax

DIM = 128
QL = 32
PL = 180
NWAY = 64
Q_DEV = 2
P_DEV = 64
GROUPS = 8
REPS = 4
QUERIES = 16
PASSAGES = 512


def routing(key):
    ref_count = Q_DEV * NWAY
    capacity = 2 * ref_count // GROUPS
    pool_size = GROUPS * capacity
    keys = jax.random.split(jax.random.fold_in(key, 7), 5)
    hot_owner = jax.random.randint(keys[0], (REPS,), 0, GROUPS)
    pool_owner = jnp.arange(pool_size, dtype=jnp.int32) // capacity
    priority = jax.random.randint(keys[1], (GROUPS, REPS, pool_size), 0, 1 << 20) * pool_size + jnp.arange(pool_size, dtype=jnp.int32)
    is_hot = pool_owner[None, None, :] == hot_owner[None, :, None]
    priority = jnp.where(is_hot, jnp.arange(pool_size, dtype=jnp.int32) - pool_size, priority)
    order = jnp.argsort(priority, axis=-1)[..., :ref_count]
    owners = pool_owner[order]
    shuffle_key = jax.random.randint(keys[2], (GROUPS, REPS, ref_count), 0, 1 << 20) * ref_count + jnp.arange(ref_count, dtype=jnp.int32)
    shuffle = jnp.argsort(shuffle_key, axis=-1)
    owners = jnp.take_along_axis(owners, shuffle, axis=-1)
    slot_rows = jax.random.randint(keys[3], (GROUPS, REPS, ref_count), 0, P_DEV)
    storage = owners * P_DEV + slot_rows
    perm_keys = jax.random.split(keys[4], REPS)
    owner_table = jax.vmap(lambda one_key: jax.random.permutation(one_key, P_DEV * GROUPS))(perm_keys).astype(jnp.int32)
    inverse = jnp.argsort(owner_table, axis=-1).astype(jnp.int32)
    wide_inverse = jnp.broadcast_to(inverse[None], (GROUPS, REPS, P_DEV * GROUPS))
    identity = jnp.take_along_axis(wide_inverse, storage, axis=-1)
    candidate_ids = identity.reshape(GROUPS, REPS, Q_DEV, NWAY).transpose(0, 2, 1, 3).reshape(GROUPS * Q_DEV, REPS, NWAY)
    return (candidate_ids.astype(jnp.int32), owner_table)


def draw_cand_ids(key, part):
    return routing(key)[0]


def draw_owner_map(key, part):
    return routing(key)[1]


def draw_queries(key, part):
    keys = jax.random.split(jax.random.fold_in(key, 11), 2)
    shape = (QUERIES, REPS, QL, DIM)
    normal_part = jnp.clip(jax.random.normal(keys[0], shape, jnp.float32), -3.5, 3.5)
    row_scale = jnp.exp(jax.random.uniform(keys[1], (QUERIES, REPS, 1, 1), jnp.float32, math.log(0.03), math.log(3.0)))
    return (0.3 * normal_part * row_scale).astype(jnp.bfloat16)


def draw_teacher(key, part):
    keys = jax.random.split(jax.random.fold_in(key, 13), 1)
    normal_part = 2.0 * jnp.clip(jax.random.normal(keys[0], (QUERIES, REPS, NWAY), jnp.float32), -6.0, 6.0)
    return normal_part


def draw_weights(key, part):
    keys = jax.random.split(jax.random.fold_in(key, 17), 1)
    query_index = jnp.arange(QUERIES, dtype=jnp.int32)[:, None]
    replica_index = jnp.arange(REPS, dtype=jnp.int32)[None, :]
    device_index = query_index // Q_DEV * REPS + replica_index
    ramp = 1.0 + 2.0 * device_index.astype(jnp.float32) / (GROUPS * REPS - 1)
    return jnp.exp(jax.random.uniform(keys[0], (QUERIES, REPS), jnp.float32, math.log(0.5), math.log(2.0))) * ramp


def place_ends(values, stream_key, low, largest):
    longest = values.shape.index(max(values.shape))
    spots = []
    for shift in (0, 1):
        where = [jax.random.randint(jax.random.fold_in(stream_key, axis), (), 0, length) for axis, length in enumerate(values.shape)]
        where[longest] = (where[longest] + shift) % values.shape[longest]
        spots.append(tuple(where))
    return values.at[spots[0]].set(low).at[spots[1]].set(largest)


def block_levels(key, shape, pieces, low, top_value):
    loudness = 1.0
    for position, shards_of in pieces:
        heights = jax.random.uniform(jax.random.fold_in(jax.random.fold_in(key, 6), position), (shards_of,), jnp.float32, low / len(pieces), top_value / len(pieces))
        loudness = loudness * jnp.repeat(jnp.exp(heights), shape[position] // shards_of).reshape((-1,) + (1,) * (len(shape) - 1 - position))
    return loudness


def gaussian(rng, extent, width, bound, shards=(), held_as=jnp.bfloat16):
    entries = width * jax.random.normal(rng, extent, jnp.float32)
    if shards:
        entries = entries * block_levels(rng, extent, shards, -0.22, 0.18)
    return jnp.clip(entries, -bound, bound).astype(held_as)


def setup_inputs(seed: int = 0) -> dict:
    seeds = jax.random.split(jax.random.key(seed), 8)
    return {
        "queries": draw_queries(jax.random.fold_in(seeds[7], 71), 0),
        "passages": gaussian(seeds[1], (PASSAGES, REPS, PL, DIM), 0.3, 1.796875, ((0, 8), (1, 4))),
        "lengths": place_ends(jax.random.randint(seeds[2], (PASSAGES, REPS), 16, PL + 1), jax.random.fold_in(seeds[2], 1), 16, PL).astype(jnp.int32),
        "cand_ids": draw_cand_ids(jax.random.fold_in(seeds[7], 71), 0),
        "owner_map": draw_owner_map(jax.random.fold_in(seeds[7], 71), 0),
        "teacher": draw_teacher(jax.random.fold_in(seeds[7], 71), 0),
        "weights": draw_weights(jax.random.fold_in(seeds[7], 71), 0),
    }


temper = 0.05


def rounded(values):
    return lax.optimization_barrier(values.astype(jnp.bfloat16)).astype(jnp.float32)


def token_softmax(products, lengths_used):
    usable = lax.broadcasted_iota(jnp.int32, products.shape, products.ndim - 1) < lengths_used[..., None, None]
    scaled = jnp.where(usable, products / temper, -1e30)
    highest = jnp.max(scaled, axis=-1, keepdims=True)
    powers = jnp.where(usable, jnp.exp(scaled - highest), 0.0)
    summed = jnp.sum(powers, axis=-1, keepdims=True)
    matched = temper * (highest[..., 0] + jnp.log(summed[..., 0]))
    return matched, powers / summed


def pair_terms(query_tokens, passage_tokens, lengths_used):
    products = jnp.einsum("id,cjd->cij", query_tokens.astype(jnp.float32), passage_tokens.astype(jnp.float32))
    matched, attention = token_softmax(products, lengths_used)
    return jnp.sum(matched, axis=-1), attention


def reference(queries, passages, lengths, cand_ids, owner_map, teacher, weights):
    query_count = queries.shape[0]
    replicas = queries.shape[1]

    def fetch_blocks(query_row, replica):
        storage_rows = owner_map[replica][cand_ids[query_row, replica]]
        return storage_rows, passages[storage_rows, replica], lengths[storage_rows, replica]

    def score_one(flat_index):
        query_row = flat_index // replicas
        replica = flat_index % replicas
        storage_rows, blocks, lengths_used = fetch_blocks(query_row, replica)
        return pair_terms(queries[query_row, replica], blocks, lengths_used)[0]

    student = lax.map(score_one, jnp.arange(query_count * replicas, dtype=jnp.int32))
    student = student.reshape(query_count, replicas, -1)
    log_student = jax.nn.log_softmax(student, axis=-1)
    log_teacher = jax.nn.log_softmax(teacher, axis=-1)
    teacher_prob = jnp.exp(log_teacher)
    divergence = jnp.sum(teacher_prob * (log_teacher - log_student), axis=-1)
    weight_sum = jnp.sum(weights)
    loss_value = jnp.sum(weights * divergence) / weight_sum
    score_grad = (query_count * replicas) * weights[..., None] / weight_sum * (jnp.exp(log_student) - teacher_prob)
    query_parts = []
    passage_parts = []
    for replica in range(replicas):
        def backward(accum_grad, query_row):
            storage_rows, blocks, lengths_used = fetch_blocks(query_row, replica)
            query_tokens = queries[query_row, replica]
            unused, attention = pair_terms(query_tokens, blocks, lengths_used)
            scaled_grad = rounded(score_grad[query_row, replica][:, None, None] * attention)
            pair_query = rounded(jnp.einsum("cij,cjd->cid", scaled_grad, blocks.astype(jnp.float32)))
            query_part = jnp.sum(pair_query, axis=0)
            pair_passage = rounded(jnp.einsum("cij,id->cjd", scaled_grad, query_tokens.astype(jnp.float32)))
            accum_grad = accum_grad.at[storage_rows].add(pair_passage)
            return accum_grad, query_part

        initial = jnp.zeros((passages.shape[0],) + passages.shape[2:], jnp.float32)
        summed, replica_grads = lax.scan(backward, initial, jnp.arange(query_count, dtype=jnp.int32))
        query_parts.append(replica_grads)
        passage_parts.append(summed.astype(jnp.bfloat16))
    return loss_value, jnp.stack(query_parts, axis=1), jnp.stack(passage_parts, axis=1)
```

```python
import functools
import math

import jax
import jax.numpy as jnp
from jax import lax
from jax.experimental import pallas as pl
from jax.experimental.pallas import tpu as pltpu
from jax.sharding import PartitionSpec as P

TEMPER = 0.05
LOG2E = math.log2(math.e)
MASKED = -1e30
KINDS = 8
UNROLL = 4
HIGHEST = lax.Precision.HIGHEST
VMEM = pltpu.VMEM
SMEM = pltpu.SMEM


def round_up(value, multiple):
    return -(-value // multiple) * multiple


def iota(shape, dim):
    return lax.broadcasted_iota(jnp.int32, shape, dim)


def three_parts(values):
    first = values.astype(jnp.bfloat16).astype(jnp.float32)
    rest = values - first
    second = rest.astype(jnp.bfloat16).astype(jnp.float32)
    third = (rest - second).astype(jnp.bfloat16).astype(jnp.float32)
    return first, second, third


def pack_kernel(passage_local, queries, cand_ids, owner_map, teacher, weights, out, aux):
    groups = out.shape[0]
    tokens = queries.shape[0]
    query_local, _, candidates = cand_ids.shape
    entries = owner_map.shape[1]
    table = owner_map[...].astype(jnp.float32)
    owner = jnp.floor((table + 0.5) * (1.0 / passage_local))
    local = table - owner * passage_local
    which = iota((8, entries), 0)
    tables = jnp.where(which == 0, owner, jnp.where(which == 1, local, 0.0)).astype(jnp.bfloat16)
    aux[...] = jnp.zeros_like(aux)
    for q in range(query_local):
        hot = (iota((entries, candidates), 0) == cand_ids[q]).astype(jnp.bfloat16)
        found = jnp.dot(tables, hot, preferred_element_type=jnp.float32)
        scores = teacher[q]
        shifted = scores - jnp.max(scores, axis=1, keepdims=True)
        log_teacher = shifted - jnp.log(jnp.sum(jnp.exp(shifted), axis=1, keepdims=True))
        weight = jnp.broadcast_to(weights[:, q : q + 1], (1, candidates))
        rows = (found[0:1], found[1:2], *three_parts(log_teacher), *three_parts(weight))
        for kind, row in enumerate(rows):
            at = kind * query_local + q
            aux[at : at + 1, 0:candidates] = row
    packed = aux[...].astype(jnp.bfloat16)
    for g in range(groups):
        out[g, 0:tokens, :] = queries[...]
        out[g, tokens:, :] = packed


def owned_rows(arrived, tokens, query_local, candidates, g, q, me):
    at = tokens + q
    owner = arrived[g, at : at + 1, 0:candidates].astype(jnp.float32)
    at = tokens + query_local + q
    local = arrived[g, at : at + 1, 0:candidates].astype(jnp.float32)
    return jnp.where(owner == me.astype(jnp.float32), local, -1.0).astype(jnp.int32)


def score_kernel(
    dims,
    count_axis,
    arrived,
    passages,
    lengths,
    weight_sums,
    scores_out,
    powers,
    inverse,
    block_row,
    block_tile,
    block_count,
    turned,
    matched,
    flags,
    flags_scalar,
    copy_done,
):
    tokens, query_local, candidates, per_tile = dims
    groups = arrived.shape[0]
    passage_count, padded, feature = passages.shape
    tiles = turned.shape[0]
    me = lax.axis_index(count_axis)
    groups_per_tile = per_tile // query_local

    column = iota(flags.shape, 1)
    passage_index = iota((passage_count, candidates), 0)
    marks = jnp.zeros(flags.shape, jnp.int32)
    for tile in range(tiles):
        hit = jnp.zeros((passage_count, candidates), jnp.int32)
        for g in range(tile * groups_per_tile, (tile + 1) * groups_per_tile):
            for q in range(query_local):
                mine = owned_rows(arrived, tokens, query_local, candidates, g, q, me)
                hit = jnp.where(passage_index == mine, 1, hit)
        any_hit = jnp.max(hit, axis=1, keepdims=True)
        marks = jnp.where(column == tile, any_hit, marks)
    flags[...] = marks
    to_scalar = pltpu.make_async_copy(flags, flags_scalar, copy_done)
    to_scalar.start()

    for tile in range(tiles):
        parts = [
            arrived[g, 0:tokens, :]
            for g in range(tile * groups_per_tile, (tile + 1) * groups_per_tile)
        ]
        block = jnp.concatenate(parts, axis=0).astype(jnp.float32)
        turned[tile] = block.T.astype(jnp.bfloat16)
    matched[...] = jnp.zeros_like(matched)
    inverse[...] = jnp.zeros_like(inverse)
    to_scalar.wait()

    def list_passage(p, count):
        for tile in range(tiles):
            block_row[0, count] = p
            block_tile[0, count] = tile
            count = count + flags_scalar[p, tile]
        return count

    count = lax.fori_loop(0, passage_count, list_passage, jnp.int32(0))
    for extra in range(UNROLL):
        block_row[0, count + extra] = passage_count
        block_tile[0, count + extra] = 0
    steps = (count + UNROLL - 1) // UNROLL
    block_count[0, 0] = steps

    token_index = iota((padded, feature), 0)
    factor = LOG2E / TEMPER

    def step(s, carry):
        for u in range(UNROLL):
            b = s * UNROLL + u
            slot = block_row[0, b]
            tile = block_tile[0, b]
            p = jnp.minimum(slot, passage_count - 1)
            products = jnp.dot(passages[p], turned[tile], preferred_element_type=jnp.float32)
            products = jnp.where(token_index < lengths[0, p], products, MASKED)
            highest = jnp.max(products, axis=0, keepdims=True)
            raised = jnp.exp2((products - highest) * factor)
            summed = jnp.sum(raised, axis=0, keepdims=True)
            powers[b] = raised.astype(jnp.bfloat16)
            matched[tile, pl.ds(slot, 1), :] = highest + TEMPER * jnp.log(summed)
            inverse[tile, pl.ds(slot, 1), :] = 1.0 / summed
        return carry

    lax.fori_loop(0, steps, step, 0)

    lanes = matched.shape[2]
    query_len = lanes // per_tile
    member = iota((lanes, 128), 0) // query_len == iota((lanes, 128), 1)
    member = member.astype(jnp.float32)
    for tile in range(tiles):
        sums = jnp.dot(
            matched[tile, 0:passage_count, :],
            member,
            precision=HIGHEST,
            preferred_element_type=jnp.float32,
        )
        for inner in range(per_tile):
            g = tile * groups_per_tile + inner // query_local
            q = inner % query_local
            mine = owned_rows(arrived, tokens, query_local, candidates, g, q, me)
            column = sums[:, inner : inner + 1]
            picked = jnp.where(passage_index == mine, column, 0.0)
            row = jnp.sum(picked, axis=0, keepdims=True)
            at = tile * per_tile + inner
            scores_out[0, at : at + 1, :] = row
    queries_all = tiles * per_tile
    total = jnp.sum(weight_sums[...], axis=1, keepdims=True)
    scores_out[0, queries_all:, :] = jnp.broadcast_to(
        total, (scores_out.shape[1] - queries_all, candidates)
    )
    for g in range(1, groups):
        scores_out[g] = scores_out[0]


def query_kernel(
    dims,
    count_axis,
    arrived,
    scores,
    passages,
    inverse,
    powers,
    block_row,
    block_tile,
    block_count,
    grads_out,
    scaled,
    loss_parts,
    multiplier,
    sums,
):
    tokens, query_local, candidates, per_tile, query_total = dims
    groups = arrived.shape[0]
    passage_count, padded, feature = passages.shape
    tiles, _, lanes = inverse.shape
    groups_per_tile = per_tile // query_local
    queries_all = tiles * per_tile
    query_len = lanes // per_tile
    me = lax.axis_index(count_axis)

    got = scores[0]
    for g in range(1, groups):
        got = got + scores[g]
    student = got[0:queries_all]
    weight_sum = got[queries_all : queries_all + 1, 0:1]

    def gather_parts(kind):
        rows = []
        for g in range(groups):
            parts = []
            for part in range(3):
                at = tokens + (kind + part) * query_local
                block = arrived[g, at : at + query_local, 0:candidates]
                parts.append(block.astype(jnp.float32))
            rows.append((parts[0] + parts[1]) + parts[2])
        return jnp.concatenate(rows, axis=0)

    log_teacher = gather_parts(2)
    weight = gather_parts(5)
    shifted = student - jnp.max(student, axis=1, keepdims=True)
    log_student = shifted - jnp.log(jnp.sum(jnp.exp(shifted), axis=1, keepdims=True))
    teacher_prob = jnp.exp(log_teacher)
    spread = jnp.sum(weight * teacher_prob * (log_teacher - log_student), axis=1, keepdims=True)
    numerator = jnp.sum(spread, axis=0, keepdims=True)
    half = iota(loss_parts.shape, 0)
    loss_parts[...] = jnp.where(half == 0, numerator, weight_sum)
    grad = (query_total * weight / weight_sum) * (jnp.exp(log_student) - teacher_prob)

    passage_index = iota((passage_count, candidates), 0)
    lane_query = iota((passage_count, lanes), 1) // query_len
    multiplier[...] = jnp.zeros_like(multiplier)
    for tile in range(tiles):
        spread_out = jnp.zeros((passage_count, lanes), jnp.float32)
        for inner in range(per_tile):
            g = tile * groups_per_tile + inner // query_local
            q = inner % query_local
            mine = owned_rows(arrived, tokens, query_local, candidates, g, q, me)
            at = tile * per_tile + inner
            picked = jnp.where(passage_index == mine, grad[at : at + 1], 0.0)
            column = jnp.sum(picked, axis=1, keepdims=True)
            spread_out = jnp.where(lane_query == inner, column, spread_out)
        multiplier[tile, 0:passage_count, :] = spread_out * inverse[tile, 0:passage_count, :]

    sums[...] = jnp.zeros_like(sums)

    def step(s, carry):
        for u in range(UNROLL):
            b = s * UNROLL + u
            slot = block_row[0, b]
            tile = block_tile[0, b]
            p = jnp.minimum(slot, passage_count - 1)
            part = powers[b].astype(jnp.float32) * multiplier[tile, pl.ds(slot, 1), :]
            part = part.astype(jnp.bfloat16)
            scaled[b] = part
            sums[tile] += lax.dot_general(
                passages[p], part, (((0,), (0,)), ((), ())), preferred_element_type=jnp.float32
            )
        return carry

    lax.fori_loop(0, block_count[0, 0], step, 0)
    for tile in range(tiles):
        turned = sums[tile].T.astype(jnp.bfloat16)
        for inner in range(groups_per_tile):
            g = tile * groups_per_tile + inner
            grads_out[g] = turned[inner * tokens : (inner + 1) * tokens]


def passage_kernel(
    dims, arrived, scaled, block_row, block_tile, block_count, out, sums, queries_all
):
    tokens, per_tile_groups = dims
    passage_count, token_len, _ = out.shape
    tiles = queries_all.shape[0]
    for tile in range(tiles):
        for inner in range(per_tile_groups):
            g = tile * per_tile_groups + inner
            queries_all[tile, inner * tokens : (inner + 1) * tokens, :] = arrived[g, 0:tokens, :]

    def clear(p, carry):
        sums[p] = jnp.zeros(sums.shape[1:], jnp.float32)
        return carry

    lax.fori_loop(0, passage_count, clear, 0)

    def step(s, carry):
        for u in range(UNROLL):
            b = s * UNROLL + u
            slot = block_row[0, b]
            sums[slot] += jnp.dot(
                scaled[b], queries_all[block_tile[0, b]], preferred_element_type=jnp.float32
            )
        return carry

    lax.fori_loop(0, block_count[0, 0], step, 0)

    def finish(p, carry):
        out[p] = sums[p, 0:token_len, :].astype(out.dtype)
        return carry

    lax.fori_loop(0, passage_count, finish, 0)


def vmem(count):
    return [pl.BlockSpec(memory_space=VMEM)] * count


def smem(count):
    return [pl.BlockSpec(memory_space=SMEM)] * count


def on_device(queries, passages, lengths, cand_ids, owner_map, teacher, weights):
    groups = lax.axis_size("grp")
    replicas = lax.axis_size("rep")
    query_local, _, query_len, feature = queries.shape
    passage_local, _, token_len, _ = passages.shape
    candidates = cand_ids.shape[2]
    tokens = query_local * query_len
    lanes = 128
    per_tile = lanes // query_len
    tiles = groups * tokens // lanes
    padded = round_up(token_len, 16)
    ref_count = query_local * candidates
    capacity = groups * (2 * ref_count // groups)
    blocks = min(passage_local * tiles, capacity) + UNROLL
    aux_rows = round_up(KINDS * query_local, 16)
    slots = round_up(passage_local + 1, 8)
    score_rows = round_up(groups * query_local + 1, 8)
    params = pltpu.CompilerParams
    shape = jax.ShapeDtypeStruct

    weight_row = weights.T
    share = pl.pallas_call(
        functools.partial(pack_kernel, passage_local),
        out_shape=shape((groups, tokens + aux_rows, feature), jnp.bfloat16),
        in_specs=vmem(5),
        out_specs=pl.BlockSpec(memory_space=VMEM),
        scratch_shapes=[VMEM((aux_rows, feature), jnp.float32)],
        name="pack",
    )(queries.reshape(tokens, feature), cand_ids, owner_map, teacher, weight_row)
    arrived = lax.all_to_all(share, "grp", split_axis=0, concat_axis=0, tiled=True)

    weight_sums = weight_row
    hop = 1
    while hop < replicas:
        ring = [(r, r ^ hop) for r in range(replicas)]
        weight_sums = weight_sums + lax.ppermute(weight_sums, "rep", ring)
        hop *= 2

    rows = jnp.pad(passages[:, 0], ((0, 0), (0, padded - token_len), (0, 0)))

    dims = (tokens, query_local, candidates, per_tile)
    scores, powers, inverse, block_row, block_tile, block_count = pl.pallas_call(
        functools.partial(score_kernel, dims, "grp"),
        out_shape=(
            shape((groups, score_rows, candidates), jnp.float32),
            shape((blocks, padded, lanes), jnp.bfloat16),
            shape((tiles, slots, lanes), jnp.float32),
            shape((1, blocks), jnp.int32),
            shape((1, blocks), jnp.int32),
            shape((1, 1), jnp.int32),
        ),
        in_specs=vmem(2) + smem(1) + vmem(1),
        out_specs=tuple(vmem(3) + smem(3)),
        scratch_shapes=[
            VMEM((tiles, feature, lanes), jnp.bfloat16),
            VMEM((tiles, slots, lanes), jnp.float32),
            VMEM((passage_local, 128), jnp.int32),
            SMEM((passage_local, 128), jnp.int32),
            pltpu.SemaphoreType.DMA,
        ],
        name="score",
    )(arrived, rows, lengths.T, weight_sums)
    all_scores = lax.all_to_all(scores, "grp", split_axis=0, concat_axis=0, tiled=True)

    query_total = query_local * groups * replicas
    grads, scaled, loss_parts = pl.pallas_call(
        functools.partial(query_kernel, dims + (query_total,), "grp"),
        out_shape=(
            shape((groups, tokens, feature), jnp.bfloat16),
            shape((blocks, padded, lanes), jnp.bfloat16),
            shape((8, 128), jnp.float32),
        ),
        in_specs=vmem(5) + smem(3),
        out_specs=tuple(vmem(3)),
        scratch_shapes=[
            VMEM((tiles, slots, lanes), jnp.float32),
            VMEM((tiles, feature, lanes), jnp.float32),
        ],
        input_output_aliases={4: 1},
        name="query_grad",
    )(arrived, all_scores, rows, inverse, powers, block_row, block_tile, block_count)
    returned = lax.all_to_all(grads, "grp", split_axis=0, concat_axis=0, tiled=True)

    passage_grad = pl.pallas_call(
        functools.partial(passage_kernel, (tokens, per_tile // query_local)),
        out_shape=shape((passage_local, token_len, feature), jnp.bfloat16),
        in_specs=vmem(2) + smem(3),
        out_specs=pl.BlockSpec(memory_space=VMEM),
        scratch_shapes=[
            VMEM((passage_local + 1, padded, feature), jnp.float32),
            VMEM((tiles, lanes, feature), jnp.bfloat16),
        ],
        name="passage_grad",
    )(arrived, scaled, block_row, block_tile, block_count)

    numerator = loss_parts[0:1, 0:1]
    weight_sum = loss_parts[1, 0]
    hop = 1
    while hop < replicas:
        ring = [(r, r ^ hop) for r in range(replicas)]
        numerator = numerator + lax.ppermute(numerator, "rep", ring)
        hop *= 2
    loss = numerator[0, 0] / weight_sum
    query_grad = jnp.sum(returned.astype(jnp.float32), axis=0)
    query_grad = query_grad.reshape(query_local, 1, query_len, feature)
    return (loss, query_grad, passage_grad[:, None])


def solution(mesh):
    return jax.shard_map(
        on_device,
        mesh=mesh,
        in_specs=(
            P("grp", "rep", None, None),
            P("grp", "rep", None, None),
            P("grp", "rep"),
            P("grp", "rep", None),
            P("rep", None),
            P("grp", "rep", None),
            P("grp", "rep"),
        ),
        out_specs=(P(), P("grp", "rep", None, None), P("grp", "rep", None, None)),
        check_vma=False,
    )
```

```python
import functools
import math

import jax
import jax.numpy as jnp
from jax import lax
from jax.experimental import pallas as pl
from jax.experimental.pallas import tpu as pltpu
from jax.sharding import PartitionSpec as P

TEMPER = 0.05
LOG2E = math.log2(math.e)
MASKED = -1e30
KINDS = 8
UNROLL = 4
SPREAD = 4
HIGHEST = lax.Precision.HIGHEST
VMEM = pltpu.VMEM
SMEM = pltpu.SMEM


def round_up(value, multiple):
    return -(-value // multiple) * multiple


def iota(shape, dim):
    return lax.broadcasted_iota(jnp.int32, shape, dim)


def three_parts(values):
    first = values.astype(jnp.bfloat16).astype(jnp.float32)
    rest = values - first
    second = rest.astype(jnp.bfloat16).astype(jnp.float32)
    third = (rest - second).astype(jnp.bfloat16).astype(jnp.float32)
    return first, second, third


def pack_kernel(passage_local, queries, cand_ids, owner_map, teacher, weights, out, aux):
    groups = out.shape[0]
    tokens = queries.shape[0]
    query_local, _, candidates = cand_ids.shape
    entries = owner_map.shape[1]
    table = owner_map[...].astype(jnp.float32)
    owner = jnp.floor((table + 0.5) * (1.0 / passage_local))
    local = table - owner * passage_local
    which = iota((8, entries), 0)
    tables = jnp.where(which == 0, owner, jnp.where(which == 1, local, 0.0)).astype(jnp.bfloat16)
    aux[...] = jnp.zeros_like(aux)
    for q in range(query_local):
        hot = (iota((entries, candidates), 0) == cand_ids[q]).astype(jnp.bfloat16)
        found = jnp.dot(tables, hot, preferred_element_type=jnp.float32)
        scores = teacher[q]
        shifted = scores - jnp.max(scores, axis=1, keepdims=True)
        log_teacher = shifted - jnp.log(jnp.sum(jnp.exp(shifted), axis=1, keepdims=True))
        weight = jnp.broadcast_to(weights[:, q : q + 1], (1, candidates))
        rows = (found[0:1], found[1:2], *three_parts(log_teacher), *three_parts(weight))
        for kind, row in enumerate(rows):
            at = kind * query_local + q
            aux[at : at + 1, 0:candidates] = row
    packed = aux[...].astype(jnp.bfloat16)
    for g in range(groups):
        out[g, 0:tokens, :] = queries[...]
        out[g, tokens:, :] = packed


def owned_rows(arrived, tokens, query_local, candidates, g, q, me):
    at = tokens + q
    owner = arrived[g, at : at + 1, 0:candidates].astype(jnp.float32)
    at = tokens + query_local + q
    local = arrived[g, at : at + 1, 0:candidates].astype(jnp.float32)
    return jnp.where(owner == me.astype(jnp.float32), local, -1.0).astype(jnp.int32)


def prepare_kernel(stored, rows_out, turned_out, gathered):
    token_len, chunk, feature = stored.shape
    padded = rows_out.shape[1]
    pitch = gathered.shape[0] // chunk
    for p in range(chunk):
        at = p * pitch + token_len
        gathered[at : (p + 1) * pitch, :] = jnp.zeros((pitch - token_len, feature), jnp.float32)

    def spread(j, carry):
        for u in range(SPREAD):
            at = j * SPREAD + u
            gathered[pl.ds(at, chunk, stride=pitch), :] = stored[at].astype(jnp.float32)
        return carry

    lax.fori_loop(0, token_len // SPREAD, spread, 0)
    for j in range(token_len - token_len % SPREAD, token_len):
        gathered[pl.ds(j, chunk, stride=pitch), :] = stored[j].astype(jnp.float32)

    for p in range(chunk):
        block = gathered[p * pitch : p * pitch + padded, :].astype(jnp.bfloat16)
        rows_out[p] = block
        turned_out[p, :, 0:padded] = block.T


def list_blocks(flags_scalar, block_row, block_tile, block_count, passage_count, tiles):
    def list_passage(p, count):
        for tile in range(tiles):
            block_row[0, count] = p
            block_tile[0, count] = tile
            count = count + flags_scalar[p, tile]
        return count

    count = lax.fori_loop(0, passage_count, list_passage, jnp.int32(0))
    for extra in range(3 * UNROLL):
        block_row[0, count + extra] = passage_count
        block_tile[0, count + extra] = 0
    steps = (count + 2 * UNROLL - 1) // (2 * UNROLL)
    block_count[0, 0] = steps
    return steps


def score_kernel(
    dims,
    axis,
    arrived,
    lengths,
    passages_hbm,
    scores_out,
    highest,
    summed,
    weight_sum,
    block_row,
    block_tile,
    block_count,
    powers_hbm,
    passages,
    turned,
    flags,
    flags_scalar,
    penalty,
    even,
    odd,
    powers,
    flags_done,
    rows_done,
    powers_done,
):
    tokens, query_local, candidates, per_tile = dims
    groups = arrived.shape[0]
    passage_count, padded, feature = passages.shape
    tiles, _, lanes = highest.shape
    me = lax.axis_index(axis)
    groups_per_tile = per_tile // query_local
    fetch_rows = pltpu.make_async_copy(passages_hbm, passages, rows_done)
    fetch_rows.start()

    column = iota(flags.shape, 1)
    passage_index = iota((passage_count, candidates), 0)
    marks = jnp.zeros(flags.shape, jnp.int32)
    for tile in range(tiles):
        hit = jnp.zeros((passage_count, candidates), jnp.int32)
        for g in range(tile * groups_per_tile, (tile + 1) * groups_per_tile):
            for q in range(query_local):
                mine = owned_rows(arrived, tokens, query_local, candidates, g, q, me)
                hit = jnp.where(passage_index == mine, 1, hit)
        any_hit = jnp.max(hit, axis=1, keepdims=True)
        marks = jnp.where(column == tile, any_hit, marks)
    flags[...] = marks
    to_scalar = pltpu.make_async_copy(flags, flags_scalar, flags_done)
    to_scalar.start()

    total = jnp.zeros((1, 1), jnp.float32)
    for g in range(groups):
        for q in range(query_local):
            for part in range(5, 8):
                at = tokens + part * query_local + q
                total = total + arrived[g, at : at + 1, 0:1].astype(jnp.float32)
    weight_sum[...] = jnp.broadcast_to(total, weight_sum.shape)
    for tile in range(tiles):
        parts = [
            arrived[g, 0:tokens, :]
            for g in range(tile * groups_per_tile, (tile + 1) * groups_per_tile)
        ]
        block = jnp.concatenate(parts, axis=0).astype(jnp.float32)
        turned[tile] = block.T.astype(jnp.bfloat16)
    highest[...] = jnp.zeros_like(highest)
    summed[...] = jnp.ones_like(summed)
    penalty[...] = jnp.where(iota(penalty.shape, 0) < padded, 0.0, MASKED)
    to_scalar.wait()
    steps = list_blocks(flags_scalar, block_row, block_tile, block_count, passage_count, tiles)
    fetch_rows.wait()

    factor = LOG2E / TEMPER

    def multiply(first, into):
        for u in range(UNROLL):
            p = jnp.minimum(block_row[0, first + u], passage_count - 1)
            tile = block_tile[0, first + u]
            into[u] = jnp.dot(passages[p], turned[tile], preferred_element_type=jnp.float32)

    def soften(first, held):
        for u in range(UNROLL):
            slot = block_row[0, first + u]
            tile = block_tile[0, first + u]
            length = lengths[0, jnp.minimum(slot, passage_count - 1)]
            products = held[u] + penalty[pl.ds(padded - length, padded), :]
            top = jnp.max(products, axis=0, keepdims=True)
            raised = jnp.exp2((products - top) * factor)
            powers[first + u] = raised.astype(jnp.bfloat16)
            highest[tile, pl.ds(slot, 1), :] = top
            summed[tile, pl.ds(slot, 1), :] = jnp.sum(raised, axis=0, keepdims=True)

    def chunk_copy(s):
        at = pl.ds(s * 2 * UNROLL, 2 * UNROLL)
        return pltpu.make_async_copy(powers.at[at], powers_hbm.at[at], powers_done.at[s])

    multiply(0, even)

    def step(s, carry):
        first = s * 2 * UNROLL
        multiply(first + UNROLL, odd)
        soften(first, even)
        multiply(first + 2 * UNROLL, even)
        soften(first + UNROLL, odd)
        chunk_copy(s).start()
        return carry

    lax.fori_loop(0, steps, step, 0)

    query_len = lanes // per_tile
    member = iota((lanes, 128), 0) // query_len == iota((lanes, 128), 1)
    member = member.astype(jnp.float32)
    scores_out[0] = jnp.zeros(scores_out.shape[1:], jnp.float32)
    for tile in range(tiles):
        matched = highest[tile, 0:passage_count, :] + TEMPER * jnp.log(
            summed[tile, 0:passage_count, :]
        )
        sums = jnp.dot(matched, member, precision=HIGHEST, preferred_element_type=jnp.float32)
        for inner in range(per_tile):
            g = tile * groups_per_tile + inner // query_local
            q = inner % query_local
            mine = owned_rows(arrived, tokens, query_local, candidates, g, q, me)
            picked = jnp.where(passage_index == mine, sums[:, inner : inner + 1], 0.0)
            at = tile * per_tile + inner
            scores_out[0, at : at + 1, 0:candidates] = jnp.sum(picked, axis=0, keepdims=True)
    for g in range(1, groups):
        scores_out[g] = scores_out[0]

    def finish(s, carry):
        chunk_copy(s).wait()
        return carry

    lax.fori_loop(0, steps, finish, 0)


def query_kernel(
    dims,
    axis,
    arrived,
    scores,
    summed,
    weight_sum,
    block_row,
    block_tile,
    block_count,
    turned_hbm,
    powers_hbm,
    grads_out,
    multiplier,
    numerator_out,
    turned,
    powers,
    sums,
    turned_done,
    powers_done,
):
    tokens, query_local, candidates, per_tile, query_total = dims
    groups = arrived.shape[0]
    tiles, slots, lanes = summed.shape
    passage_count, _, padded = turned.shape
    padded = powers.shape[1]
    groups_per_tile = per_tile // query_local
    queries_all = tiles * per_tile
    query_len = lanes // per_tile
    me = lax.axis_index(axis)
    steps = block_count[0, 0]

    fetch_turned = pltpu.make_async_copy(turned_hbm, turned, turned_done)
    fetch_turned.start()

    def chunk_copy(s):
        at = pl.ds(s * 2 * UNROLL, 2 * UNROLL)
        return pltpu.make_async_copy(powers_hbm.at[at], powers.at[at], powers_done.at[s])

    def fetch(s, carry):
        chunk_copy(s).start()
        return carry

    lax.fori_loop(0, steps, fetch, 0)

    got = scores[0]
    for g in range(1, groups):
        got = got + scores[g]
    student = got[0:queries_all, 0:candidates]

    def gather_parts(kind):
        rows = []
        for g in range(groups):
            parts = []
            for part in range(3):
                at = tokens + (kind + part) * query_local
                block = arrived[g, at : at + query_local, 0:candidates]
                parts.append(block.astype(jnp.float32))
            rows.append((parts[0] + parts[1]) + parts[2])
        return jnp.concatenate(rows, axis=0)

    log_teacher = gather_parts(2)
    weight = gather_parts(5)
    shifted = student - jnp.max(student, axis=1, keepdims=True)
    log_student = shifted - jnp.log(jnp.sum(jnp.exp(shifted), axis=1, keepdims=True))
    teacher_prob = jnp.exp(log_teacher)
    spread = jnp.sum(weight * teacher_prob * (log_teacher - log_student), axis=1, keepdims=True)
    numerator = jnp.sum(spread, axis=0, keepdims=True)
    numerator_out[...] = jnp.broadcast_to(numerator, numerator_out.shape)
    scale = query_total / weight_sum[0:1, 0:1]
    grad = (weight * scale) * (jnp.exp(log_student) - teacher_prob)

    passage_index = iota((passage_count, candidates), 0)
    lane_query = iota((passage_count, lanes), 1) // query_len
    for tile in range(tiles):
        spread_out = jnp.zeros((passage_count, lanes), jnp.float32)
        for inner in range(per_tile):
            g = tile * groups_per_tile + inner // query_local
            q = inner % query_local
            mine = owned_rows(arrived, tokens, query_local, candidates, g, q, me)
            at = tile * per_tile + inner
            picked = jnp.where(passage_index == mine, grad[at : at + 1], 0.0)
            total = jnp.sum(picked, axis=1, keepdims=True)
            spread_out = jnp.where(lane_query == inner, total, spread_out)
        multiplier[tile, 0:passage_count, :] = spread_out / summed[tile, 0:passage_count, :]
        multiplier[tile, passage_count:, :] = jnp.zeros((slots - passage_count, lanes), jnp.float32)

    sums[...] = jnp.zeros_like(sums)
    fetch_turned.wait()

    def step(s, carry):
        chunk_copy(s).wait()
        for u in range(2 * UNROLL):
            b = s * 2 * UNROLL + u
            slot = block_row[0, b]
            tile = block_tile[0, b]
            p = jnp.minimum(slot, passage_count - 1)
            part = powers[b].astype(jnp.float32) * multiplier[tile, pl.ds(slot, 1), :]
            part = part.astype(jnp.bfloat16)
            sums[tile] += jnp.dot(
                turned[p, :, 0:padded], part, preferred_element_type=jnp.float32
            )
        return carry

    lax.fori_loop(0, steps, step, 0)
    for tile in range(tiles):
        back = sums[tile].T.astype(jnp.bfloat16)
        for inner in range(groups_per_tile):
            g = tile * groups_per_tile + inner
            grads_out[g] = back[inner * tokens : (inner + 1) * tokens]


def passage_kernel(
    dims,
    arrived,
    multiplier,
    block_row,
    block_tile,
    block_count,
    powers_hbm,
    out,
    powers,
    sums,
    queries_all,
    powers_done,
):
    tokens, per_tile_groups = dims
    token_len, passage_count, feature = out.shape
    tiles = queries_all.shape[0]
    padded = powers.shape[1]
    pitch = sums.shape[0] // (passage_count + 1)
    steps = block_count[0, 0]

    def chunk_copy(s):
        at = pl.ds(s * 2 * UNROLL, 2 * UNROLL)
        return pltpu.make_async_copy(powers_hbm.at[at], powers.at[at], powers_done.at[s])

    def fetch(s, carry):
        chunk_copy(s).start()
        return carry

    lax.fori_loop(0, steps, fetch, 0)
    for tile in range(tiles):
        for inner in range(per_tile_groups):
            g = tile * per_tile_groups + inner
            queries_all[tile, inner * tokens : (inner + 1) * tokens, :] = arrived[g, 0:tokens, :]

    def clear(p, carry):
        sums[pl.ds(p * pitch, pitch), :] = jnp.zeros((pitch, feature), jnp.float32)
        return carry

    lax.fori_loop(0, passage_count, clear, 0)

    def step(s, carry):
        chunk_copy(s).wait()
        for u in range(2 * UNROLL):
            b = s * 2 * UNROLL + u
            slot = block_row[0, b]
            tile = block_tile[0, b]
            part = powers[b].astype(jnp.float32) * multiplier[tile, pl.ds(slot, 1), :]
            at = pl.ds(pl.multiple_of(slot * pitch, 8), padded)
            sums[at, :] += jnp.dot(
                part.astype(jnp.bfloat16), queries_all[tile], preferred_element_type=jnp.float32
            )
        return carry

    lax.fori_loop(0, steps, step, 0)

    def store(j, carry):
        for u in range(SPREAD):
            at = j * SPREAD + u
            out[at] = sums[pl.ds(at, passage_count, stride=pitch), :].astype(out.dtype)
        return carry

    lax.fori_loop(0, token_len // SPREAD, store, 0)
    for j in range(token_len - token_len % SPREAD, token_len):
        out[j] = sums[pl.ds(j, passage_count, stride=pitch), :].astype(out.dtype)


def vmem(count):
    return [pl.BlockSpec(memory_space=VMEM)] * count


def smem(count):
    return [pl.BlockSpec(memory_space=SMEM)] * count


def over_replicas(values, replicas):
    hop = 1
    while hop < replicas:
        ring = [(r, r ^ hop) for r in range(replicas)]
        values = values + lax.ppermute(values, "rep", ring)
        hop *= 2
    return values


def hbm(count):
    return [pl.BlockSpec(memory_space=pltpu.HBM)] * count


def on_device(queries, passages, lengths, cand_ids, owner_map, teacher, weights):
    groups = lax.axis_size("grp")
    replicas = lax.axis_size("rep")
    query_local, _, query_len, feature = queries.shape
    passage_local, _, token_len, _ = passages.shape
    candidates = cand_ids.shape[2]
    tokens = query_local * query_len
    lanes = 128
    per_tile = lanes // query_len
    tiles = groups * tokens // lanes
    padded = round_up(token_len, 16)
    pitch = round_up(padded, 16) + 8
    ref_count = query_local * candidates
    capacity = groups * (2 * ref_count // groups)
    limit = min(passage_local * tiles, capacity)
    blocks = limit + 3 * UNROLL
    chunks = -(-limit // (2 * UNROLL))
    aux_rows = round_up(KINDS * query_local, 16)
    slots = round_up(passage_local + 1, 8)
    score_rows = round_up(groups * query_local, 8)
    shape = jax.ShapeDtypeStruct
    params = pltpu.CompilerParams(vmem_limit_bytes=36 * 2**20)

    share = pl.pallas_call(
        functools.partial(pack_kernel, passage_local),
        out_shape=shape((groups, tokens + aux_rows, feature), jnp.bfloat16),
        in_specs=vmem(5),
        out_specs=pl.BlockSpec(memory_space=VMEM),
        scratch_shapes=[VMEM((aux_rows, feature), jnp.float32)],
        name="pack",
        compiler_params=params,
    )(queries.reshape(tokens, feature), cand_ids, owner_map, teacher, weights.T)
    arrived = lax.all_to_all(share, "grp", split_axis=0, concat_axis=0, tiled=True)

    chunk = math.gcd(passage_local, 16)
    rows, turned = pl.pallas_call(
        prepare_kernel,
        grid=(passage_local // chunk,),
        out_shape=(
            shape((passage_local, padded, feature), jnp.bfloat16),
            shape((passage_local, feature, round_up(padded, 128)), jnp.bfloat16),
        ),
        in_specs=[pl.BlockSpec((token_len, chunk, feature), lambda i: (0, i, 0))],
        out_specs=(
            pl.BlockSpec((chunk, padded, feature), lambda i: (i, 0, 0)),
            pl.BlockSpec((chunk, feature, round_up(padded, 128)), lambda i: (i, 0, 0)),
        ),
        scratch_shapes=[VMEM((chunk * pitch, feature), jnp.float32)],
        name="prepare",
        compiler_params=params,
    )(passages[:, 0].transpose(1, 0, 2))

    dims = (tokens, query_local, candidates, per_tile)
    scores, highest, summed, weight_sum, block_row, block_tile, block_count, powers = (
        pl.pallas_call(
            functools.partial(score_kernel, dims, "grp"),
            out_shape=(
                shape((groups, score_rows, 128), jnp.float32),
                shape((tiles, slots, lanes), jnp.float32),
                shape((tiles, slots, lanes), jnp.float32),
                shape((1, 128), jnp.float32),
                shape((1, blocks), jnp.int32),
                shape((1, blocks), jnp.int32),
                shape((1, 1), jnp.int32),
                shape((chunks * 2 * UNROLL, padded, lanes), jnp.bfloat16),
            ),
            in_specs=vmem(1) + smem(1) + hbm(1),
            out_specs=tuple(vmem(4) + smem(3) + hbm(1)),
            scratch_shapes=[
                VMEM((passage_local, padded, feature), jnp.bfloat16),
                VMEM((tiles, feature, lanes), jnp.bfloat16),
                VMEM((passage_local, 128), jnp.int32),
                SMEM((passage_local, 128), jnp.int32),
                VMEM((2 * padded, lanes), jnp.float32),
                VMEM((UNROLL, padded, lanes), jnp.float32),
                VMEM((UNROLL, padded, lanes), jnp.float32),
                VMEM((chunks * 2 * UNROLL, padded, lanes), jnp.bfloat16),
                pltpu.SemaphoreType.DMA,
                pltpu.SemaphoreType.DMA,
                pltpu.SemaphoreType.DMA((chunks,)),
            ],
            name="score",
            compiler_params=params,
        )(arrived, lengths.T, rows)
    )
    all_scores = lax.all_to_all(scores, "grp", split_axis=0, concat_axis=0, tiled=True)
    weight_sum = over_replicas(weight_sum, replicas)

    query_total = query_local * groups * replicas
    grads, multiplier, numerator = pl.pallas_call(
        functools.partial(query_kernel, dims + (query_total,), "grp"),
        out_shape=(
            shape((groups, tokens, feature), jnp.bfloat16),
            shape((tiles, slots, lanes), jnp.float32),
            shape((1, 128), jnp.float32),
        ),
        in_specs=vmem(4) + smem(3) + hbm(2),
        out_specs=tuple(vmem(3)),
        scratch_shapes=[
            VMEM(turned.shape, jnp.bfloat16),
            VMEM(powers.shape, jnp.bfloat16),
            VMEM((tiles, feature, lanes), jnp.float32),
            pltpu.SemaphoreType.DMA,
            pltpu.SemaphoreType.DMA((chunks,)),
        ],
        name="query_grad",
        compiler_params=params,
    )(arrived, all_scores, summed, weight_sum, block_row, block_tile, block_count, turned, powers)
    returned = lax.all_to_all(grads, "grp", split_axis=0, concat_axis=0, tiled=True)

    passage_grad = pl.pallas_call(
        functools.partial(passage_kernel, (tokens, per_tile // query_local)),
        out_shape=shape((token_len, passage_local, feature), jnp.bfloat16),
        in_specs=vmem(2) + smem(3) + hbm(1),
        out_specs=pl.BlockSpec(memory_space=VMEM),
        scratch_shapes=[
            VMEM(powers.shape, jnp.bfloat16),
            VMEM(((passage_local + 1) * pitch, feature), jnp.float32),
            VMEM((tiles, lanes, feature), jnp.bfloat16),
            pltpu.SemaphoreType.DMA((chunks,)),
        ],
        name="passage_grad",
        compiler_params=params,
    )(arrived, multiplier, block_row, block_tile, block_count, powers)
    numerator = over_replicas(numerator, replicas)

    loss = numerator[0, 0] / weight_sum[0, 0]
    query_grad = jnp.sum(returned.astype(jnp.float32), axis=0)
    query_grad = query_grad.reshape(query_local, 1, query_len, feature)
    return (loss, query_grad, passage_grad.transpose(1, 0, 2)[:, None])


def solution(mesh):
    return jax.shard_map(
        on_device,
        mesh=mesh,
        in_specs=(
            P("grp", "rep", None, None),
            P("grp", "rep", None, None),
            P("grp", "rep"),
            P("grp", "rep", None),
            P("rep", None),
            P("grp", "rep", None),
            P("grp", "rep"),
        ),
        out_specs=(P(), P("grp", "rep", None, None), P("grp", "rep", None, None)),
        check_vma=False,
    )
```

```python
import functools
import math

import jax
import jax.numpy as jnp
from jax import lax
from jax.experimental import pallas as pl
from jax.experimental.pallas import tpu as pltpu
from jax.sharding import PartitionSpec as P

TEMPER = 0.05
LOG2E = math.log2(math.e)
MASKED = -1e30
KINDS = 8
UNROLL = 4
SPREAD = 4
HIGHEST = lax.Precision.HIGHEST
VMEM = pltpu.VMEM
SMEM = pltpu.SMEM


def round_up(value, multiple):
    return -(-value // multiple) * multiple


def iota(shape, dim):
    return lax.broadcasted_iota(jnp.int32, shape, dim)


def three_parts(values):
    first = values.astype(jnp.bfloat16).astype(jnp.float32)
    rest = values - first
    second = rest.astype(jnp.bfloat16).astype(jnp.float32)
    third = (rest - second).astype(jnp.bfloat16).astype(jnp.float32)
    return first, second, third


def pack_kernel(passage_local, queries, cand_ids, owner_map, teacher, weights, out, aux):
    groups = out.shape[0]
    tokens = queries.shape[0]
    query_local, _, candidates = cand_ids.shape
    entries = owner_map.shape[1]
    table = owner_map[...].astype(jnp.float32)
    owner = jnp.floor((table + 0.5) * (1.0 / passage_local))
    local = table - owner * passage_local
    which = iota((8, entries), 0)
    tables = jnp.where(which == 0, owner, jnp.where(which == 1, local, 0.0)).astype(jnp.bfloat16)
    aux[...] = jnp.zeros_like(aux)
    for q in range(query_local):
        hot = (iota((entries, candidates), 0) == cand_ids[q]).astype(jnp.bfloat16)
        found = jnp.dot(tables, hot, preferred_element_type=jnp.float32)
        scores = teacher[q]
        shifted = scores - jnp.max(scores, axis=1, keepdims=True)
        log_teacher = shifted - jnp.log(jnp.sum(jnp.exp(shifted), axis=1, keepdims=True))
        weight = jnp.broadcast_to(weights[:, q : q + 1], (1, candidates))
        rows = (found[0:1], found[1:2], *three_parts(log_teacher), *three_parts(weight))
        for kind, row in enumerate(rows):
            at = kind * query_local + q
            aux[at : at + 1, 0:candidates] = row
    packed = aux[...].astype(jnp.bfloat16)
    for g in range(groups):
        out[g, 0:tokens, :] = queries[...]
        out[g, tokens:, :] = packed


def owned_rows(arrived, tokens, query_local, candidates, g, q, me):
    at = tokens + q
    owner = arrived[g, at : at + 1, 0:candidates].astype(jnp.float32)
    at = tokens + query_local + q
    local = arrived[g, at : at + 1, 0:candidates].astype(jnp.float32)
    return jnp.where(owner == me.astype(jnp.float32), local, -1.0).astype(jnp.int32)


def prepare_kernel(stored, rows_out, turned_out, gathered):
    token_len, chunk, feature = stored.shape
    padded = rows_out.shape[1]
    pitch = gathered.shape[0] // chunk
    for p in range(chunk):
        at = p * pitch + token_len
        gathered[at : (p + 1) * pitch, :] = jnp.zeros((pitch - token_len, feature), jnp.float32)

    def spread(j, carry):
        for u in range(SPREAD):
            at = j * SPREAD + u
            gathered[pl.ds(at, chunk, stride=pitch), :] = stored[at].astype(jnp.float32)
        return carry

    lax.fori_loop(0, token_len // SPREAD, spread, 0)
    for j in range(token_len - token_len % SPREAD, token_len):
        gathered[pl.ds(j, chunk, stride=pitch), :] = stored[j].astype(jnp.float32)

    for p in range(chunk):
        block = gathered[p * pitch : p * pitch + padded, :].astype(jnp.bfloat16)
        rows_out[p] = block
        turned_out[p, :, 0:padded] = block.T


def list_blocks(flags_scalar, block_row, block_tile, block_count, passage_count, tiles):
    def list_passage(p, count):
        for tile in range(tiles):
            block_row[0, count] = p
            block_tile[0, count] = tile
            count = count + flags_scalar[p, tile]
        return count

    count = lax.fori_loop(0, passage_count, list_passage, jnp.int32(0))
    for extra in range(3 * UNROLL):
        block_row[0, count + extra] = passage_count
        block_tile[0, count + extra] = 0
    steps = (count + 2 * UNROLL - 1) // (2 * UNROLL)
    block_count[0, 0] = steps
    return steps


def score_kernel(
    dims,
    axis,
    arrived,
    lengths,
    passages_hbm,
    scores_out,
    highest,
    summed,
    weight_sum,
    block_row,
    block_tile,
    block_count,
    powers_hbm,
    passages,
    turned,
    flags,
    flags_scalar,
    penalty,
    even,
    odd,
    powers,
    flags_done,
    rows_done,
    powers_done,
):
    tokens, query_local, candidates, per_tile = dims
    groups = arrived.shape[0]
    passage_count, padded, feature = passages.shape
    tiles, _, lanes = highest.shape
    me = lax.axis_index(axis)
    groups_per_tile = per_tile // query_local
    fetch_rows = pltpu.make_async_copy(passages_hbm, passages, rows_done)
    fetch_rows.start()

    column = iota(flags.shape, 1)
    passage_index = iota((passage_count, candidates), 0)
    marks = jnp.zeros(flags.shape, jnp.int32)
    for tile in range(tiles):
        hit = jnp.zeros((passage_count, candidates), jnp.int32)
        for g in range(tile * groups_per_tile, (tile + 1) * groups_per_tile):
            for q in range(query_local):
                mine = owned_rows(arrived, tokens, query_local, candidates, g, q, me)
                hit = jnp.where(passage_index == mine, 1, hit)
        any_hit = jnp.max(hit, axis=1, keepdims=True)
        marks = jnp.where(column == tile, any_hit, marks)
    flags[...] = marks
    to_scalar = pltpu.make_async_copy(flags, flags_scalar, flags_done)
    to_scalar.start()

    total = jnp.zeros((1, 1), jnp.float32)
    for g in range(groups):
        for q in range(query_local):
            for part in range(5, 8):
                at = tokens + part * query_local + q
                total = total + arrived[g, at : at + 1, 0:1].astype(jnp.float32)
    weight_sum[...] = jnp.broadcast_to(total, weight_sum.shape)
    for tile in range(tiles):
        parts = [
            arrived[g, 0:tokens, :]
            for g in range(tile * groups_per_tile, (tile + 1) * groups_per_tile)
        ]
        block = jnp.concatenate(parts, axis=0).astype(jnp.float32)
        turned[tile] = block.T.astype(jnp.bfloat16)
    highest[...] = jnp.zeros_like(highest)
    summed[...] = jnp.ones_like(summed)
    penalty[...] = jnp.where(iota(penalty.shape, 0) < padded, 0.0, MASKED)
    to_scalar.wait()
    steps = list_blocks(flags_scalar, block_row, block_tile, block_count, passage_count, tiles)
    fetch_rows.wait()

    factor = LOG2E / TEMPER

    def multiply(first, into):
        for u in range(UNROLL):
            p = jnp.minimum(block_row[0, first + u], passage_count - 1)
            tile = block_tile[0, first + u]
            into[u] = jnp.dot(passages[p], turned[tile], preferred_element_type=jnp.float32)

    def soften(first, held):
        for u in range(UNROLL):
            slot = block_row[0, first + u]
            tile = block_tile[0, first + u]
            length = lengths[0, jnp.minimum(slot, passage_count - 1)]
            products = held[u] + penalty[pl.ds(padded - length, padded), :]
            top = jnp.max(products, axis=0, keepdims=True)
            raised = jnp.exp2((products - top) * factor)
            powers[first + u] = raised.astype(jnp.bfloat16)
            highest[tile, pl.ds(slot, 1), :] = top
            summed[tile, pl.ds(slot, 1), :] = jnp.sum(raised, axis=0, keepdims=True)

    def chunk_copy(s):
        at = pl.ds(s * 2 * UNROLL, 2 * UNROLL)
        return pltpu.make_async_copy(powers.at[at], powers_hbm.at[at], powers_done.at[s])

    multiply(0, even)

    def step(s, carry):
        first = s * 2 * UNROLL
        multiply(first + UNROLL, odd)
        soften(first, even)
        multiply(first + 2 * UNROLL, even)
        soften(first + UNROLL, odd)
        chunk_copy(s).start()
        return carry

    lax.fori_loop(0, steps, step, 0)

    query_len = lanes // per_tile
    member = iota((lanes, 128), 0) // query_len == iota((lanes, 128), 1)
    member = member.astype(jnp.float32)
    scores_out[0] = jnp.zeros(scores_out.shape[1:], jnp.float32)
    for tile in range(tiles):
        matched = highest[tile, 0:passage_count, :] + TEMPER * jnp.log(
            summed[tile, 0:passage_count, :]
        )
        sums = jnp.dot(matched, member, precision=HIGHEST, preferred_element_type=jnp.float32)
        for inner in range(per_tile):
            g = tile * groups_per_tile + inner // query_local
            q = inner % query_local
            mine = owned_rows(arrived, tokens, query_local, candidates, g, q, me)
            picked = jnp.where(passage_index == mine, sums[:, inner : inner + 1], 0.0)
            at = tile * per_tile + inner
            scores_out[0, at : at + 1, 0:candidates] = jnp.sum(picked, axis=0, keepdims=True)
    for g in range(1, groups):
        scores_out[g] = scores_out[0]

    def finish(s, carry):
        chunk_copy(s).wait()
        return carry

    lax.fori_loop(0, steps, finish, 0)


def query_kernel(
    dims,
    axis,
    arrived,
    scores,
    summed,
    weight_sum,
    block_row,
    block_tile,
    block_count,
    turned_hbm,
    powers_hbm,
    grads_out,
    multiplier,
    numerator_out,
    turned,
    powers,
    sums,
    turned_done,
    powers_done,
):
    tokens, query_local, candidates, per_tile, query_total = dims
    groups = arrived.shape[0]
    tiles, slots, lanes = summed.shape
    passage_count, _, padded = turned.shape
    padded = powers.shape[1]
    groups_per_tile = per_tile // query_local
    queries_all = tiles * per_tile
    query_len = lanes // per_tile
    me = lax.axis_index(axis)
    steps = block_count[0, 0]

    fetch_turned = pltpu.make_async_copy(turned_hbm, turned, turned_done)
    fetch_turned.start()

    def chunk_copy(s):
        at = pl.ds(s * 2 * UNROLL, 2 * UNROLL)
        return pltpu.make_async_copy(powers_hbm.at[at], powers.at[at], powers_done.at[s])

    def fetch(s, carry):
        chunk_copy(s).start()
        return carry

    lax.fori_loop(0, steps, fetch, 0)

    got = scores[0]
    for g in range(1, groups):
        got = got + scores[g]
    student = got[0:queries_all, 0:candidates]

    def gather_parts(kind):
        rows = []
        for g in range(groups):
            parts = []
            for part in range(3):
                at = tokens + (kind + part) * query_local
                block = arrived[g, at : at + query_local, 0:candidates]
                parts.append(block.astype(jnp.float32))
            rows.append((parts[0] + parts[1]) + parts[2])
        return jnp.concatenate(rows, axis=0)

    log_teacher = gather_parts(2)
    weight = gather_parts(5)
    shifted = student - jnp.max(student, axis=1, keepdims=True)
    log_student = shifted - jnp.log(jnp.sum(jnp.exp(shifted), axis=1, keepdims=True))
    teacher_prob = jnp.exp(log_teacher)
    spread = jnp.sum(weight * teacher_prob * (log_teacher - log_student), axis=1, keepdims=True)
    numerator = jnp.sum(spread, axis=0, keepdims=True)
    numerator_out[...] = jnp.broadcast_to(numerator, numerator_out.shape)
    scale = query_total / weight_sum[0:1, 0:1]
    grad = (weight * scale) * (jnp.exp(log_student) - teacher_prob)

    passage_index = iota((passage_count, candidates), 0)
    lane_query = iota((passage_count, lanes), 1) // query_len
    for tile in range(tiles):
        spread_out = jnp.zeros((passage_count, lanes), jnp.float32)
        for inner in range(per_tile):
            g = tile * groups_per_tile + inner // query_local
            q = inner % query_local
            mine = owned_rows(arrived, tokens, query_local, candidates, g, q, me)
            at = tile * per_tile + inner
            picked = jnp.where(passage_index == mine, grad[at : at + 1], 0.0)
            total = jnp.sum(picked, axis=1, keepdims=True)
            spread_out = jnp.where(lane_query == inner, total, spread_out)
        multiplier[tile, 0:passage_count, :] = spread_out / summed[tile, 0:passage_count, :]
        multiplier[tile, passage_count:, :] = jnp.zeros((slots - passage_count, lanes), jnp.float32)

    sums[...] = jnp.zeros_like(sums)
    fetch_turned.wait()

    def step(s, carry):
        chunk_copy(s).wait()
        for u in range(2 * UNROLL):
            b = s * 2 * UNROLL + u
            slot = block_row[0, b]
            tile = block_tile[0, b]
            p = jnp.minimum(slot, passage_count - 1)
            part = powers[b].astype(jnp.float32) * multiplier[tile, pl.ds(slot, 1), :]
            part = part.astype(jnp.bfloat16)
            sums[tile] += jnp.dot(
                turned[p, :, 0:padded], part, preferred_element_type=jnp.float32
            )
        return carry

    lax.fori_loop(0, steps, step, 0)
    for tile in range(tiles):
        back = sums[tile].T.astype(jnp.bfloat16)
        for inner in range(groups_per_tile):
            g = tile * groups_per_tile + inner
            grads_out[g] = back[inner * tokens : (inner + 1) * tokens]


def passage_kernel(
    dims,
    arrived,
    multiplier,
    block_row,
    block_tile,
    block_count,
    powers_hbm,
    out,
    powers,
    sums,
    queries_all,
    powers_done,
):
    tokens, per_tile_groups = dims
    token_len, passage_count, feature = out.shape
    tiles = queries_all.shape[0]
    padded = powers.shape[1]
    pitch = sums.shape[0] // (passage_count + 1)
    steps = block_count[0, 0]

    def chunk_copy(s):
        at = pl.ds(s * 2 * UNROLL, 2 * UNROLL)
        return pltpu.make_async_copy(powers_hbm.at[at], powers.at[at], powers_done.at[s])

    def fetch(s, carry):
        chunk_copy(s).start()
        return carry

    lax.fori_loop(0, steps, fetch, 0)
    for tile in range(tiles):
        for inner in range(per_tile_groups):
            g = tile * per_tile_groups + inner
            queries_all[tile, inner * tokens : (inner + 1) * tokens, :] = arrived[g, 0:tokens, :]

    def clear(p, carry):
        sums[pl.ds(p * pitch, pitch), :] = jnp.zeros((pitch, feature), jnp.float32)
        return carry

    lax.fori_loop(0, passage_count, clear, 0)

    def step(s, carry):
        chunk_copy(s).wait()
        for u in range(2 * UNROLL):
            b = s * 2 * UNROLL + u
            slot = block_row[0, b]
            tile = block_tile[0, b]
            part = powers[b].astype(jnp.float32) * multiplier[tile, pl.ds(slot, 1), :]
            at = pl.ds(pl.multiple_of(slot * pitch, 8), padded)
            sums[at, :] += jnp.dot(
                part.astype(jnp.bfloat16), queries_all[tile], preferred_element_type=jnp.float32
            )
        return carry

    lax.fori_loop(0, steps, step, 0)

    def store(j, carry):
        for u in range(SPREAD):
            at = j * SPREAD + u
            out[at] = sums[pl.ds(at, passage_count, stride=pitch), :].astype(out.dtype)
        return carry

    lax.fori_loop(0, token_len // SPREAD, store, 0)
    for j in range(token_len - token_len % SPREAD, token_len):
        out[j] = sums[pl.ds(j, passage_count, stride=pitch), :].astype(out.dtype)


def vmem(count):
    return [pl.BlockSpec(memory_space=VMEM)] * count


def smem(count):
    return [pl.BlockSpec(memory_space=SMEM)] * count


def over_replicas(values, replicas):
    hop = 1
    while hop < replicas:
        ring = [(r, r ^ hop) for r in range(replicas)]
        values = values + lax.ppermute(values, "rep", ring)
        hop *= 2
    return values


def hbm(count):
    return [pl.BlockSpec(memory_space=pltpu.HBM)] * count


def on_device(queries, passages, lengths, cand_ids, owner_map, teacher, weights):
    groups = lax.axis_size("grp")
    replicas = lax.axis_size("rep")
    query_local, _, query_len, feature = queries.shape
    passage_local, _, token_len, _ = passages.shape
    candidates = cand_ids.shape[2]
    tokens = query_local * query_len
    lanes = 128
    per_tile = lanes // query_len
    tiles = groups * tokens // lanes
    padded = round_up(token_len, 16)
    pitch = round_up(padded, 16) + 8
    ref_count = query_local * candidates
    capacity = groups * (2 * ref_count // groups)
    limit = min(passage_local * tiles, capacity)
    blocks = limit + 3 * UNROLL
    chunks = -(-limit // (2 * UNROLL))
    aux_rows = round_up(KINDS * query_local, 16)
    slots = round_up(passage_local + 1, 8)
    score_rows = round_up(groups * query_local, 8)
    shape = jax.ShapeDtypeStruct
    params = pltpu.CompilerParams(vmem_limit_bytes=62 * 2**20)

    share = pl.pallas_call(
        functools.partial(pack_kernel, passage_local),
        out_shape=shape((groups, tokens + aux_rows, feature), jnp.bfloat16),
        in_specs=vmem(5),
        out_specs=pl.BlockSpec(memory_space=VMEM),
        scratch_shapes=[VMEM((aux_rows, feature), jnp.float32)],
        name="pack",
        compiler_params=params,
    )(queries.reshape(tokens, feature), cand_ids, owner_map, teacher, weights.T)
    arrived = lax.all_to_all(share, "grp", split_axis=0, concat_axis=0, tiled=True)

    chunk = math.gcd(passage_local, 16)
    rows, turned = pl.pallas_call(
        prepare_kernel,
        grid=(passage_local // chunk,),
        out_shape=(
            shape((passage_local, padded, feature), jnp.bfloat16),
            shape((passage_local, feature, round_up(padded, 128)), jnp.bfloat16),
        ),
        in_specs=[pl.BlockSpec((token_len, chunk, feature), lambda i: (0, i, 0))],
        out_specs=(
            pl.BlockSpec((chunk, padded, feature), lambda i: (i, 0, 0)),
            pl.BlockSpec((chunk, feature, round_up(padded, 128)), lambda i: (i, 0, 0)),
        ),
        scratch_shapes=[VMEM((chunk * pitch, feature), jnp.float32)],
        name="prepare",
        compiler_params=params,
    )(passages[:, 0].transpose(1, 0, 2))

    dims = (tokens, query_local, candidates, per_tile)
    scores, highest, summed, weight_sum, block_row, block_tile, block_count, powers = (
        pl.pallas_call(
            functools.partial(score_kernel, dims, "grp"),
            out_shape=(
                shape((groups, score_rows, 128), jnp.float32),
                shape((tiles, slots, lanes), jnp.float32),
                shape((tiles, slots, lanes), jnp.float32),
                shape((1, 128), jnp.float32),
                shape((1, blocks), jnp.int32),
                shape((1, blocks), jnp.int32),
                shape((1, 1), jnp.int32),
                shape((chunks * 2 * UNROLL, padded, lanes), jnp.bfloat16),
            ),
            in_specs=vmem(1) + smem(1) + hbm(1),
            out_specs=tuple(vmem(4) + smem(3) + hbm(1)),
            scratch_shapes=[
                VMEM((passage_local, padded, feature), jnp.bfloat16),
                VMEM((tiles, feature, lanes), jnp.bfloat16),
                VMEM((passage_local, 128), jnp.int32),
                SMEM((passage_local, 128), jnp.int32),
                VMEM((2 * padded, lanes), jnp.float32),
                VMEM((UNROLL, padded, lanes), jnp.float32),
                VMEM((UNROLL, padded, lanes), jnp.float32),
                VMEM((chunks * 2 * UNROLL, padded, lanes), jnp.bfloat16),
                pltpu.SemaphoreType.DMA,
                pltpu.SemaphoreType.DMA,
                pltpu.SemaphoreType.DMA((chunks,)),
            ],
            name="score",
            compiler_params=params,
        )(arrived, lengths.T, rows)
    )
    all_scores = lax.all_to_all(scores, "grp", split_axis=0, concat_axis=0, tiled=True)
    weight_sum = over_replicas(weight_sum, replicas)

    query_total = query_local * groups * replicas
    grads, multiplier, numerator = pl.pallas_call(
        functools.partial(query_kernel, dims + (query_total,), "grp"),
        out_shape=(
            shape((groups, tokens, feature), jnp.bfloat16),
            shape((tiles, slots, lanes), jnp.float32),
            shape((1, 128), jnp.float32),
        ),
        in_specs=vmem(4) + smem(3) + hbm(2),
        out_specs=tuple(vmem(3)),
        scratch_shapes=[
            VMEM(turned.shape, jnp.bfloat16),
            VMEM(powers.shape, jnp.bfloat16),
            VMEM((tiles, feature, lanes), jnp.float32),
            pltpu.SemaphoreType.DMA,
            pltpu.SemaphoreType.DMA((chunks,)),
        ],
        name="query_grad",
        compiler_params=params,
    )(arrived, all_scores, summed, weight_sum, block_row, block_tile, block_count, turned, powers)
    returned = lax.all_to_all(grads, "grp", split_axis=0, concat_axis=0, tiled=True)

    passage_grad = pl.pallas_call(
        functools.partial(passage_kernel, (tokens, per_tile // query_local)),
        out_shape=shape((token_len, passage_local, feature), jnp.bfloat16),
        in_specs=vmem(2) + smem(3) + hbm(1),
        out_specs=pl.BlockSpec(memory_space=VMEM),
        scratch_shapes=[
            VMEM(powers.shape, jnp.bfloat16),
            VMEM(((passage_local + 1) * pitch, feature), jnp.float32),
            VMEM((tiles, lanes, feature), jnp.bfloat16),
            pltpu.SemaphoreType.DMA((chunks,)),
        ],
        name="passage_grad",
        compiler_params=params,
    )(arrived, multiplier, block_row, block_tile, block_count, powers)
    numerator = over_replicas(numerator, replicas)

    loss = numerator[0, 0] / weight_sum[0, 0]
    query_grad = jnp.sum(returned.astype(jnp.float32), axis=0)
    query_grad = query_grad.reshape(query_local, 1, query_len, feature)
    return (loss, query_grad, passage_grad.transpose(1, 0, 2)[:, None])


def solution(mesh):
    return jax.shard_map(
        on_device,
        mesh=mesh,
        in_specs=(
            P("grp", "rep", None, None),
            P("grp", "rep", None, None),
            P("grp", "rep"),
            P("grp", "rep", None),
            P("rep", None),
            P("grp", "rep", None),
            P("grp", "rep"),
        ),
        out_specs=(P(), P("grp", "rep", None, None), P("grp", "rep", None, None)),
        check_vma=False,
    )
```

```python
import functools
import math

import jax
import jax.numpy as jnp
from jax import lax
from jax.experimental import pallas as pl
from jax.experimental.pallas import tpu as pltpu
from jax.sharding import PartitionSpec as P

TEMPER = 0.05
LOG2E = math.log2(math.e)
MASKED = -1e30
KINDS = 8
UNROLL = 8
SPREAD = 4
HIGHEST = lax.Precision.HIGHEST
VMEM = pltpu.VMEM
SMEM = pltpu.SMEM


def round_up(value, multiple):
    return -(-value // multiple) * multiple


def iota(shape, dim):
    return lax.broadcasted_iota(jnp.int32, shape, dim)


def three_parts(values):
    first = values.astype(jnp.bfloat16).astype(jnp.float32)
    rest = values - first
    second = rest.astype(jnp.bfloat16).astype(jnp.float32)
    third = (rest - second).astype(jnp.bfloat16).astype(jnp.float32)
    return first, second, third


def pack_kernel(passage_local, queries, cand_ids, owner_map, teacher, weights, out, aux):
    groups = out.shape[0]
    tokens = queries.shape[0]
    query_local, _, candidates = cand_ids.shape
    entries = owner_map.shape[1]
    table = owner_map[...].astype(jnp.float32)
    owner = jnp.floor((table + 0.5) * (1.0 / passage_local))
    local = table - owner * passage_local
    which = iota((8, entries), 0)
    tables = jnp.where(which == 0, owner, jnp.where(which == 1, local, 0.0)).astype(jnp.bfloat16)
    aux[...] = jnp.zeros_like(aux)
    for q in range(query_local):
        hot = (iota((entries, candidates), 0) == cand_ids[q]).astype(jnp.bfloat16)
        found = jnp.dot(tables, hot, preferred_element_type=jnp.float32)
        scores = teacher[q]
        shifted = scores - jnp.max(scores, axis=1, keepdims=True)
        log_teacher = shifted - jnp.log(jnp.sum(jnp.exp(shifted), axis=1, keepdims=True))
        weight = jnp.broadcast_to(weights[:, q : q + 1], (1, candidates))
        rows = (found[0:1], found[1:2], *three_parts(log_teacher), *three_parts(weight))
        for kind, row in enumerate(rows):
            at = kind * query_local + q
            aux[at : at + 1, 0:candidates] = row
    packed = aux[...].astype(jnp.bfloat16)
    for g in range(groups):
        out[g, 0:tokens, :] = queries[...]
        out[g, tokens:, :] = packed


def owned_rows(arrived, tokens, query_local, candidates, g, q, me):
    at = tokens + q
    owner = arrived[g, at : at + 1, 0:candidates].astype(jnp.float32)
    at = tokens + query_local + q
    local = arrived[g, at : at + 1, 0:candidates].astype(jnp.float32)
    return jnp.where(owner == me.astype(jnp.float32), local, -1.0).astype(jnp.int32)


def prepare_kernel(stored, rows_out, gathered):
    token_len, chunk, feature = stored.shape
    padded = rows_out.shape[1]
    pitch = gathered.shape[0] // chunk
    for p in range(chunk):
        at = p * pitch + token_len
        gathered[at : (p + 1) * pitch, :] = jnp.zeros((pitch - token_len, feature), jnp.float32)

    def spread(j, carry):
        for u in range(SPREAD):
            at = j * SPREAD + u
            gathered[pl.ds(at, chunk, stride=pitch), :] = stored[at].astype(jnp.float32)
        return carry

    lax.fori_loop(0, token_len // SPREAD, spread, 0)
    for j in range(token_len - token_len % SPREAD, token_len):
        gathered[pl.ds(j, chunk, stride=pitch), :] = stored[j].astype(jnp.float32)

    for p in range(chunk):
        rows_out[p] = gathered[p * pitch : p * pitch + padded, :].astype(jnp.bfloat16)


def list_blocks(flags_scalar, block_row, block_tile, block_count, passage_count, tiles):
    def list_passage(p, count):
        for tile in range(tiles):
            block_row[0, count] = p
            block_tile[0, count] = tile
            count = count + flags_scalar[p, tile]
        return count

    count = lax.fori_loop(0, passage_count, list_passage, jnp.int32(0))
    for extra in range(3 * UNROLL):
        block_row[0, count + extra] = passage_count
        block_tile[0, count + extra] = 0
    steps = (count + 2 * UNROLL - 1) // (2 * UNROLL)
    block_count[0, 0] = steps
    return steps


def score_kernel(
    dims,
    axis,
    arrived,
    lengths,
    passages_hbm,
    scores_out,
    highest,
    summed,
    weight_sum,
    block_row,
    block_tile,
    block_count,
    powers_hbm,
    passages,
    turned,
    flags,
    flags_scalar,
    penalty,
    even,
    odd,
    even_top,
    odd_top,
    powers,
    flags_done,
    rows_done,
    powers_done,
):
    tokens, query_local, candidates, per_tile = dims
    groups = arrived.shape[0]
    passage_count, padded, feature = passages.shape
    tiles, _, lanes = highest.shape
    me = lax.axis_index(axis)
    groups_per_tile = per_tile // query_local
    fetch_rows = pltpu.make_async_copy(passages_hbm, passages, rows_done)
    fetch_rows.start()

    column = iota(flags.shape, 1)
    passage_index = iota((passage_count, candidates), 0)
    marks = jnp.zeros(flags.shape, jnp.int32)
    for tile in range(tiles):
        hit = jnp.zeros((passage_count, candidates), jnp.int32)
        for g in range(tile * groups_per_tile, (tile + 1) * groups_per_tile):
            for q in range(query_local):
                mine = owned_rows(arrived, tokens, query_local, candidates, g, q, me)
                hit = jnp.where(passage_index == mine, 1, hit)
        any_hit = jnp.max(hit, axis=1, keepdims=True)
        marks = jnp.where(column == tile, any_hit, marks)
    flags[...] = marks
    to_scalar = pltpu.make_async_copy(flags, flags_scalar, flags_done)
    to_scalar.start()

    total = jnp.zeros((1, 1), jnp.float32)
    for g in range(groups):
        for q in range(query_local):
            for part in range(5, 8):
                at = tokens + part * query_local + q
                total = total + arrived[g, at : at + 1, 0:1].astype(jnp.float32)
    weight_sum[...] = jnp.broadcast_to(total, weight_sum.shape)
    for tile in range(tiles):
        parts = [
            arrived[g, 0:tokens, :]
            for g in range(tile * groups_per_tile, (tile + 1) * groups_per_tile)
        ]
        block = jnp.concatenate(parts, axis=0).astype(jnp.float32)
        turned[tile] = block.T.astype(jnp.bfloat16)
    highest[...] = jnp.zeros_like(highest)
    summed[...] = jnp.ones_like(summed)
    penalty[...] = jnp.where(iota(penalty.shape, 0) < padded, 0.0, MASKED)
    to_scalar.wait()
    steps = list_blocks(flags_scalar, block_row, block_tile, block_count, passage_count, tiles)
    fetch_rows.wait()

    factor = LOG2E / TEMPER

    def multiply(first, into, tops):
        for u in range(UNROLL):
            p = jnp.minimum(block_row[0, first + u], passage_count - 1)
            tile = block_tile[0, first + u]
            products = jnp.dot(passages[p], turned[tile], preferred_element_type=jnp.float32)
            products = products + penalty[pl.ds(padded - lengths[0, p], padded), :]
            into[u] = products
            tops[u : u + 1, :] = jnp.max(products, axis=0, keepdims=True)

    def soften(first, held, tops):
        for u in range(UNROLL):
            slot = block_row[0, first + u]
            tile = block_tile[0, first + u]
            top = tops[u : u + 1, :]
            raised = jnp.exp2((held[u] - top) * factor)
            powers[first + u] = raised.astype(jnp.bfloat16)
            highest[tile, pl.ds(slot, 1), :] = top
            summed[tile, pl.ds(slot, 1), :] = jnp.sum(raised, axis=0, keepdims=True)

    def chunk_copy(s):
        at = pl.ds(s * 2 * UNROLL, 2 * UNROLL)
        return pltpu.make_async_copy(powers.at[at], powers_hbm.at[at], powers_done.at[s])

    multiply(0, even, even_top)

    def step(s, carry):
        first = s * 2 * UNROLL
        multiply(first + UNROLL, odd, odd_top)
        soften(first, even, even_top)
        multiply(first + 2 * UNROLL, even, even_top)
        soften(first + UNROLL, odd, odd_top)
        chunk_copy(s).start()
        return carry

    lax.fori_loop(0, steps, step, 0)

    query_len = lanes // per_tile
    member = iota((lanes, 128), 0) // query_len == iota((lanes, 128), 1)
    member = member.astype(jnp.float32)
    scores_out[0] = jnp.zeros(scores_out.shape[1:], jnp.float32)
    for tile in range(tiles):
        matched = highest[tile, 0:passage_count, :] + TEMPER * jnp.log(
            summed[tile, 0:passage_count, :]
        )
        sums = jnp.dot(matched, member, precision=HIGHEST, preferred_element_type=jnp.float32)
        for inner in range(per_tile):
            g = tile * groups_per_tile + inner // query_local
            q = inner % query_local
            mine = owned_rows(arrived, tokens, query_local, candidates, g, q, me)
            picked = jnp.where(passage_index == mine, sums[:, inner : inner + 1], 0.0)
            at = tile * per_tile + inner
            scores_out[0, at : at + 1, 0:candidates] = jnp.sum(picked, axis=0, keepdims=True)
    for g in range(1, groups):
        scores_out[g] = scores_out[0]

    def finish(s, carry):
        chunk_copy(s).wait()
        return carry

    lax.fori_loop(0, steps, finish, 0)


def pair_sums(values):
    while len(values) > 1:
        values = [values[i] + values[i + 1] for i in range(0, len(values), 2)]
    return values[0]


def query_kernel(dims, axis, arrived, scores, summed, *refs):
    tokens, query_local, candidates, per_tile, query_total, replicas = dims
    weight_sums, refs = refs[:replicas], refs[replicas:]
    block_row, block_tile, block_count, passages_hbm, powers_hbm = refs[:5]
    grads_out, multiplier, numerator_out, weight_sum_out = refs[5:9]
    passages, powers, sums, rows_done, powers_done = refs[9:]
    groups = arrived.shape[0]
    tiles, slots, lanes = summed.shape
    passage_count, padded, _ = passages.shape
    groups_per_tile = per_tile // query_local
    queries_all = tiles * per_tile
    query_len = lanes // per_tile
    me = lax.axis_index(axis)
    steps = block_count[0, 0]

    fetch_rows = pltpu.make_async_copy(passages_hbm, passages, rows_done)
    fetch_rows.start()

    def chunk_copy(s):
        at = pl.ds(s * 2 * UNROLL, 2 * UNROLL)
        return pltpu.make_async_copy(powers_hbm.at[at], powers.at[at], powers_done.at[s])

    def fetch(s, carry):
        chunk_copy(s).start()
        return carry

    lax.fori_loop(0, steps, fetch, 0)

    got = scores[0]
    for g in range(1, groups):
        got = got + scores[g]
    student = got[0:queries_all, 0:candidates]

    def gather_parts(kind):
        rows = []
        for g in range(groups):
            parts = []
            for part in range(3):
                at = tokens + (kind + part) * query_local
                block = arrived[g, at : at + query_local, 0:candidates]
                parts.append(block.astype(jnp.float32))
            rows.append((parts[0] + parts[1]) + parts[2])
        return jnp.concatenate(rows, axis=0)

    log_teacher = gather_parts(2)
    weight = gather_parts(5)
    shifted = student - jnp.max(student, axis=1, keepdims=True)
    log_student = shifted - jnp.log(jnp.sum(jnp.exp(shifted), axis=1, keepdims=True))
    teacher_prob = jnp.exp(log_teacher)
    spread = jnp.sum(weight * teacher_prob * (log_teacher - log_student), axis=1, keepdims=True)
    numerator = jnp.sum(spread, axis=0, keepdims=True)
    numerator_out[...] = jnp.broadcast_to(numerator, numerator_out.shape)
    weight_sum = pair_sums([one[...] for one in weight_sums])
    weight_sum_out[...] = weight_sum
    scale = query_total / weight_sum[0:1, 0:1]
    grad = (weight * scale) * (jnp.exp(log_student) - teacher_prob)

    passage_index = iota((passage_count, candidates), 0)
    lane_query = iota((passage_count, lanes), 1) // query_len
    for tile in range(tiles):
        spread_out = jnp.zeros((passage_count, lanes), jnp.float32)
        for inner in range(per_tile):
            g = tile * groups_per_tile + inner // query_local
            q = inner % query_local
            mine = owned_rows(arrived, tokens, query_local, candidates, g, q, me)
            at = tile * per_tile + inner
            picked = jnp.where(passage_index == mine, grad[at : at + 1], 0.0)
            total = jnp.sum(picked, axis=1, keepdims=True)
            spread_out = jnp.where(lane_query == inner, total, spread_out)
        multiplier[tile, 0:passage_count, :] = spread_out / summed[tile, 0:passage_count, :]
        multiplier[tile, passage_count:, :] = jnp.zeros((slots - passage_count, lanes), jnp.float32)

    sums[...] = jnp.zeros_like(sums)
    fetch_rows.wait()

    def step(s, carry):
        chunk_copy(s).wait()
        for u in range(2 * UNROLL):
            b = s * 2 * UNROLL + u
            slot = block_row[0, b]
            tile = block_tile[0, b]
            p = jnp.minimum(slot, passage_count - 1)
            part = powers[b].astype(jnp.float32) * multiplier[tile, pl.ds(slot, 1), :]
            part = part.astype(jnp.bfloat16)
            sums[tile] += lax.dot_general(
                passages[p], part, (((0,), (0,)), ((), ())), preferred_element_type=jnp.float32
            )
        return carry

    lax.fori_loop(0, steps, step, 0)
    for tile in range(tiles):
        back = sums[tile].T.astype(jnp.bfloat16)
        for inner in range(groups_per_tile):
            g = tile * groups_per_tile + inner
            grads_out[g] = back[inner * tokens : (inner + 1) * tokens]


def passage_kernel(
    dims,
    arrived,
    multiplier,
    block_row,
    block_tile,
    block_count,
    powers_hbm,
    out,
    powers,
    sums,
    queries_all,
    powers_done,
):
    tokens, per_tile_groups = dims
    token_len, passage_count, feature = out.shape
    tiles = queries_all.shape[0]
    padded = powers.shape[1]
    pitch = sums.shape[0] // (passage_count + 1)
    steps = block_count[0, 0]

    def chunk_copy(s):
        at = pl.ds(s * 2 * UNROLL, 2 * UNROLL)
        return pltpu.make_async_copy(powers_hbm.at[at], powers.at[at], powers_done.at[s])

    def fetch(s, carry):
        chunk_copy(s).start()
        return carry

    lax.fori_loop(0, steps, fetch, 0)
    for tile in range(tiles):
        for inner in range(per_tile_groups):
            g = tile * per_tile_groups + inner
            queries_all[tile, inner * tokens : (inner + 1) * tokens, :] = arrived[g, 0:tokens, :]

    def clear(p, carry):
        sums[pl.ds(p * pitch, pitch), :] = jnp.zeros((pitch, feature), jnp.float32)
        return carry

    lax.fori_loop(0, passage_count, clear, 0)

    def step(s, carry):
        chunk_copy(s).wait()
        for u in range(2 * UNROLL):
            b = s * 2 * UNROLL + u
            slot = block_row[0, b]
            tile = block_tile[0, b]
            part = powers[b].astype(jnp.float32) * multiplier[tile, pl.ds(slot, 1), :]
            at = pl.ds(pl.multiple_of(slot * pitch, 8), padded)
            sums[at, :] += jnp.dot(
                part.astype(jnp.bfloat16), queries_all[tile], preferred_element_type=jnp.float32
            )
        return carry

    lax.fori_loop(0, steps, step, 0)

    def store(j, carry):
        for u in range(SPREAD):
            at = j * SPREAD + u
            out[at] = sums[pl.ds(at, passage_count, stride=pitch), :].astype(out.dtype)
        return carry

    lax.fori_loop(0, token_len // SPREAD, store, 0)
    for j in range(token_len - token_len % SPREAD, token_len):
        out[j] = sums[pl.ds(j, passage_count, stride=pitch), :].astype(out.dtype)


def vmem(count):
    return [pl.BlockSpec(memory_space=VMEM)] * count


def smem(count):
    return [pl.BlockSpec(memory_space=SMEM)] * count


def from_replicas(values, replicas):
    rings = [[(r, r ^ hop) for r in range(replicas)] for hop in range(1, replicas)]
    return [values] + [lax.ppermute(values, "rep", ring) for ring in rings]


def hbm(count):
    return [pl.BlockSpec(memory_space=pltpu.HBM)] * count


def on_device(queries, passages, lengths, cand_ids, owner_map, teacher, weights):
    groups = lax.axis_size("grp")
    replicas = lax.axis_size("rep")
    query_local, _, query_len, feature = queries.shape
    passage_local, _, token_len, _ = passages.shape
    candidates = cand_ids.shape[2]
    tokens = query_local * query_len
    lanes = 128
    per_tile = lanes // query_len
    tiles = groups * tokens // lanes
    padded = round_up(token_len, 16)
    pitch = round_up(padded, 16) + 8
    ref_count = query_local * candidates
    capacity = groups * (2 * ref_count // groups)
    limit = min(passage_local * tiles, capacity)
    blocks = limit + 3 * UNROLL
    chunks = -(-limit // (2 * UNROLL))
    aux_rows = round_up(KINDS * query_local, 16)
    slots = round_up(passage_local + 1, 8)
    score_rows = round_up(groups * query_local, 8)
    shape = jax.ShapeDtypeStruct
    params = pltpu.CompilerParams(vmem_limit_bytes=62 * 2**20)

    share = pl.pallas_call(
        functools.partial(pack_kernel, passage_local),
        out_shape=shape((groups, tokens + aux_rows, feature), jnp.bfloat16),
        in_specs=vmem(5),
        out_specs=pl.BlockSpec(memory_space=VMEM),
        scratch_shapes=[VMEM((aux_rows, feature), jnp.float32)],
        name="pack",
        compiler_params=params,
    )(queries.reshape(tokens, feature), cand_ids, owner_map, teacher, weights.T)
    arrived = lax.all_to_all(share, "grp", split_axis=0, concat_axis=0, tiled=True)

    chunk = math.gcd(passage_local, 16)
    rows = pl.pallas_call(
        prepare_kernel,
        grid=(passage_local // chunk,),
        out_shape=shape((passage_local, padded, feature), jnp.bfloat16),
        in_specs=[pl.BlockSpec((token_len, chunk, feature), lambda i: (0, i, 0))],
        out_specs=pl.BlockSpec((chunk, padded, feature), lambda i: (i, 0, 0)),
        scratch_shapes=[VMEM((chunk * pitch, feature), jnp.float32)],
        name="prepare",
        compiler_params=params,
    )(passages[:, 0].transpose(1, 0, 2))

    dims = (tokens, query_local, candidates, per_tile)
    scores, highest, summed, weight_sum, block_row, block_tile, block_count, powers = (
        pl.pallas_call(
            functools.partial(score_kernel, dims, "grp"),
            out_shape=(
                shape((groups, score_rows, 128), jnp.float32),
                shape((tiles, slots, lanes), jnp.float32),
                shape((tiles, slots, lanes), jnp.float32),
                shape((1, 128), jnp.float32),
                shape((1, blocks), jnp.int32),
                shape((1, blocks), jnp.int32),
                shape((1, 1), jnp.int32),
                shape((chunks * 2 * UNROLL, padded, lanes), jnp.bfloat16),
            ),
            in_specs=vmem(1) + smem(1) + hbm(1),
            out_specs=tuple(vmem(4) + smem(3) + hbm(1)),
            scratch_shapes=[
                VMEM((passage_local, padded, feature), jnp.bfloat16),
                VMEM((tiles, feature, lanes), jnp.bfloat16),
                VMEM((passage_local, 128), jnp.int32),
                SMEM((passage_local, 128), jnp.int32),
                VMEM((2 * padded, lanes), jnp.float32),
                VMEM((UNROLL, padded, lanes), jnp.float32),
                VMEM((UNROLL, padded, lanes), jnp.float32),
                VMEM((UNROLL, lanes), jnp.float32),
                VMEM((UNROLL, lanes), jnp.float32),
                VMEM((chunks * 2 * UNROLL, padded, lanes), jnp.bfloat16),
                pltpu.SemaphoreType.DMA,
                pltpu.SemaphoreType.DMA,
                pltpu.SemaphoreType.DMA((chunks,)),
            ],
            name="score",
            compiler_params=params,
        )(arrived, lengths.T, rows)
    )
    all_scores = lax.all_to_all(scores, "grp", split_axis=0, concat_axis=0, tiled=True)
    weight_sums = from_replicas(weight_sum, replicas)

    query_total = query_local * groups * replicas
    grads, multiplier, numerator, weight_sum = pl.pallas_call(
        functools.partial(query_kernel, dims + (query_total, replicas), "grp"),
        out_shape=(
            shape((groups, tokens, feature), jnp.bfloat16),
            shape((tiles, slots, lanes), jnp.float32),
            shape((1, 128), jnp.float32),
            shape((1, 128), jnp.float32),
        ),
        in_specs=vmem(3 + replicas) + smem(3) + hbm(2),
        out_specs=tuple(vmem(4)),
        scratch_shapes=[
            VMEM(rows.shape, jnp.bfloat16),
            VMEM(powers.shape, jnp.bfloat16),
            VMEM((tiles, feature, lanes), jnp.float32),
            pltpu.SemaphoreType.DMA,
            pltpu.SemaphoreType.DMA((chunks,)),
        ],
        name="query_grad",
        compiler_params=params,
    )(arrived, all_scores, summed, *weight_sums, block_row, block_tile, block_count, rows, powers)
    returned = lax.all_to_all(grads, "grp", split_axis=0, concat_axis=0, tiled=True)

    passage_grad = pl.pallas_call(
        functools.partial(passage_kernel, (tokens, per_tile // query_local)),
        out_shape=shape((token_len, passage_local, feature), jnp.bfloat16),
        in_specs=vmem(2) + smem(3) + hbm(1),
        out_specs=pl.BlockSpec(memory_space=VMEM),
        scratch_shapes=[
            VMEM(powers.shape, jnp.bfloat16),
            VMEM(((passage_local + 1) * pitch, feature), jnp.float32),
            VMEM((tiles, lanes, feature), jnp.bfloat16),
            pltpu.SemaphoreType.DMA((chunks,)),
        ],
        name="passage_grad",
        compiler_params=params,
        cost_estimate=pl.CostEstimate(
            flops=2 * limit * padded * lanes * feature,
            bytes_accessed=2 * limit * padded * lanes,
            transcendentals=0,
        ),
    )(arrived, multiplier, block_row, block_tile, block_count, powers)
    numerators = from_replicas(numerator, replicas)

    loss = pair_sums(numerators)[0, 0] / weight_sum[0, 0]
    query_grad = jnp.sum(returned.astype(jnp.float32), axis=0)
    query_grad = query_grad.reshape(query_local, 1, query_len, feature)
    return (loss, query_grad, passage_grad.transpose(1, 0, 2)[:, None])


def solution(mesh):
    return jax.shard_map(
        on_device,
        mesh=mesh,
        in_specs=(
            P("grp", "rep", None, None),
            P("grp", "rep", None, None),
            P("grp", "rep"),
            P("grp", "rep", None),
            P("rep", None),
            P("grp", "rep", None),
            P("grp", "rep"),
        ),
        out_specs=(P(), P("grp", "rep", None, None), P("grp", "rep", None, None)),
        check_vma=False,
    )
```

```python
import functools
import math

import jax
import jax.numpy as jnp
from jax import lax
from jax.experimental import pallas as pl
from jax.experimental.pallas import tpu as pltpu
from jax.sharding import PartitionSpec as P


TEMPER = 0.05
LOG2E = math.log2(math.e)
MASKED = -1e30
KINDS = 8
UNROLL = 8
SPREAD = 4
STORE = 5
PIECES = 4
HIGHEST = lax.Precision.HIGHEST
VMEM = pltpu.VMEM
SMEM = pltpu.SMEM


def round_up(value, multiple):
    return -(-value // multiple) * multiple


def iota(shape, dim):
    return lax.broadcasted_iota(jnp.int32, shape, dim)


def three_parts(values):
    first = values.astype(jnp.bfloat16).astype(jnp.float32)
    rest = values - first
    second = rest.astype(jnp.bfloat16).astype(jnp.float32)
    third = (rest - second).astype(jnp.bfloat16).astype(jnp.float32)
    return first, second, third


def pack_kernel(passage_local, queries, cand_ids, owner_map, teacher, weights, out, aux):
    groups = out.shape[0]
    tokens = queries.shape[0]
    query_local, _, candidates = cand_ids.shape
    entries = owner_map.shape[1]
    table = owner_map[...].astype(jnp.float32)
    owner = jnp.floor((table + 0.5) * (1.0 / passage_local))
    local = table - owner * passage_local
    which = iota((8, entries), 0)
    tables = jnp.where(which == 0, owner, jnp.where(which == 1, local, 0.0)).astype(jnp.bfloat16)
    aux[...] = jnp.zeros_like(aux)
    for q in range(query_local):
        hot = (iota((entries, candidates), 0) == cand_ids[q]).astype(jnp.bfloat16)
        found = jnp.dot(tables, hot, preferred_element_type=jnp.float32)
        scores = teacher[q]
        shifted = scores - jnp.max(scores, axis=1, keepdims=True)
        log_teacher = shifted - jnp.log(jnp.sum(jnp.exp(shifted), axis=1, keepdims=True))
        weight = jnp.broadcast_to(weights[:, q : q + 1], (1, candidates))
        rows = (found[0:1], found[1:2], *three_parts(log_teacher), *three_parts(weight))
        for kind, row in enumerate(rows):
            at = kind * query_local + q
            aux[at : at + 1, 0:candidates] = row
    packed = aux[...].astype(jnp.bfloat16)
    for g in range(groups):
        out[g, 0:tokens, :] = queries[...]
        out[g, tokens:, :] = packed


def owned_rows(arrived, tokens, query_local, candidates, g, q, me):
    at = tokens + q
    owner = arrived[g, at : at + 1, 0:candidates].astype(jnp.float32)
    at = tokens + query_local + q
    local = arrived[g, at : at + 1, 0:candidates].astype(jnp.float32)
    return jnp.where(owner == me.astype(jnp.float32), local, -1.0).astype(jnp.int32)


def prepare_kernel(stored, rows_out, gathered):
    token_len, chunk, feature = stored.shape
    padded = rows_out.shape[1]
    pitch = gathered.shape[0] // chunk
    for p in range(chunk):
        at = p * pitch + token_len
        gathered[at : (p + 1) * pitch, :] = jnp.zeros((pitch - token_len, feature), jnp.float32)

    def spread(j, carry):
        for u in range(SPREAD):
            at = j * SPREAD + u
            gathered[pl.ds(at, chunk, stride=pitch), :] = stored[at].astype(jnp.float32)
        return carry

    lax.fori_loop(0, token_len // SPREAD, spread, 0)
    for j in range(token_len - token_len % SPREAD, token_len):
        gathered[pl.ds(j, chunk, stride=pitch), :] = stored[j].astype(jnp.float32)

    for p in range(chunk):
        rows_out[p] = gathered[p * pitch : p * pitch + padded, :].astype(jnp.bfloat16)


def list_blocks(flags_scalar, block_code, block_count, passage_count, tiles):
    base = code_base(tiles)
    ahead = math.gcd(passage_count, 4)

    def list_passages(step, count):
        for inner in range(ahead):
            p = step * ahead + inner
            for tile in range(tiles):
                block_code[0, count] = p * base + tile
                count = count + flags_scalar[p, tile]
        return count

    count = lax.fori_loop(0, passage_count // ahead, list_passages, jnp.int32(0))
    for extra in range(3 * UNROLL):
        block_code[0, count + extra] = passage_count * base
    steps = (count + 2 * UNROLL - 1) // (2 * UNROLL)
    block_count[0, 0] = steps
    return steps


def code_base(tiles):
    return 1 << (tiles - 1).bit_length()


def decode(block_code, block, tiles):
    code = block_code[0, block]
    base = code_base(tiles)
    return code >> (base.bit_length() - 1), code & (base - 1)


def score_kernel(
    dims,
    axis,
    arrived,
    lengths,
    *refs,
):
    tokens, query_local, candidates, per_tile, replicas = dims
    weights, refs = refs[:replicas], refs[replicas:]
    passages_hbm, scores_out, summed, block_code, block_count, powers_hbm, *scratch = refs
    score_body(
        (tokens, query_local, candidates, per_tile),
        lax.axis_index(axis),
        arrived,
        lengths,
        pair_sums([one[...] for one in weights]),
        passages_hbm,
        scores_out,
        summed,
        block_code,
        block_count,
        powers_hbm,
        *scratch,
    )


def score_body(
    dims,
    me,
    arrived,
    lengths,
    weights,
    passages_hbm,
    scores_out,
    summed,
    block_code,
    block_count,
    powers_hbm,
    highest,
    passages,
    turned,
    flags,
    flags_scalar,
    penalty,
    even,
    odd,
    even_top,
    odd_top,
    powers,
    flags_done,
    rows_done,
    powers_done,
):
    tokens, query_local, candidates, per_tile = dims
    groups = arrived.shape[0]
    passage_count, padded, _ = passages.shape
    tiles, _, lanes = highest.shape
    groups_per_tile = per_tile // query_local
    fetch_rows = pltpu.make_async_copy(passages_hbm, passages, rows_done)
    fetch_rows.start()

    column = iota(flags.shape, 1)
    passage_index = iota((passage_count, candidates), 0)
    marks = jnp.zeros(flags.shape, jnp.int32)
    for tile in range(tiles):
        hit = jnp.zeros((passage_count, candidates), jnp.int32)
        for g in range(tile * groups_per_tile, (tile + 1) * groups_per_tile):
            for q in range(query_local):
                mine = owned_rows(arrived, tokens, query_local, candidates, g, q, me)
                hit = jnp.where(passage_index == mine, 1, hit)
        any_hit = jnp.max(hit, axis=1, keepdims=True)
        marks = jnp.where(column == tile, any_hit, marks)
    flags[...] = marks
    to_scalar = pltpu.make_async_copy(flags, flags_scalar, flags_done)
    to_scalar.start()

    for tile in range(tiles):
        parts = [
            arrived[g, 0:tokens, :]
            for g in range(tile * groups_per_tile, (tile + 1) * groups_per_tile)
        ]
        block = jnp.concatenate(parts, axis=0).astype(jnp.float32)
        turned[tile] = block.T.astype(jnp.bfloat16)
    highest[...] = jnp.zeros_like(highest)
    summed[...] = jnp.ones_like(summed)
    penalty[...] = jnp.where(iota(penalty.shape, 0) < padded, 0.0, MASKED)
    to_scalar.wait()
    steps = list_blocks(flags_scalar, block_code, block_count, passage_count, tiles)
    fetch_rows.wait()

    factor = LOG2E / TEMPER

    def multiply(first, into, tops):
        for u in range(UNROLL):
            slot, tile = decode(block_code, first + u, tiles)
            p = jnp.minimum(slot, passage_count - 1)
            products = jnp.dot(passages[p], turned[tile], preferred_element_type=jnp.float32)
            products = products + penalty[pl.ds(padded - lengths[0, p], padded), :]
            into[u] = products
            tops[u : u + 1, :] = jnp.max(products, axis=0, keepdims=True)

    def soften(first, held, tops):
        for u in range(UNROLL):
            slot, tile = decode(block_code, first + u, tiles)
            top = tops[u : u + 1, :]
            raised = jnp.exp2((held[u] - top) * factor)
            powers[first + u] = raised.astype(jnp.bfloat16)
            highest[tile, pl.ds(slot, 1), :] = top
            summed[tile, pl.ds(slot, 1), :] = jnp.sum(raised, axis=0, keepdims=True)

    def chunk_copy(s):
        at = pl.ds(s * 2 * UNROLL, 2 * UNROLL)
        return pltpu.make_async_copy(powers.at[at], powers_hbm.at[at], powers_done.at[s])

    multiply(0, even, even_top)

    def step(s, carry):
        first = s * 2 * UNROLL
        multiply(first + UNROLL, odd, odd_top)
        soften(first, even, even_top)
        multiply(first + 2 * UNROLL, even, even_top)
        soften(first + UNROLL, odd, odd_top)
        chunk_copy(s).start()
        return carry

    lax.fori_loop(0, steps, step, 0)

    query_len = lanes // per_tile
    member = iota((lanes, 128), 0) // query_len == iota((lanes, 128), 1)
    member = member.astype(jnp.float32)
    weight_part = jnp.sum(weights, axis=1, keepdims=True)
    scores_out[0] = jnp.broadcast_to(weight_part, scores_out.shape[1:])
    for tile in range(tiles):
        matched = highest[tile, 0:passage_count, :] + TEMPER * jnp.log(
            summed[tile, 0:passage_count, :]
        )
        sums = jnp.dot(matched, member, precision=HIGHEST, preferred_element_type=jnp.float32)
        for inner in range(per_tile):
            g = tile * groups_per_tile + inner // query_local
            q = inner % query_local
            mine = owned_rows(arrived, tokens, query_local, candidates, g, q, me)
            picked = jnp.where(passage_index == mine, sums[:, inner : inner + 1], 0.0)
            at = tile * per_tile + inner
            scores_out[0, at : at + 1, 0:candidates] = jnp.sum(picked, axis=0, keepdims=True)
    for g in range(1, groups):
        scores_out[g] = scores_out[0]

    def finish(s, carry):
        chunk_copy(s).wait()
        return carry

    lax.fori_loop(0, steps, finish, 0)


def pair_sums(values):
    while len(values) > 1:
        values = [values[i] + values[i + 1] for i in range(0, len(values), 2)]
    return values[0]


def query_kernel(
    dims,
    axis,
    arrived,
    scores,
    summed,
    block_code,
    block_count,
    passages_hbm,
    powers_hbm,
    grads_out,
    multiplier,
    numerator_out,
    weight_sum_out,
    passages,
    powers,
    sums,
    rows_done,
    powers_done,
):
    tokens, query_local, candidates, per_tile, query_total = dims
    groups = arrived.shape[0]
    tiles, slots, lanes = summed.shape
    passage_count, _, _ = passages.shape
    groups_per_tile = per_tile // query_local
    queries_all = tiles * per_tile
    query_len = lanes // per_tile
    me = lax.axis_index(axis)
    steps = block_count[0, 0]

    fetch_rows = pltpu.make_async_copy(passages_hbm, passages, rows_done)
    fetch_rows.start()

    def chunk_copy(s):
        at = pl.ds(s * 2 * UNROLL, 2 * UNROLL)
        return pltpu.make_async_copy(powers_hbm.at[at], powers.at[at], powers_done.at[s])

    def fetch(s, carry):
        chunk_copy(s).start()
        return carry

    lax.fori_loop(0, steps, fetch, 0)

    got = scores[0]
    for g in range(1, groups):
        got = got + scores[g]
    student = got[0:queries_all, 0:candidates]

    def gather_parts(kind):
        rows = []
        for g in range(groups):
            parts = []
            for part in range(3):
                at = tokens + (kind + part) * query_local
                block = arrived[g, at : at + query_local, 0:candidates]
                parts.append(block.astype(jnp.float32))
            rows.append((parts[0] + parts[1]) + parts[2])
        return jnp.concatenate(rows, axis=0)

    log_teacher = gather_parts(2)
    weight = gather_parts(5)
    shifted = student - jnp.max(student, axis=1, keepdims=True)
    log_student = shifted - jnp.log(jnp.sum(jnp.exp(shifted), axis=1, keepdims=True))
    teacher_prob = jnp.exp(log_teacher)
    spread = jnp.sum(weight * teacher_prob * (log_teacher - log_student), axis=1, keepdims=True)
    numerator = jnp.sum(spread, axis=0, keepdims=True)
    numerator_out[...] = jnp.broadcast_to(numerator, numerator_out.shape)
    weight_sum = got[0:1, candidates : candidates + 1]
    weight_sum_out[...] = jnp.broadcast_to(weight_sum, weight_sum_out.shape)
    scale = query_total / weight_sum
    grad = (weight * scale) * (jnp.exp(log_student) - teacher_prob)

    passage_index = iota((passage_count, candidates), 0)
    lane_query = iota((passage_count, lanes), 1) // query_len
    for tile in range(tiles):
        spread_out = jnp.zeros((passage_count, lanes), jnp.float32)
        for inner in range(per_tile):
            g = tile * groups_per_tile + inner // query_local
            q = inner % query_local
            mine = owned_rows(arrived, tokens, query_local, candidates, g, q, me)
            at = tile * per_tile + inner
            picked = jnp.where(passage_index == mine, grad[at : at + 1], 0.0)
            total = jnp.sum(picked, axis=1, keepdims=True)
            spread_out = jnp.where(lane_query == inner, total, spread_out)
        multiplier[tile, 0:passage_count, :] = spread_out / summed[tile, 0:passage_count, :]
        multiplier[tile, passage_count:, :] = jnp.zeros((slots - passage_count, lanes), jnp.float32)

    sums[...] = jnp.zeros_like(sums)
    fetch_rows.wait()

    def step(s, carry):
        chunk_copy(s).wait()
        for u in range(2 * UNROLL):
            b = s * 2 * UNROLL + u
            slot, tile = decode(block_code, b, tiles)
            p = jnp.minimum(slot, passage_count - 1)
            part = powers[b].astype(jnp.float32) * multiplier[tile, pl.ds(slot, 1), :]
            part = part.astype(jnp.bfloat16)
            sums[tile] += lax.dot_general(
                passages[p], part, (((0,), (0,)), ((), ())), preferred_element_type=jnp.float32
            )
        return carry

    lax.fori_loop(0, steps, step, 0)
    for tile in range(tiles):
        back = sums[tile].T.astype(jnp.bfloat16)
        for inner in range(groups_per_tile):
            g = tile * groups_per_tile + inner
            grads_out[g] = back[inner * tokens : (inner + 1) * tokens]


def passage_kernel(
    dims,
    arrived,
    multiplier,
    block_code,
    block_count,
    powers_hbm,
    out_hbm,
    out,
    powers,
    sums,
    queries_all,
    powers_done,
    out_done,
):
    tokens, per_tile_groups = dims
    token_len, passage_count, feature = out.shape
    tiles = queries_all.shape[0]
    padded = powers.shape[1]
    pitch = sums.shape[0] // (passage_count + 1)
    steps = block_count[0, 0]

    def chunk_copy(s):
        at = pl.ds(s * 2 * UNROLL, 2 * UNROLL)
        return pltpu.make_async_copy(powers_hbm.at[at], powers.at[at], powers_done.at[s])

    def fetch(s, carry):
        chunk_copy(s).start()
        return carry

    lax.fori_loop(0, steps, fetch, 0)
    for tile in range(tiles):
        for inner in range(per_tile_groups):
            g = tile * per_tile_groups + inner
            queries_all[tile, inner * tokens : (inner + 1) * tokens, :] = arrived[g, 0:tokens, :]

    def clear(p, carry):
        sums[pl.ds(p * pitch, pitch), :] = jnp.zeros((pitch, feature), jnp.float32)
        return carry

    lax.fori_loop(0, passage_count, clear, 0)

    def step(s, carry):
        chunk_copy(s).wait()
        for u in range(2 * UNROLL):
            b = s * 2 * UNROLL + u
            slot, tile = decode(block_code, b, tiles)
            part = powers[b].astype(jnp.float32) * multiplier[tile, pl.ds(slot, 1), :]
            at = pl.ds(slot * pitch, padded)
            sums[at, :] += jnp.dot(
                part.astype(jnp.bfloat16), queries_all[tile], preferred_element_type=jnp.float32
            )
        return carry

    lax.fori_loop(0, steps, step, 0)

    pieces = out_done.shape[0]
    piece = token_len // pieces
    copies = []
    for k in range(pieces):
        first = k * piece
        last = token_len if k == pieces - 1 else first + piece

        def store(j, carry, first=first):
            for u in range(STORE):
                at = first + j * STORE + u
                out[at] = sums[pl.ds(at, passage_count, stride=pitch), :].astype(out.dtype)
            return carry

        whole = (last - first) // STORE
        lax.fori_loop(0, whole, store, 0)
        for at in range(first + whole * STORE, last):
            out[at] = sums[pl.ds(at, passage_count, stride=pitch), :].astype(out.dtype)
        rows = pl.ds(first, last - first)
        copies.append(pltpu.make_async_copy(out.at[rows], out_hbm.at[rows], out_done.at[k]))
        copies[-1].start()
    for copy in copies:
        copy.wait()


def vmem(count):
    return [pl.BlockSpec(memory_space=VMEM)] * count


def smem(count):
    return [pl.BlockSpec(memory_space=SMEM)] * count


def from_replicas(values, replicas):
    rings = [[(r, r ^ hop) for r in range(replicas)] for hop in range(1, replicas)]
    return [values] + [lax.ppermute(values, "rep", ring) for ring in rings]


def hbm(count):
    return [pl.BlockSpec(memory_space=pltpu.HBM)] * count


def on_device(queries, passages, lengths, cand_ids, owner_map, teacher, weights):
    groups = lax.axis_size("grp")
    replicas = lax.axis_size("rep")
    query_local, _, query_len, feature = queries.shape
    passage_local, _, token_len, _ = passages.shape
    candidates = cand_ids.shape[2]
    tokens = query_local * query_len
    lanes = 128
    per_tile = lanes // query_len
    tiles = groups * tokens // lanes
    padded = round_up(token_len, 16)
    pitch = padded + 9
    ref_count = query_local * candidates
    capacity = groups * (2 * ref_count // groups)
    limit = min(passage_local * tiles, capacity)
    blocks = limit + 3 * UNROLL
    chunks = -(-limit // (2 * UNROLL))
    aux_rows = round_up(KINDS * query_local, 16)
    slots = round_up(passage_local + 1, 8)
    score_rows = round_up(groups * query_local, 8)
    shape = jax.ShapeDtypeStruct
    alone = pltpu.CompilerParams(vmem_limit_bytes=62 * 2**20)
    params = pltpu.CompilerParams(vmem_limit_bytes=52 * 2**20)

    share = pl.pallas_call(
        functools.partial(pack_kernel, passage_local),
        out_shape=shape((groups, tokens + aux_rows, feature), jnp.bfloat16),
        in_specs=vmem(5),
        out_specs=pl.BlockSpec(memory_space=VMEM),
        scratch_shapes=[VMEM((aux_rows, feature), jnp.float32)],
        name="pack",
        compiler_params=alone,
    )(queries.reshape(tokens, feature), cand_ids, owner_map, teacher, weights.T)
    arrived = lax.all_to_all(share, "grp", split_axis=0, concat_axis=0, tiled=True)

    replica_weights = from_replicas(weights.T, replicas)

    chunk = math.gcd(passage_local, 16)
    rows = pl.pallas_call(
        prepare_kernel,
        grid=(passage_local // chunk,),
        out_shape=shape((passage_local, padded, feature), jnp.bfloat16),
        in_specs=[pl.BlockSpec((token_len, chunk, feature), lambda i: (0, i, 0))],
        out_specs=pl.BlockSpec((chunk, padded, feature), lambda i: (i, 0, 0)),
        scratch_shapes=[VMEM((chunk * pitch, feature), jnp.float32)],
        name="prepare",
        compiler_params=params,
    )(passages[:, 0].transpose(1, 0, 2))

    dims = (tokens, query_local, candidates, per_tile)
    scores, summed, block_code, block_count, powers = (
        pl.pallas_call(
            functools.partial(score_kernel, dims + (replicas,), "grp"),
            out_shape=(
                shape((groups, score_rows, 128), jnp.float32),
                shape((tiles, slots, lanes), jnp.float32),
                shape((1, blocks), jnp.int32),
                shape((1, 1), jnp.int32),
                shape((chunks * 2 * UNROLL, padded, lanes), jnp.bfloat16),
            ),
            in_specs=vmem(1) + smem(1) + vmem(replicas) + hbm(1),
            out_specs=tuple(vmem(2) + smem(2) + hbm(1)),
            scratch_shapes=[
                VMEM((tiles, slots, lanes), jnp.float32),
                VMEM((passage_local, padded, feature), jnp.bfloat16),
                VMEM((tiles, feature, lanes), jnp.bfloat16),
                VMEM((passage_local, 128), jnp.int32),
                SMEM((passage_local, 128), jnp.int32),
                VMEM((2 * padded, lanes), jnp.float32),
                VMEM((UNROLL, padded, lanes), jnp.float32),
                VMEM((UNROLL, padded, lanes), jnp.float32),
                VMEM((UNROLL, lanes), jnp.float32),
                VMEM((UNROLL, lanes), jnp.float32),
                VMEM((chunks * 2 * UNROLL, padded, lanes), jnp.bfloat16),
                pltpu.SemaphoreType.DMA,
                pltpu.SemaphoreType.DMA,
                pltpu.SemaphoreType.DMA((chunks,)),
            ],
            name="score",
            compiler_params=params,
        )(arrived, lengths.T, *replica_weights, rows)
    )
    all_scores = lax.all_to_all(scores, "grp", split_axis=0, concat_axis=0, tiled=True)

    query_total = query_local * groups * replicas
    grads, multiplier, numerator, weight_sum = pl.pallas_call(
        functools.partial(query_kernel, dims + (query_total,), "grp"),
        out_shape=(
            shape((groups, tokens, feature), jnp.bfloat16),
            shape((tiles, slots, lanes), jnp.float32),
            shape((1, 128), jnp.float32),
            shape((1, 128), jnp.float32),
        ),
        in_specs=vmem(3) + smem(2) + hbm(2),
        out_specs=tuple(vmem(4)),
        scratch_shapes=[
            VMEM(rows.shape, jnp.bfloat16),
            VMEM(powers.shape, jnp.bfloat16),
            VMEM((tiles, feature, lanes), jnp.float32),
            pltpu.SemaphoreType.DMA,
            pltpu.SemaphoreType.DMA((chunks,)),
        ],
        name="query_grad",
        compiler_params=params,
    )(arrived, all_scores, summed, block_code, block_count, rows, powers)
    returned = lax.all_to_all(grads, "grp", split_axis=0, concat_axis=0, tiled=True)

    passage_grad = pl.pallas_call(
        functools.partial(passage_kernel, (tokens, per_tile // query_local)),
        out_shape=shape((token_len, passage_local, feature), jnp.bfloat16),
        in_specs=vmem(2) + smem(2) + hbm(1),
        out_specs=pl.BlockSpec(memory_space=pltpu.HBM),
        scratch_shapes=[
            VMEM((token_len, passage_local, feature), jnp.bfloat16),
            VMEM(powers.shape, jnp.bfloat16),
            VMEM(((passage_local + 1) * pitch, feature), jnp.float32),
            VMEM((tiles, lanes, feature), jnp.bfloat16),
            pltpu.SemaphoreType.DMA((chunks,)),
            pltpu.SemaphoreType.DMA((PIECES,)),
        ],
        name="passage_grad",
        compiler_params=params,
        cost_estimate=pl.CostEstimate(
            flops=2 * limit * padded * lanes * feature,
            bytes_accessed=2 * limit * padded * lanes,
            transcendentals=0,
        ),
    )(arrived, multiplier, block_code, block_count, powers)
    numerators = from_replicas(numerator, replicas)

    loss = pair_sums(numerators)[0, 0] / weight_sum[0, 0]
    query_grad = jnp.sum(returned.astype(jnp.float32), axis=0)
    query_grad = query_grad.reshape(query_local, 1, query_len, feature)
    return (loss, query_grad, passage_grad.transpose(1, 0, 2)[:, None])


def solution(mesh):
    return jax.shard_map(
        on_device,
        mesh=mesh,
        in_specs=(
            P("grp", "rep", None, None),
            P("grp", "rep", None, None),
            P("grp", "rep"),
            P("grp", "rep", None),
            P("rep", None),
            P("grp", "rep", None),
            P("grp", "rep"),
        ),
        out_specs=(P(), P("grp", "rep", None, None), P("grp", "rep", None, None)),
        check_vma=False,
    )
```

```python
import functools
import math

import jax
import jax.numpy as jnp
from jax import lax
from jax.experimental import pallas as pl
from jax.experimental.pallas import tpu as pltpu
from jax.sharding import PartitionSpec as P


TEMPER = 0.05
LOG2E = math.log2(math.e)
MASKED = -1e30
KINDS = 8
UNROLL = 8
SPREAD = 4
SUMS = 4
STORE = 5
PIECES = 4
HIGHEST = lax.Precision.HIGHEST
VMEM = pltpu.VMEM
SMEM = pltpu.SMEM


def round_up(value, multiple):
    return -(-value // multiple) * multiple


def iota(shape, dim):
    return lax.broadcasted_iota(jnp.int32, shape, dim)


def three_parts(values):
    first = values.astype(jnp.bfloat16).astype(jnp.float32)
    rest = values - first
    second = rest.astype(jnp.bfloat16).astype(jnp.float32)
    third = (rest - second).astype(jnp.bfloat16).astype(jnp.float32)
    return first, second, third


def pack_kernel(passage_local, queries, cand_ids, owner_map, teacher, weights, out, aux):
    groups = out.shape[0]
    tokens = queries.shape[0]
    query_local, _, candidates = cand_ids.shape
    entries = owner_map.shape[1]
    table = owner_map[...].astype(jnp.float32)
    owner = jnp.floor((table + 0.5) * (1.0 / passage_local))
    local = table - owner * passage_local
    which = iota((8, entries), 0)
    tables = jnp.where(which == 0, owner, jnp.where(which == 1, local, 0.0)).astype(jnp.bfloat16)
    aux[...] = jnp.zeros_like(aux)
    for q in range(query_local):
        hot = (iota((entries, candidates), 0) == cand_ids[q]).astype(jnp.bfloat16)
        found = jnp.dot(tables, hot, preferred_element_type=jnp.float32)
        scores = teacher[q]
        shifted = scores - jnp.max(scores, axis=1, keepdims=True)
        log_teacher = shifted - jnp.log(jnp.sum(jnp.exp(shifted), axis=1, keepdims=True))
        weight = jnp.broadcast_to(weights[:, q : q + 1], (1, candidates))
        rows = (found[0:1], found[1:2], *three_parts(log_teacher), *three_parts(weight))
        for kind, row in enumerate(rows):
            at = kind * query_local + q
            aux[at : at + 1, 0:candidates] = row
    packed = aux[...].astype(jnp.bfloat16)
    for g in range(groups):
        out[g, 0:tokens, :] = queries[...]
        out[g, tokens:, :] = packed


def owned_rows(arrived, tokens, query_local, candidates, g, q, me):
    at = tokens + q
    owner = arrived[g, at : at + 1, 0:candidates].astype(jnp.float32)
    at = tokens + query_local + q
    local = arrived[g, at : at + 1, 0:candidates].astype(jnp.float32)
    return jnp.where(owner == me.astype(jnp.float32), local, -1.0).astype(jnp.int32)


def prepare_kernel(stored, rows_out, turned_out, gathered):
    token_len, chunk, feature = stored.shape
    padded = rows_out.shape[1]
    pitch = gathered.shape[0] // chunk

    def clear(p, carry):
        at = pl.ds(p * pitch + token_len, padded - token_len)
        gathered[at, :] = jnp.zeros((padded - token_len, feature), jnp.float32)
        return carry

    lax.fori_loop(0, chunk, clear, 0)

    def spread(j, carry):
        for u in range(SPREAD):
            at = j * SPREAD + u
            gathered[pl.ds(at, chunk, stride=pitch), :] = stored[at].astype(jnp.float32)
        return carry

    lax.fori_loop(0, token_len // SPREAD, spread, 0)
    for j in range(token_len - token_len % SPREAD, token_len):
        gathered[pl.ds(j, chunk, stride=pitch), :] = stored[j].astype(jnp.float32)

    ahead = math.gcd(chunk, 8)

    def collect(step, carry):
        for inner in range(ahead):
            p = step * ahead + inner
            block = gathered[pl.ds(p * pitch, padded), :].astype(jnp.bfloat16)
            rows_out[p] = block
            turned_out[p, :, 0:padded] = block.T
        return carry

    lax.fori_loop(0, chunk // ahead, collect, 0)


def list_blocks(flags_scalar, block_code, block_count, passage_count, tiles):
    base = code_base(tiles)
    ahead = math.gcd(passage_count, 4)

    def list_passages(step, count):
        for inner in range(ahead):
            p = step * ahead + inner
            for tile in range(tiles):
                block_code[0, count] = p * base + tile
                count = count + flags_scalar[p, tile]
        return count

    count = lax.fori_loop(0, passage_count // ahead, list_passages, jnp.int32(0))
    for extra in range(3 * UNROLL):
        block_code[0, count + extra] = passage_count * base
    steps = (count + 2 * UNROLL - 1) // (2 * UNROLL)
    block_count[0, 0] = steps
    return steps


def code_base(tiles):
    return 1 << (tiles - 1).bit_length()


def decode(block_code, block, tiles):
    code = block_code[0, block]
    base = code_base(tiles)
    return code >> (base.bit_length() - 1), code & (base - 1)


def score_kernel(
    dims,
    axis,
    arrived,
    lengths,
    *refs,
):
    tokens, query_local, candidates, per_tile, replicas = dims
    weights, refs = refs[:replicas], refs[replicas:]
    passages, scores_out, summed, block_code, block_count, powers_hbm, *scratch = refs
    score_body(
        (tokens, query_local, candidates, per_tile),
        lax.axis_index(axis),
        arrived,
        lengths,
        pair_sums([one[...] for one in weights]),
        passages,
        scores_out,
        summed,
        block_code,
        block_count,
        powers_hbm,
        *scratch,
    )


def score_body(
    dims,
    me,
    arrived,
    lengths,
    weights,
    passages,
    scores_out,
    summed,
    block_code,
    block_count,
    powers_hbm,
    highest,
    turned,
    flags,
    flags_scalar,
    penalty,
    even,
    odd,
    even_top,
    odd_top,
    powers,
    flags_done,
    powers_done,
):
    tokens, query_local, candidates, per_tile = dims
    groups = arrived.shape[0]
    passage_count, padded, _ = passages.shape
    tiles, _, lanes = highest.shape
    groups_per_tile = per_tile // query_local

    column = iota(flags.shape, 1)
    passage_index = iota((passage_count, candidates), 0)
    marks = jnp.zeros(flags.shape, jnp.int32)
    for tile in range(tiles):
        hit = jnp.zeros((passage_count, candidates), jnp.int32)
        for g in range(tile * groups_per_tile, (tile + 1) * groups_per_tile):
            for q in range(query_local):
                mine = owned_rows(arrived, tokens, query_local, candidates, g, q, me)
                hit = jnp.where(passage_index == mine, 1, hit)
        any_hit = jnp.max(hit, axis=1, keepdims=True)
        marks = jnp.where(column == tile, any_hit, marks)
    flags[...] = marks
    to_scalar = pltpu.make_async_copy(flags, flags_scalar, flags_done)
    to_scalar.start()

    for tile in range(tiles):
        parts = [
            arrived[g, 0:tokens, :]
            for g in range(tile * groups_per_tile, (tile + 1) * groups_per_tile)
        ]
        block = jnp.concatenate(parts, axis=0).astype(jnp.float32)
        turned[tile] = block.T.astype(jnp.bfloat16)
    highest[...] = jnp.zeros_like(highest)
    summed[...] = jnp.ones_like(summed)
    penalty[...] = jnp.where(iota(penalty.shape, 0) < padded, 0.0, MASKED)
    to_scalar.wait()
    steps = list_blocks(flags_scalar, block_code, block_count, passage_count, tiles)

    factor = LOG2E / TEMPER

    def multiply(first, into, tops):
        for u in range(UNROLL):
            slot, tile = decode(block_code, first + u, tiles)
            p = jnp.minimum(slot, passage_count - 1)
            products = jnp.dot(passages[p], turned[tile], preferred_element_type=jnp.float32)
            products = products + penalty[pl.ds(padded - lengths[0, p], padded), :]
            into[u] = products
            tops[u : u + 1, :] = jnp.max(products, axis=0, keepdims=True)

    def soften(first, held, tops):
        for u in range(UNROLL):
            slot, tile = decode(block_code, first + u, tiles)
            top = tops[u : u + 1, :]
            raised = jnp.exp2((held[u] - top) * factor)
            powers[first + u] = raised.astype(jnp.bfloat16)
            highest[tile, pl.ds(slot, 1), :] = top
            summed[tile, pl.ds(slot, 1), :] = jnp.sum(raised, axis=0, keepdims=True)

    def chunk_copy(s):
        at = pl.ds(s * 2 * UNROLL, 2 * UNROLL)
        return pltpu.make_async_copy(powers.at[at], powers_hbm.at[at], powers_done.at[s])

    multiply(0, even, even_top)

    def step(s, carry):
        first = s * 2 * UNROLL
        multiply(first + UNROLL, odd, odd_top)
        soften(first, even, even_top)
        multiply(first + 2 * UNROLL, even, even_top)
        soften(first + UNROLL, odd, odd_top)
        chunk_copy(s).start()
        return carry

    lax.fori_loop(0, steps, step, 0)

    query_len = lanes // per_tile
    member = iota((lanes, 128), 0) // query_len == iota((lanes, 128), 1)
    member = member.astype(jnp.float32)
    weight_part = jnp.sum(weights, axis=1, keepdims=True)
    scores_out[0] = jnp.broadcast_to(weight_part, scores_out.shape[1:])
    for tile in range(tiles):
        matched = highest[tile, 0:passage_count, :] + TEMPER * jnp.log(
            summed[tile, 0:passage_count, :]
        )
        sums = jnp.dot(matched, member, precision=HIGHEST, preferred_element_type=jnp.float32)
        for inner in range(per_tile):
            g = tile * groups_per_tile + inner // query_local
            q = inner % query_local
            mine = owned_rows(arrived, tokens, query_local, candidates, g, q, me)
            picked = jnp.where(passage_index == mine, sums[:, inner : inner + 1], 0.0)
            at = tile * per_tile + inner
            scores_out[0, at : at + 1, 0:candidates] = jnp.sum(picked, axis=0, keepdims=True)
    for g in range(1, groups):
        scores_out[g] = scores_out[0]

    def finish(s, carry):
        chunk_copy(s).wait()
        return carry

    lax.fori_loop(0, steps, finish, 0)


def pair_sums(values):
    while len(values) > 1:
        values = [values[i] + values[i + 1] for i in range(0, len(values), 2)]
    return values[0]


def query_kernel(
    dims,
    axis,
    arrived,
    scores,
    summed,
    turned,
    block_code,
    block_count,
    powers_hbm,
    grads_out,
    multiplier,
    numerator_out,
    weight_sum_out,
    powers,
    factors,
    powers_done,
    *sums,
):
    tokens, query_local, candidates, per_tile, query_total = dims
    groups = arrived.shape[0]
    tiles, slots, lanes = summed.shape
    passage_count = turned.shape[0]
    padded = powers.shape[1]
    groups_per_tile = per_tile // query_local
    queries_all = tiles * per_tile
    query_len = lanes // per_tile
    me = lax.axis_index(axis)
    steps = block_count[0, 0]

    def chunk_copy(s):
        at = pl.ds(s * 2 * UNROLL, 2 * UNROLL)
        return pltpu.make_async_copy(powers_hbm.at[at], powers.at[at], powers_done.at[s])

    def fetch(s, carry):
        chunk_copy(s).start()
        return carry

    lax.fori_loop(0, steps, fetch, 0)

    got = scores[0]
    for g in range(1, groups):
        got = got + scores[g]
    student = got[0:queries_all, 0:candidates]

    def gather_parts(kind):
        rows = []
        for g in range(groups):
            parts = []
            for part in range(3):
                at = tokens + (kind + part) * query_local
                block = arrived[g, at : at + query_local, 0:candidates]
                parts.append(block.astype(jnp.float32))
            rows.append((parts[0] + parts[1]) + parts[2])
        return jnp.concatenate(rows, axis=0)

    log_teacher = gather_parts(2)
    weight = gather_parts(5)
    shifted = student - jnp.max(student, axis=1, keepdims=True)
    log_student = shifted - jnp.log(jnp.sum(jnp.exp(shifted), axis=1, keepdims=True))
    teacher_prob = jnp.exp(log_teacher)
    spread = jnp.sum(weight * teacher_prob * (log_teacher - log_student), axis=1, keepdims=True)
    numerator = jnp.sum(spread, axis=0, keepdims=True)
    numerator_out[...] = jnp.broadcast_to(numerator, numerator_out.shape)
    weight_sum = got[0:1, candidates : candidates + 1]
    weight_sum_out[...] = jnp.broadcast_to(weight_sum, weight_sum_out.shape)
    scale = query_total / weight_sum
    grad = (weight * scale) * (jnp.exp(log_student) - teacher_prob)

    passage_index = iota((passage_count, candidates), 0)
    lane_query = iota((passage_count, lanes), 1) // query_len
    for tile in range(tiles):
        spread_out = jnp.zeros((passage_count, lanes), jnp.float32)
        for inner in range(per_tile):
            g = tile * groups_per_tile + inner // query_local
            q = inner % query_local
            mine = owned_rows(arrived, tokens, query_local, candidates, g, q, me)
            at = tile * per_tile + inner
            picked = jnp.where(passage_index == mine, grad[at : at + 1], 0.0)
            total = jnp.sum(picked, axis=1, keepdims=True)
            spread_out = jnp.where(lane_query == inner, total, spread_out)
        factors[tile, 0:passage_count, :] = spread_out / summed[tile, 0:passage_count, :]
        factors[tile, passage_count:, :] = jnp.zeros((slots - passage_count, lanes), jnp.float32)
    multiplier[...] = factors[...]

    for one in sums:
        one[...] = jnp.zeros_like(one)

    def step(s, carry):
        chunk_copy(s).wait()
        for u in range(2 * UNROLL):
            b = s * 2 * UNROLL + u
            slot, tile = decode(block_code, b, tiles)
            p = jnp.minimum(slot, passage_count - 1)
            part = powers[b].astype(jnp.float32) * factors[tile, pl.ds(slot, 1), :]
            part = part.astype(jnp.bfloat16)
            sums[u % len(sums)][tile] += jnp.dot(
                turned[p, :, 0:padded], part, preferred_element_type=jnp.float32
            )
        return carry

    lax.fori_loop(0, steps, step, 0)
    for tile in range(tiles):
        back = pair_sums([one[tile] for one in sums]).T.astype(jnp.bfloat16)
        for inner in range(groups_per_tile):
            g = tile * groups_per_tile + inner
            grads_out[g] = back[inner * tokens : (inner + 1) * tokens]


def passage_kernel(
    dims,
    arrived,
    multiplier,
    block_code,
    block_count,
    powers_hbm,
    out_hbm,
    out,
    powers,
    sums,
    queries_all,
    powers_done,
    out_done,
):
    tokens, per_tile_groups = dims
    token_len, passage_count, feature = out.shape
    tiles = queries_all.shape[0]
    padded = powers.shape[1]
    pitch = sums.shape[0] // (passage_count + 1)
    steps = block_count[0, 0]

    def chunk_copy(s):
        at = pl.ds(s * 2 * UNROLL, 2 * UNROLL)
        return pltpu.make_async_copy(powers_hbm.at[at], powers.at[at], powers_done.at[s])

    def fetch(s, carry):
        chunk_copy(s).start()
        return carry

    lax.fori_loop(0, steps, fetch, 0)
    for tile in range(tiles):
        for inner in range(per_tile_groups):
            g = tile * per_tile_groups + inner
            queries_all[tile, inner * tokens : (inner + 1) * tokens, :] = arrived[g, 0:tokens, :]

    def clear(p, carry):
        sums[pl.ds(p * pitch, pitch), :] = jnp.zeros((pitch, feature), jnp.float32)
        return carry

    lax.fori_loop(0, passage_count, clear, 0)

    def step(s, carry):
        chunk_copy(s).wait()
        for u in range(2 * UNROLL):
            b = s * 2 * UNROLL + u
            slot, tile = decode(block_code, b, tiles)
            part = powers[b].astype(jnp.float32) * multiplier[tile, pl.ds(slot, 1), :]
            at = pl.ds(slot * pitch, padded)
            sums[at, :] += jnp.dot(
                part.astype(jnp.bfloat16), queries_all[tile], preferred_element_type=jnp.float32
            )
        return carry

    lax.fori_loop(0, steps, step, 0)

    pieces = out_done.shape[0]
    piece = token_len // pieces
    copies = []
    for k in range(pieces):
        first = k * piece
        last = token_len if k == pieces - 1 else first + piece

        def store(j, carry, first=first):
            for u in range(STORE):
                at = first + j * STORE + u
                out[at] = sums[pl.ds(at, passage_count, stride=pitch), :].astype(out.dtype)
            return carry

        whole = (last - first) // STORE
        lax.fori_loop(0, whole, store, 0)
        for at in range(first + whole * STORE, last):
            out[at] = sums[pl.ds(at, passage_count, stride=pitch), :].astype(out.dtype)
        rows = pl.ds(first, last - first)
        copies.append(pltpu.make_async_copy(out.at[rows], out_hbm.at[rows], out_done.at[k]))
        copies[-1].start()
    for copy in copies:
        copy.wait()


def vmem(count):
    return [pl.BlockSpec(memory_space=VMEM)] * count


def smem(count):
    return [pl.BlockSpec(memory_space=SMEM)] * count


def from_replicas(values, replicas):
    rings = [[(r, r ^ hop) for r in range(replicas)] for hop in range(1, replicas)]
    return [values] + [lax.ppermute(values, "rep", ring) for ring in rings]


def hbm(count):
    return [pl.BlockSpec(memory_space=pltpu.HBM)] * count


def on_device(queries, passages, lengths, cand_ids, owner_map, teacher, weights):
    groups = lax.axis_size("grp")
    replicas = lax.axis_size("rep")
    query_local, _, query_len, feature = queries.shape
    passage_local, _, token_len, _ = passages.shape
    candidates = cand_ids.shape[2]
    tokens = query_local * query_len
    lanes = 128
    per_tile = lanes // query_len
    tiles = groups * tokens // lanes
    padded = round_up(token_len, 16)
    pitch = padded + 9
    ref_count = query_local * candidates
    capacity = groups * (2 * ref_count // groups)
    limit = min(passage_local * tiles, capacity)
    blocks = limit + 3 * UNROLL
    chunks = -(-limit // (2 * UNROLL))
    aux_rows = round_up(KINDS * query_local, 16)
    slots = round_up(passage_local + 1, 8)
    score_rows = round_up(groups * query_local, 8)
    shape = jax.ShapeDtypeStruct
    alone = pltpu.CompilerParams(vmem_limit_bytes=62 * 2**20)
    params = pltpu.CompilerParams(vmem_limit_bytes=48 * 2**20)

    share = pl.pallas_call(
        functools.partial(pack_kernel, passage_local),
        out_shape=shape((groups, tokens + aux_rows, feature), jnp.bfloat16),
        in_specs=vmem(5),
        out_specs=pl.BlockSpec(memory_space=VMEM),
        scratch_shapes=[VMEM((aux_rows, feature), jnp.float32)],
        name="pack",
        compiler_params=alone,
    )(queries.reshape(tokens, feature), cand_ids, owner_map, teacher, weights.T)
    arrived = lax.all_to_all(share, "grp", split_axis=0, concat_axis=0, tiled=True)

    replica_weights = from_replicas(weights.T, replicas)

    rows, turned = pl.pallas_call(
        prepare_kernel,
        out_shape=(
            shape((passage_local, padded, feature), jnp.bfloat16),
            shape((passage_local, feature, round_up(padded, 128)), jnp.bfloat16),
        ),
        in_specs=vmem(1),
        out_specs=tuple(vmem(2)),
        scratch_shapes=[VMEM((passage_local * pitch, feature), jnp.float32)],
        name="prepare",
        compiler_params=params,
    )(passages[:, 0].transpose(1, 0, 2))

    dims = (tokens, query_local, candidates, per_tile)
    scores, summed, block_code, block_count, powers = (
        pl.pallas_call(
            functools.partial(score_kernel, dims + (replicas,), "grp"),
            out_shape=(
                shape((groups, score_rows, 128), jnp.float32),
                shape((tiles, slots, lanes), jnp.float32),
                shape((1, blocks), jnp.int32),
                shape((1, 1), jnp.int32),
                shape((chunks * 2 * UNROLL, padded, lanes), jnp.bfloat16),
            ),
            in_specs=vmem(1) + smem(1) + vmem(replicas + 1),
            out_specs=tuple(vmem(2) + smem(2) + hbm(1)),
            scratch_shapes=[
                VMEM((tiles, slots, lanes), jnp.float32),
                VMEM((tiles, feature, lanes), jnp.bfloat16),
                VMEM((passage_local, 128), jnp.int32),
                SMEM((passage_local, 128), jnp.int32),
                VMEM((2 * padded, lanes), jnp.float32),
                VMEM((UNROLL, padded, lanes), jnp.float32),
                VMEM((UNROLL, padded, lanes), jnp.float32),
                VMEM((UNROLL, lanes), jnp.float32),
                VMEM((UNROLL, lanes), jnp.float32),
                VMEM((chunks * 2 * UNROLL, padded, lanes), jnp.bfloat16),
                pltpu.SemaphoreType.DMA,
                pltpu.SemaphoreType.DMA((chunks,)),
            ],
            name="score",
            compiler_params=params,
        )(arrived, lengths.T, *replica_weights, rows)
    )
    all_scores = lax.all_to_all(scores, "grp", split_axis=0, concat_axis=0, tiled=True)

    query_total = query_local * groups * replicas
    grads, multiplier, numerator, weight_sum = pl.pallas_call(
        functools.partial(query_kernel, dims + (query_total,), "grp"),
        out_shape=(
            shape((groups, tokens, feature), jnp.bfloat16),
            shape((tiles, slots, lanes), jnp.float32),
            shape((1, 128), jnp.float32),
            shape((1, 128), jnp.float32),
        ),
        in_specs=vmem(4) + smem(2) + hbm(1),
        out_specs=tuple(vmem(4)),
        scratch_shapes=[
            VMEM(powers.shape, jnp.bfloat16),
            VMEM((tiles, slots, lanes), jnp.float32),
            pltpu.SemaphoreType.DMA((chunks,)),
        ]
        + [VMEM((tiles, feature, lanes), jnp.float32)] * SUMS,
        name="query_grad",
        compiler_params=params,
    )(arrived, all_scores, summed, turned, block_code, block_count, powers)
    returned = lax.all_to_all(grads, "grp", split_axis=0, concat_axis=0, tiled=True)

    passage_grad = pl.pallas_call(
        functools.partial(passage_kernel, (tokens, per_tile // query_local)),
        out_shape=shape((token_len, passage_local, feature), jnp.bfloat16),
        in_specs=vmem(2) + smem(2) + hbm(1),
        out_specs=pl.BlockSpec(memory_space=pltpu.HBM),
        scratch_shapes=[
            VMEM((token_len, passage_local, feature), jnp.bfloat16),
            VMEM(powers.shape, jnp.bfloat16),
            VMEM(((passage_local + 1) * pitch, feature), jnp.float32),
            VMEM((tiles, lanes, feature), jnp.bfloat16),
            pltpu.SemaphoreType.DMA((chunks,)),
            pltpu.SemaphoreType.DMA((PIECES,)),
        ],
        name="passage_grad",
        compiler_params=params,
        cost_estimate=pl.CostEstimate(
            flops=2 * limit * padded * lanes * feature,
            bytes_accessed=2 * limit * padded * lanes,
            transcendentals=0,
        ),
    )(arrived, multiplier, block_code, block_count, powers)
    numerators = from_replicas(numerator, replicas)

    loss = pair_sums(numerators)[0, 0] / weight_sum[0, 0]
    query_grad = jnp.sum(returned.astype(jnp.float32), axis=0)
    query_grad = query_grad.reshape(query_local, 1, query_len, feature)
    return (loss, query_grad, passage_grad.transpose(1, 0, 2)[:, None])


def solution(mesh):
    return jax.shard_map(
        on_device,
        mesh=mesh,
        in_specs=(
            P("grp", "rep", None, None),
            P("grp", "rep", None, None),
            P("grp", "rep"),
            P("grp", "rep", None),
            P("rep", None),
            P("grp", "rep", None),
            P("grp", "rep"),
        ),
        out_specs=(P(), P("grp", "rep", None, None), P("grp", "rep", None, None)),
        check_vma=False,
    )
```

```python
import functools
import math

import jax
import jax.numpy as jnp
from jax import lax
from jax.experimental import pallas as pl
from jax.experimental.pallas import tpu as pltpu
from jax.sharding import PartitionSpec as P


TEMPER = 0.05
LOG2E = math.log2(math.e)
MASKED = -1e30
KINDS = 8
UNROLL = 8
AHEAD = 3
SPREAD = 5
SUMS = 4
STORE = 5
PIECES = 4
HIGHEST = lax.Precision.HIGHEST
VMEM = pltpu.VMEM
SMEM = pltpu.SMEM


def round_up(value, multiple):
    return -(-value // multiple) * multiple


def iota(shape, dim):
    return lax.broadcasted_iota(jnp.int32, shape, dim)


def three_parts(values):
    first = values.astype(jnp.bfloat16).astype(jnp.float32)
    rest = values - first
    second = rest.astype(jnp.bfloat16).astype(jnp.float32)
    third = (rest - second).astype(jnp.bfloat16).astype(jnp.float32)
    return first, second, third


def pack_kernel(passage_local, queries, cand_ids, owner_map, teacher, weights, out, aux):
    groups = out.shape[0]
    tokens = queries.shape[0]
    query_local, _, candidates = cand_ids.shape
    entries = owner_map.shape[1]
    table = owner_map[...].astype(jnp.float32)
    owner = jnp.floor((table + 0.5) * (1.0 / passage_local))
    local = table - owner * passage_local
    which = iota((8, entries), 0)
    tables = jnp.where(which == 0, owner, jnp.where(which == 1, local, 0.0)).astype(jnp.bfloat16)
    aux[...] = jnp.zeros_like(aux)
    for q in range(query_local):
        hot = (iota((entries, candidates), 0) == cand_ids[q]).astype(jnp.bfloat16)
        found = jnp.dot(tables, hot, preferred_element_type=jnp.float32)
        scores = teacher[q]
        shifted = scores - jnp.max(scores, axis=1, keepdims=True)
        log_teacher = shifted - jnp.log(jnp.sum(jnp.exp(shifted), axis=1, keepdims=True))
        weight = jnp.broadcast_to(weights[:, q : q + 1], (1, candidates))
        rows = (found[0:1], found[1:2], *three_parts(log_teacher), *three_parts(weight))
        for kind, row in enumerate(rows):
            at = kind * query_local + q
            aux[at : at + 1, 0:candidates] = row
    packed = aux[...].astype(jnp.bfloat16)
    for g in range(groups):
        out[g, 0:tokens, :] = queries[...]
        out[g, tokens:, :] = packed


def owned_rows(arrived, tokens, query_local, candidates, g, q, me):
    at = tokens + q
    owner = arrived[g, at : at + 1, 0:candidates].astype(jnp.float32)
    at = tokens + query_local + q
    local = arrived[g, at : at + 1, 0:candidates].astype(jnp.float32)
    return jnp.where(owner == me.astype(jnp.float32), local, -1.0).astype(jnp.int32)


def prepare_kernel(stored_hbm, rows_hbm, stored, gathered, rows, stored_done, rows_done):
    token_len, chunk, feature = stored.shape
    padded = rows.shape[1]
    pitch = gathered.shape[0] // chunk
    pieces = stored_done.shape[0]
    piece = token_len // pieces
    spans = [(k * piece, token_len if k == pieces - 1 else (k + 1) * piece) for k in range(pieces)]
    copies = []
    for k, (first, last) in enumerate(spans):
        at = pl.ds(first, last - first)
        copies.append(pltpu.make_async_copy(stored_hbm.at[at], stored.at[at], stored_done.at[k]))
        copies[-1].start()

    def clear(p, carry):
        at = pl.ds(p * pitch + token_len, padded - token_len)
        gathered[at, :] = jnp.zeros((padded - token_len, feature), jnp.float32)
        return carry

    lax.fori_loop(0, chunk, clear, 0)
    for copy, (first, last) in zip(copies, spans):
        copy.wait()

        def spread(j, carry, first=first):
            for u in range(SPREAD):
                at = first + j * SPREAD + u
                gathered[pl.ds(at, chunk, stride=pitch), :] = stored[at].astype(jnp.float32)
            return carry

        whole = (last - first) // SPREAD
        lax.fori_loop(0, whole, spread, 0)
        for at in range(first + whole * SPREAD, last):
            gathered[pl.ds(at, chunk, stride=pitch), :] = stored[at].astype(jnp.float32)

    parts = rows_done.shape[0]
    part = chunk // parts
    ahead = math.gcd(part, 4)
    copies = []
    for k in range(parts):

        def collect(step, carry, first=k * part):
            for inner in range(ahead):
                p = first + step * ahead + inner
                rows[p] = gathered[pl.ds(p * pitch, padded), :].astype(jnp.bfloat16)
            return carry

        lax.fori_loop(0, part // ahead, collect, 0)
        at = pl.ds(k * part, part)
        copies.append(pltpu.make_async_copy(rows.at[at], rows_hbm.at[at], rows_done.at[k]))
        copies[-1].start()
    for copy in copies:
        copy.wait()


def list_blocks(flags_scalar, block_code, block_count, passage_count, tiles):
    base = code_base(tiles)
    ahead = math.gcd(passage_count, 4)

    def list_passages(step, count):
        for inner in range(ahead):
            p = step * ahead + inner
            for tile in range(tiles):
                block_code[0, count] = p * base + tile
                count = count + flags_scalar[tile, p]
        return count

    count = lax.fori_loop(0, passage_count // ahead, list_passages, jnp.int32(0))
    for extra in range(3 * UNROLL):
        block_code[0, count + extra] = passage_count * base
    steps = (count + 2 * UNROLL - 1) // (2 * UNROLL)
    block_count[0, 0] = steps
    return steps


def code_base(tiles):
    return 1 << (tiles - 1).bit_length()


def decode(block_code, block, tiles):
    code = block_code[0, block]
    base = code_base(tiles)
    return code >> (base.bit_length() - 1), code & (base - 1)


def score_kernel(
    dims,
    axis,
    arrived,
    lengths,
    *refs,
):
    tokens, query_local, candidates, per_tile, replicas = dims
    weights, refs = refs[:replicas], refs[replicas:]
    passages_hbm, scores_out, summed, block_code, block_count, powers_hbm, *scratch = refs
    score_body(
        (tokens, query_local, candidates, per_tile),
        lax.axis_index(axis),
        arrived,
        lengths,
        pair_sums([one[...] for one in weights]),
        passages_hbm,
        scores_out,
        summed,
        block_code,
        block_count,
        powers_hbm,
        *scratch,
    )


def score_body(
    dims,
    me,
    arrived,
    lengths,
    weights,
    passages_hbm,
    scores_out,
    summed,
    block_code,
    block_count,
    powers_hbm,
    highest,
    passages,
    turned,
    flags,
    flags_scalar,
    penalty,
    even,
    odd,
    even_top,
    odd_top,
    powers,
    flags_done,
    rows_done,
    powers_done,
):
    tokens, query_local, candidates, per_tile = dims
    groups = arrived.shape[0]
    passage_count, padded, _ = passages.shape
    tiles, _, lanes = highest.shape
    groups_per_tile = per_tile // query_local
    fetch_rows = pltpu.make_async_copy(passages_hbm, passages, rows_done)
    fetch_rows.start()

    column = iota((passage_count, 128), 1)
    passage_index = iota((passage_count, candidates), 0)
    marks = jnp.zeros((passage_count, 128), jnp.float32)
    for tile in range(tiles):
        hit = jnp.zeros((passage_count, candidates), jnp.int32)
        for g in range(tile * groups_per_tile, (tile + 1) * groups_per_tile):
            for q in range(query_local):
                mine = owned_rows(arrived, tokens, query_local, candidates, g, q, me)
                hit = jnp.where(passage_index == mine, 1, hit)
        any_hit = jnp.max(hit.astype(jnp.float32), axis=1, keepdims=True)
        marks = jnp.where(column == tile, any_hit, marks)
    flags[...] = marks.T[0 : flags.shape[0]].astype(jnp.int32)
    to_scalar = pltpu.make_async_copy(flags, flags_scalar, flags_done)
    to_scalar.start()

    for tile in range(tiles):
        parts = [
            arrived[g, 0:tokens, :]
            for g in range(tile * groups_per_tile, (tile + 1) * groups_per_tile)
        ]
        block = jnp.concatenate(parts, axis=0).astype(jnp.float32)
        turned[tile] = block.T.astype(jnp.bfloat16)
    highest[...] = jnp.zeros_like(highest)
    summed[...] = jnp.ones_like(summed)
    penalty[...] = jnp.where(iota(penalty.shape, 0) < padded, 0.0, MASKED)
    to_scalar.wait()
    steps = list_blocks(flags_scalar, block_code, block_count, passage_count, tiles)
    fetch_rows.wait()

    factor = LOG2E / TEMPER

    def multiply(first, into, tops):
        for u in range(UNROLL):
            slot, tile = decode(block_code, first + u, tiles)
            p = jnp.minimum(slot, passage_count - 1)
            products = jnp.dot(passages[p], turned[tile], preferred_element_type=jnp.float32)
            products = products + penalty[pl.ds(padded - lengths[0, p], padded), :]
            into[u] = products
            tops[u : u + 1, :] = jnp.max(products, axis=0, keepdims=True)

    def soften(first, held, tops):
        for u in range(UNROLL):
            slot, tile = decode(block_code, first + u, tiles)
            top = tops[u : u + 1, :]
            raised = jnp.exp2((held[u] - top) * factor)
            powers[first + u] = raised.astype(jnp.bfloat16)
            highest[tile, pl.ds(slot, 1), :] = top
            summed[tile, pl.ds(slot, 1), :] = jnp.sum(raised, axis=0, keepdims=True)

    def chunk_copy(s):
        at = pl.ds(s * 2 * UNROLL, 2 * UNROLL)
        return pltpu.make_async_copy(powers.at[at], powers_hbm.at[at], powers_done.at[s])

    multiply(0, even, even_top)

    def step(s, carry):
        first = s * 2 * UNROLL
        multiply(first + UNROLL, odd, odd_top)
        soften(first, even, even_top)
        multiply(first + 2 * UNROLL, even, even_top)
        soften(first + UNROLL, odd, odd_top)
        chunk_copy(s).start()
        return carry

    lax.fori_loop(0, steps, step, 0)

    query_len = lanes // per_tile
    member = iota((lanes, 128), 0) // query_len == iota((lanes, 128), 1)
    member = member.astype(jnp.float32)
    weight_part = jnp.sum(weights, axis=1, keepdims=True)
    scores_out[0] = jnp.broadcast_to(weight_part, scores_out.shape[1:])
    for tile in range(tiles):
        matched = highest[tile, 0:passage_count, :] + TEMPER * jnp.log(
            summed[tile, 0:passage_count, :]
        )
        sums = jnp.dot(matched, member, precision=HIGHEST, preferred_element_type=jnp.float32)
        for inner in range(per_tile):
            g = tile * groups_per_tile + inner // query_local
            q = inner % query_local
            mine = owned_rows(arrived, tokens, query_local, candidates, g, q, me)
            picked = jnp.where(passage_index == mine, sums[:, inner : inner + 1], 0.0)
            at = tile * per_tile + inner
            scores_out[0, at : at + 1, 0:candidates] = jnp.sum(picked, axis=0, keepdims=True)
    for g in range(1, groups):
        scores_out[g] = scores_out[0]

    def finish(s, carry):
        chunk_copy(s).wait()
        return carry

    lax.fori_loop(0, steps, finish, 0)


def pair_sums(values):
    while len(values) > 1:
        values = [values[i] + values[i + 1] for i in range(0, len(values), 2)]
    return values[0]


def query_kernel(
    dims,
    axis,
    arrived,
    scores,
    summed,
    block_code,
    block_count,
    passages_hbm,
    powers_hbm,
    grads_out,
    multiplier,
    numerator_out,
    weight_sum_out,
    passages,
    powers,
    factors,
    rows_done,
    powers_done,
    *sums,
):
    tokens, query_local, candidates, per_tile, query_total = dims
    groups = arrived.shape[0]
    tiles, slots, lanes = summed.shape
    passage_count = passages.shape[0]
    groups_per_tile = per_tile // query_local
    queries_all = tiles * per_tile
    query_len = lanes // per_tile
    me = lax.axis_index(axis)
    steps = block_count[0, 0]
    fetch_rows = pltpu.make_async_copy(passages_hbm, passages, rows_done)
    fetch_rows.start()

    def chunk_copy(s):
        at = pl.ds(s * 2 * UNROLL, 2 * UNROLL)
        return pltpu.make_async_copy(powers_hbm.at[at], powers.at[at], powers_done.at[s])

    for s in range(AHEAD):
        pl.when(s < steps)(chunk_copy(s).start)

    got = scores[0]
    for g in range(1, groups):
        got = got + scores[g]
    student = got[0:queries_all, 0:candidates]

    def gather_parts(kind):
        rows = []
        for g in range(groups):
            parts = []
            for part in range(3):
                at = tokens + (kind + part) * query_local
                block = arrived[g, at : at + query_local, 0:candidates]
                parts.append(block.astype(jnp.float32))
            rows.append((parts[0] + parts[1]) + parts[2])
        return jnp.concatenate(rows, axis=0)

    log_teacher = gather_parts(2)
    weight = gather_parts(5)
    shifted = student - jnp.max(student, axis=1, keepdims=True)
    log_student = shifted - jnp.log(jnp.sum(jnp.exp(shifted), axis=1, keepdims=True))
    teacher_prob = jnp.exp(log_teacher)
    spread = jnp.sum(weight * teacher_prob * (log_teacher - log_student), axis=1, keepdims=True)
    numerator = jnp.sum(spread, axis=0, keepdims=True)
    numerator_out[...] = jnp.broadcast_to(numerator, numerator_out.shape)
    weight_sum = got[0:1, candidates : candidates + 1]
    weight_sum_out[...] = jnp.broadcast_to(weight_sum, weight_sum_out.shape)
    scale = query_total / weight_sum
    grad = (weight * scale) * (jnp.exp(log_student) - teacher_prob)

    passage_index = iota((passage_count, candidates), 0)
    lane_query = iota((passage_count, lanes), 1) // query_len
    for tile in range(tiles):
        spread_out = jnp.zeros((passage_count, lanes), jnp.float32)
        for inner in range(per_tile):
            g = tile * groups_per_tile + inner // query_local
            q = inner % query_local
            mine = owned_rows(arrived, tokens, query_local, candidates, g, q, me)
            at = tile * per_tile + inner
            picked = jnp.where(passage_index == mine, grad[at : at + 1], 0.0)
            total = jnp.sum(picked, axis=1, keepdims=True)
            spread_out = jnp.where(lane_query == inner, total, spread_out)
        factors[tile, 0:passage_count, :] = spread_out / summed[tile, 0:passage_count, :]
        factors[tile, passage_count:, :] = jnp.zeros((slots - passage_count, lanes), jnp.float32)
    multiplier[...] = factors[...]

    for one in sums:
        one[...] = jnp.zeros_like(one)

    fetch_rows.wait()

    def step(s, carry):
        pl.when(s + AHEAD < steps)(lambda: chunk_copy(s + AHEAD).start())
        chunk_copy(s).wait()
        for u in range(2 * UNROLL):
            b = s * 2 * UNROLL + u
            slot, tile = decode(block_code, b, tiles)
            p = jnp.minimum(slot, passage_count - 1)
            part = powers[b].astype(jnp.float32) * factors[tile, pl.ds(slot, 1), :]
            part = part.astype(jnp.bfloat16)
            sums[u % len(sums)][tile] += lax.dot_general(
                passages[p], part, (((0,), (0,)), ((), ())), preferred_element_type=jnp.float32
            )
        return carry

    lax.fori_loop(0, steps, step, 0)
    for tile in range(tiles):
        back = pair_sums([one[tile] for one in sums]).T.astype(jnp.bfloat16)
        for inner in range(groups_per_tile):
            g = tile * groups_per_tile + inner
            grads_out[g] = back[inner * tokens : (inner + 1) * tokens]


def passage_kernel(
    dims,
    arrived,
    multiplier,
    block_code,
    block_count,
    powers_hbm,
    out_hbm,
    out,
    powers,
    sums,
    queries_all,
    powers_done,
    out_done,
):
    tokens, per_tile_groups = dims
    token_len, passage_count, feature = out.shape
    tiles = queries_all.shape[0]
    padded = powers.shape[1]
    pitch = sums.shape[0] // (passage_count + 1)
    steps = block_count[0, 0]

    def chunk_copy(s):
        at = pl.ds(s * 2 * UNROLL, 2 * UNROLL)
        return pltpu.make_async_copy(powers_hbm.at[at], powers.at[at], powers_done.at[s])

    for s in range(AHEAD):
        pl.when(s < steps)(chunk_copy(s).start)
    for tile in range(tiles):
        for inner in range(per_tile_groups):
            g = tile * per_tile_groups + inner
            queries_all[tile, inner * tokens : (inner + 1) * tokens, :] = arrived[g, 0:tokens, :]

    def clear(p, carry):
        sums[pl.ds(p * pitch, pitch), :] = jnp.zeros((pitch, feature), jnp.float32)
        return carry

    lax.fori_loop(0, passage_count, clear, 0)

    def step(s, carry):
        pl.when(s + AHEAD < steps)(lambda: chunk_copy(s + AHEAD).start())
        chunk_copy(s).wait()
        for u in range(2 * UNROLL):
            b = s * 2 * UNROLL + u
            slot, tile = decode(block_code, b, tiles)
            part = powers[b].astype(jnp.float32) * multiplier[tile, pl.ds(slot, 1), :]
            at = pl.ds(slot * pitch, padded)
            sums[at, :] += jnp.dot(
                part.astype(jnp.bfloat16), queries_all[tile], preferred_element_type=jnp.float32
            )
        return carry

    lax.fori_loop(0, steps, step, 0)

    pieces = out_done.shape[0]
    piece = token_len // pieces
    copies = []
    for k in range(pieces):
        first = k * piece
        last = token_len if k == pieces - 1 else first + piece

        def store(j, carry, first=first):
            for u in range(STORE):
                at = first + j * STORE + u
                out[at] = sums[pl.ds(at, passage_count, stride=pitch), :].astype(out.dtype)
            return carry

        whole = (last - first) // STORE
        lax.fori_loop(0, whole, store, 0)
        for at in range(first + whole * STORE, last):
            out[at] = sums[pl.ds(at, passage_count, stride=pitch), :].astype(out.dtype)
        rows = pl.ds(first, last - first)
        copies.append(pltpu.make_async_copy(out.at[rows], out_hbm.at[rows], out_done.at[k]))
        copies[-1].start()
    for copy in copies:
        copy.wait()


def vmem(count):
    return [pl.BlockSpec(memory_space=VMEM)] * count


def smem(count):
    return [pl.BlockSpec(memory_space=SMEM)] * count


def from_replicas(values, replicas):
    rings = [[(r, r ^ hop) for r in range(replicas)] for hop in range(1, replicas)]
    return [values] + [lax.ppermute(values, "rep", ring) for ring in rings]


def hbm(count):
    return [pl.BlockSpec(memory_space=pltpu.HBM)] * count


def on_device(queries, passages, lengths, cand_ids, owner_map, teacher, weights):
    groups = lax.axis_size("grp")
    replicas = lax.axis_size("rep")
    query_local, _, query_len, feature = queries.shape
    passage_local, _, token_len, _ = passages.shape
    candidates = cand_ids.shape[2]
    tokens = query_local * query_len
    lanes = 128
    per_tile = lanes // query_len
    tiles = groups * tokens // lanes
    padded = round_up(token_len, 16)
    pitch = padded + 9
    ref_count = query_local * candidates
    capacity = groups * (2 * ref_count // groups)
    limit = min(passage_local * tiles, capacity)
    blocks = limit + 3 * UNROLL
    chunks = -(-limit // (2 * UNROLL))
    aux_rows = round_up(KINDS * query_local, 16)
    slots = round_up(passage_local + 1, 8)
    score_rows = round_up(groups * query_local, 8)
    shape = jax.ShapeDtypeStruct
    alone = pltpu.CompilerParams(vmem_limit_bytes=62 * 2**20)
    params = pltpu.CompilerParams(vmem_limit_bytes=52 * 2**20)

    share = pl.pallas_call(
        functools.partial(pack_kernel, passage_local),
        out_shape=shape((groups, tokens + aux_rows, feature), jnp.bfloat16),
        in_specs=vmem(5),
        out_specs=pl.BlockSpec(memory_space=VMEM),
        scratch_shapes=[VMEM((aux_rows, feature), jnp.float32)],
        name="pack",
        compiler_params=alone,
    )(queries.reshape(tokens, feature), cand_ids, owner_map, teacher, weights.T)
    arrived = lax.all_to_all(share, "grp", split_axis=0, concat_axis=0, tiled=True)

    replica_weights = from_replicas(weights.T, replicas)

    rows = pl.pallas_call(
        prepare_kernel,
        out_shape=shape((passage_local, padded, feature), jnp.bfloat16),
        in_specs=hbm(1),
        out_specs=pl.BlockSpec(memory_space=pltpu.HBM),
        scratch_shapes=[
            VMEM((token_len, passage_local, feature), jnp.bfloat16),
            VMEM((passage_local * pitch, feature), jnp.float32),
            VMEM((passage_local, padded, feature), jnp.bfloat16),
            pltpu.SemaphoreType.DMA((PIECES,)),
            pltpu.SemaphoreType.DMA((math.gcd(passage_local, PIECES),)),
        ],
        name="prepare",
        compiler_params=params,
    )(passages[:, 0].transpose(1, 0, 2))

    dims = (tokens, query_local, candidates, per_tile)
    scores, summed, block_code, block_count, powers = (
        pl.pallas_call(
            functools.partial(score_kernel, dims + (replicas,), "grp"),
            out_shape=(
                shape((groups, score_rows, 128), jnp.float32),
                shape((tiles, slots, lanes), jnp.float32),
                shape((1, blocks), jnp.int32),
                shape((1, 1), jnp.int32),
                shape((chunks * 2 * UNROLL, padded, lanes), jnp.bfloat16),
            ),
            in_specs=vmem(1) + smem(1) + vmem(replicas) + hbm(1),
            out_specs=tuple(vmem(2) + smem(2) + hbm(1)),
            scratch_shapes=[
                VMEM((tiles, slots, lanes), jnp.float32),
                VMEM((passage_local, padded, feature), jnp.bfloat16),
                VMEM((tiles, feature, lanes), jnp.bfloat16),
                VMEM((round_up(tiles, 8), passage_local), jnp.int32),
                SMEM((round_up(tiles, 8), passage_local), jnp.int32),
                VMEM((2 * padded, lanes), jnp.float32),
                VMEM((UNROLL, padded, lanes), jnp.float32),
                VMEM((UNROLL, padded, lanes), jnp.float32),
                VMEM((UNROLL, lanes), jnp.float32),
                VMEM((UNROLL, lanes), jnp.float32),
                VMEM((chunks * 2 * UNROLL, padded, lanes), jnp.bfloat16),
                pltpu.SemaphoreType.DMA,
                pltpu.SemaphoreType.DMA,
                pltpu.SemaphoreType.DMA((chunks,)),
            ],
            name="score",
            compiler_params=params,
        )(arrived, lengths.T, *replica_weights, rows)
    )
    all_scores = lax.all_to_all(scores, "grp", split_axis=0, concat_axis=0, tiled=True)

    query_total = query_local * groups * replicas
    grads, multiplier, numerator, weight_sum = pl.pallas_call(
        functools.partial(query_kernel, dims + (query_total,), "grp"),
        out_shape=(
            shape((groups, tokens, feature), jnp.bfloat16),
            shape((tiles, slots, lanes), jnp.float32),
            shape((1, 128), jnp.float32),
            shape((1, 128), jnp.float32),
        ),
        in_specs=vmem(3) + smem(2) + hbm(2),
        out_specs=tuple(vmem(4)),
        scratch_shapes=[
            VMEM(rows.shape, jnp.bfloat16),
            VMEM(powers.shape, jnp.bfloat16),
            VMEM((tiles, slots, lanes), jnp.float32),
            pltpu.SemaphoreType.DMA,
            pltpu.SemaphoreType.DMA((chunks,)),
        ]
        + [VMEM((tiles, feature, lanes), jnp.float32)] * SUMS,
        name="query_grad",
        compiler_params=params,
    )(arrived, all_scores, summed, block_code, block_count, rows, powers)
    returned = lax.all_to_all(grads, "grp", split_axis=0, concat_axis=0, tiled=True)

    passage_grad = pl.pallas_call(
        functools.partial(passage_kernel, (tokens, per_tile // query_local)),
        out_shape=shape((token_len, passage_local, feature), jnp.bfloat16),
        in_specs=vmem(2) + smem(2) + hbm(1),
        out_specs=pl.BlockSpec(memory_space=pltpu.HBM),
        scratch_shapes=[
            VMEM((token_len, passage_local, feature), jnp.bfloat16),
            VMEM(powers.shape, jnp.bfloat16),
            VMEM(((passage_local + 1) * pitch, feature), jnp.float32),
            VMEM((tiles, lanes, feature), jnp.bfloat16),
            pltpu.SemaphoreType.DMA((chunks,)),
            pltpu.SemaphoreType.DMA((PIECES,)),
        ],
        name="passage_grad",
        compiler_params=params,
        cost_estimate=pl.CostEstimate(
            flops=2 * limit * padded * lanes * feature,
            bytes_accessed=2 * limit * padded * lanes,
            transcendentals=0,
        ),
    )(arrived, multiplier, block_code, block_count, powers)
    numerators = from_replicas(numerator, replicas)

    loss = pair_sums(numerators)[0, 0] / weight_sum[0, 0]
    query_grad = jnp.sum(returned.astype(jnp.float32), axis=0)
    query_grad = query_grad.reshape(query_local, 1, query_len, feature)
    return (loss, query_grad, passage_grad.transpose(1, 0, 2)[:, None])


def solution(mesh):
    return jax.shard_map(
        on_device,
        mesh=mesh,
        in_specs=(
            P("grp", "rep", None, None),
            P("grp", "rep", None, None),
            P("grp", "rep"),
            P("grp", "rep", None),
            P("rep", None),
            P("grp", "rep", None),
            P("grp", "rep"),
        ),
        out_specs=(P(), P("grp", "rep", None, None), P("grp", "rep", None, None)),
        check_vma=False,
    )
```

```python
import functools
import math

import jax
import jax.numpy as jnp
from jax import lax
from jax.experimental import pallas as pl
from jax.experimental.pallas import tpu as pltpu
from jax.sharding import PartitionSpec as P


TEMPER = 0.05
LOG2E = math.log2(math.e)
MASKED = -1e30
KINDS = 8
UNROLL = 14
SPREAD = 5
SUMS = 4
STORE = 5
PIECES = 4
HIGHEST = lax.Precision.HIGHEST
VMEM = pltpu.VMEM
SMEM = pltpu.SMEM


def round_up(value, multiple):
    return -(-value // multiple) * multiple


def iota(shape, dim):
    return lax.broadcasted_iota(jnp.int32, shape, dim)


def three_parts(values):
    first = values.astype(jnp.bfloat16).astype(jnp.float32)
    rest = values - first
    second = rest.astype(jnp.bfloat16).astype(jnp.float32)
    third = (rest - second).astype(jnp.bfloat16).astype(jnp.float32)
    return first, second, third


def pack_kernel(passage_local, queries, cand_ids, owner_map, teacher, weights, out, aux):
    groups = out.shape[0]
    tokens = queries.shape[0]
    query_local, _, candidates = cand_ids.shape
    entries = owner_map.shape[1]
    table = owner_map[...].astype(jnp.float32)
    owner = jnp.floor((table + 0.5) * (1.0 / passage_local))
    local = table - owner * passage_local
    which = iota((8, entries), 0)
    tables = jnp.where(which == 0, owner, jnp.where(which == 1, local, 0.0)).astype(jnp.bfloat16)
    aux[...] = jnp.zeros_like(aux)
    for q in range(query_local):
        hot = (iota((entries, candidates), 0) == cand_ids[q]).astype(jnp.bfloat16)
        found = jnp.dot(tables, hot, preferred_element_type=jnp.float32)
        scores = teacher[q]
        shifted = scores - jnp.max(scores, axis=1, keepdims=True)
        log_teacher = shifted - jnp.log(jnp.sum(jnp.exp(shifted), axis=1, keepdims=True))
        weight = jnp.broadcast_to(weights[:, q : q + 1], (1, candidates))
        rows = (found[0:1], found[1:2], *three_parts(log_teacher), *three_parts(weight))
        for kind, row in enumerate(rows):
            at = kind * query_local + q
            aux[at : at + 1, 0:candidates] = row
    packed = aux[...].astype(jnp.bfloat16)
    for g in range(groups):
        out[g, 0:tokens, :] = queries[...]
        out[g, tokens:, :] = packed


def owned_rows(arrived, tokens, query_local, candidates, g, q, me):
    at = tokens + q
    owner = arrived[g, at : at + 1, 0:candidates].astype(jnp.float32)
    at = tokens + query_local + q
    local = arrived[g, at : at + 1, 0:candidates].astype(jnp.float32)
    return jnp.where(owner == me.astype(jnp.float32), local, -1.0).astype(jnp.int32)


def prepare_kernel(stored_hbm, rows_hbm, stored, gathered, rows, stored_done, rows_done):
    token_len, chunk, feature = stored.shape
    padded = rows.shape[1]
    pitch = gathered.shape[0] // chunk
    pieces = stored_done.shape[0]
    piece = token_len // pieces
    spans = [(k * piece, token_len if k == pieces - 1 else (k + 1) * piece) for k in range(pieces)]
    copies = []
    for k, (first, last) in enumerate(spans):
        at = pl.ds(first, last - first)
        copies.append(pltpu.make_async_copy(stored_hbm.at[at], stored.at[at], stored_done.at[k]))
        copies[-1].start()

    def clear(p, carry):
        at = pl.ds(p * pitch + token_len, padded - token_len)
        gathered[at, :] = jnp.zeros((padded - token_len, feature), jnp.float32)
        return carry

    lax.fori_loop(0, chunk, clear, 0)
    for copy, (first, last) in zip(copies, spans):
        copy.wait()

        def spread(j, carry, first=first):
            for u in range(SPREAD):
                at = first + j * SPREAD + u
                gathered[pl.ds(at, chunk, stride=pitch), :] = stored[at].astype(jnp.float32)
            return carry

        whole = (last - first) // SPREAD
        lax.fori_loop(0, whole, spread, 0)
        for at in range(first + whole * SPREAD, last):
            gathered[pl.ds(at, chunk, stride=pitch), :] = stored[at].astype(jnp.float32)

    parts = rows_done.shape[0]
    part = chunk // parts
    ahead = math.gcd(part, 4)
    copies = []
    for k in range(parts):

        def collect(step, carry, first=k * part):
            for inner in range(ahead):
                p = first + step * ahead + inner
                rows[p] = gathered[pl.ds(p * pitch, padded), :].astype(jnp.bfloat16)
            return carry

        lax.fori_loop(0, part // ahead, collect, 0)
        at = pl.ds(k * part, part)
        copies.append(pltpu.make_async_copy(rows.at[at], rows_hbm.at[at], rows_done.at[k]))
        copies[-1].start()
    for copy in copies:
        copy.wait()


def list_blocks(flags_scalar, block_code, block_count, passage_count, tiles):
    base = code_base(tiles)
    ahead = math.gcd(passage_count, 4)

    def list_passages(step, count):
        for inner in range(ahead):
            p = step * ahead + inner
            for tile in range(tiles):
                block_code[0, count] = p * base + tile
                count = count + flags_scalar[p, tile]
        return count

    count = lax.fori_loop(0, passage_count // ahead, list_passages, jnp.int32(0))
    for extra in range(3 * UNROLL):
        block_code[0, count + extra] = passage_count * base
    steps = (count + 2 * UNROLL - 1) // (2 * UNROLL)
    block_count[0, 0] = steps
    return steps


def code_base(tiles):
    return 1 << (tiles - 1).bit_length()


def decode(block_code, block, tiles):
    code = block_code[0, block]
    base = code_base(tiles)
    return code >> (base.bit_length() - 1), code & (base - 1)


def score_kernel(
    dims,
    axis,
    arrived,
    lengths,
    *refs,
):
    tokens, query_local, candidates, per_tile, replicas = dims
    weights, refs = refs[:replicas], refs[replicas:]
    passages_hbm, scores_out, summed, block_code, block_count, powers_hbm, *scratch = refs
    score_body(
        (tokens, query_local, candidates, per_tile),
        lax.axis_index(axis),
        arrived,
        lengths,
        pair_sums([one[...] for one in weights]),
        passages_hbm,
        scores_out,
        summed,
        block_code,
        block_count,
        powers_hbm,
        *scratch,
    )


def score_body(
    dims,
    me,
    arrived,
    lengths,
    weights,
    passages_hbm,
    scores_out,
    summed,
    block_code,
    block_count,
    powers_hbm,
    highest,
    passages,
    turned,
    flags,
    flags_scalar,
    penalty,
    even,
    odd,
    even_top,
    odd_top,
    powers,
    flags_done,
    rows_done,
    powers_done,
):
    tokens, query_local, candidates, per_tile = dims
    groups = arrived.shape[0]
    passage_count, padded, _ = passages.shape
    tiles, _, lanes = highest.shape
    groups_per_tile = per_tile // query_local
    fetch_rows = pltpu.make_async_copy(passages_hbm, passages, rows_done)
    fetch_rows.start()

    column = iota(flags.shape, 1)
    passage_index = iota((passage_count, candidates), 0)
    marks = jnp.zeros(flags.shape, jnp.int32)
    for tile in range(tiles):
        hit = jnp.zeros((passage_count, candidates), jnp.int32)
        for g in range(tile * groups_per_tile, (tile + 1) * groups_per_tile):
            for q in range(query_local):
                mine = owned_rows(arrived, tokens, query_local, candidates, g, q, me)
                hit = jnp.where(passage_index == mine, 1, hit)
        any_hit = jnp.max(hit, axis=1, keepdims=True)
        marks = jnp.where(column == tile, any_hit, marks)
    flags[...] = marks
    to_scalar = pltpu.make_async_copy(flags, flags_scalar, flags_done)
    to_scalar.start()

    for tile in range(tiles):
        parts = [
            arrived[g, 0:tokens, :]
            for g in range(tile * groups_per_tile, (tile + 1) * groups_per_tile)
        ]
        block = jnp.concatenate(parts, axis=0).astype(jnp.float32)
        turned[tile] = block.T.astype(jnp.bfloat16)
    highest[...] = jnp.zeros_like(highest)
    summed[...] = jnp.ones_like(summed)
    penalty[...] = jnp.where(iota(penalty.shape, 0) < padded, 0.0, MASKED)
    to_scalar.wait()
    steps = list_blocks(flags_scalar, block_code, block_count, passage_count, tiles)
    fetch_rows.wait()

    factor = LOG2E / TEMPER

    def multiply(first, into, tops):
        for u in range(UNROLL):
            slot, tile = decode(block_code, first + u, tiles)
            p = jnp.minimum(slot, passage_count - 1)
            products = jnp.dot(passages[p], turned[tile], preferred_element_type=jnp.float32)
            products = products + penalty[pl.ds(padded - lengths[0, p], padded), :]
            into[u] = products
            tops[u : u + 1, :] = jnp.max(products, axis=0, keepdims=True)

    def soften(first, held, tops):
        for u in range(UNROLL):
            slot, tile = decode(block_code, first + u, tiles)
            top = tops[u : u + 1, :]
            raised = jnp.exp2((held[u] - top) * factor)
            powers[first + u] = raised.astype(jnp.bfloat16)
            highest[tile, pl.ds(slot, 1), :] = top
            summed[tile, pl.ds(slot, 1), :] = jnp.sum(raised, axis=0, keepdims=True)

    def chunk_copy(s):
        at = pl.ds(s * 2 * UNROLL, 2 * UNROLL)
        return pltpu.make_async_copy(powers.at[at], powers_hbm.at[at], powers_done.at[s])

    multiply(0, even, even_top)

    def step(s, carry):
        first = s * 2 * UNROLL
        multiply(first + UNROLL, odd, odd_top)
        soften(first, even, even_top)
        multiply(first + 2 * UNROLL, even, even_top)
        soften(first + UNROLL, odd, odd_top)
        chunk_copy(s).start()
        return carry

    lax.fori_loop(0, steps, step, 0)

    query_len = lanes // per_tile
    member = iota((lanes, 128), 0) // query_len == iota((lanes, 128), 1)
    member = member.astype(jnp.float32)
    weight_part = jnp.sum(weights, axis=1, keepdims=True)
    scores_out[0] = jnp.broadcast_to(weight_part, scores_out.shape[1:])
    for tile in range(tiles):
        matched = highest[tile, 0:passage_count, :] + TEMPER * jnp.log(
            summed[tile, 0:passage_count, :]
        )
        sums = jnp.dot(matched, member, precision=HIGHEST, preferred_element_type=jnp.float32)
        for inner in range(per_tile):
            g = tile * groups_per_tile + inner // query_local
            q = inner % query_local
            mine = owned_rows(arrived, tokens, query_local, candidates, g, q, me)
            picked = jnp.where(passage_index == mine, sums[:, inner : inner + 1], 0.0)
            at = tile * per_tile + inner
            scores_out[0, at : at + 1, 0:candidates] = jnp.sum(picked, axis=0, keepdims=True)
    for g in range(1, groups):
        scores_out[g] = scores_out[0]

    def finish(s, carry):
        chunk_copy(s).wait()
        return carry

    lax.fori_loop(0, steps, finish, 0)


def pair_sums(values):
    while len(values) > 1:
        values = [values[i] + values[i + 1] for i in range(0, len(values), 2)]
    return values[0]


def query_kernel(
    dims,
    axis,
    arrived,
    scores,
    summed,
    block_code,
    block_count,
    passages_hbm,
    powers_hbm,
    grads_out,
    multiplier,
    numerator_out,
    weight_sum_out,
    passages,
    powers,
    factors,
    rows_done,
    powers_done,
    *sums,
):
    tokens, query_local, candidates, per_tile, query_total = dims
    groups = arrived.shape[0]
    tiles, slots, lanes = summed.shape
    passage_count = passages.shape[0]
    groups_per_tile = per_tile // query_local
    queries_all = tiles * per_tile
    query_len = lanes // per_tile
    me = lax.axis_index(axis)
    steps = block_count[0, 0]
    fetch_rows = pltpu.make_async_copy(passages_hbm, passages, rows_done)
    fetch_rows.start()

    def chunk_copy(s):
        at = pl.ds(s * 2 * UNROLL, 2 * UNROLL)
        return pltpu.make_async_copy(powers_hbm.at[at], powers.at[at], powers_done.at[s])

    def fetch(s, carry):
        chunk_copy(s).start()
        return carry

    lax.fori_loop(0, steps, fetch, 0)

    got = scores[0]
    for g in range(1, groups):
        got = got + scores[g]
    student = got[0:queries_all, 0:candidates]

    def gather_parts(kind):
        rows = []
        for g in range(groups):
            parts = []
            for part in range(3):
                at = tokens + (kind + part) * query_local
                block = arrived[g, at : at + query_local, 0:candidates]
                parts.append(block.astype(jnp.float32))
            rows.append((parts[0] + parts[1]) + parts[2])
        return jnp.concatenate(rows, axis=0)

    log_teacher = gather_parts(2)
    weight = gather_parts(5)
    shifted = student - jnp.max(student, axis=1, keepdims=True)
    log_student = shifted - jnp.log(jnp.sum(jnp.exp(shifted), axis=1, keepdims=True))
    teacher_prob = jnp.exp(log_teacher)
    spread = jnp.sum(weight * teacher_prob * (log_teacher - log_student), axis=1, keepdims=True)
    numerator = jnp.sum(spread, axis=0, keepdims=True)
    numerator_out[...] = jnp.broadcast_to(numerator, numerator_out.shape)
    weight_sum = got[0:1, candidates : candidates + 1]
    weight_sum_out[...] = jnp.broadcast_to(weight_sum, weight_sum_out.shape)
    scale = query_total / weight_sum
    grad = (weight * scale) * (jnp.exp(log_student) - teacher_prob)

    passage_index = iota((passage_count, candidates), 0)
    lane_query = iota((passage_count, lanes), 1) // query_len
    for tile in range(tiles):
        spread_out = jnp.zeros((passage_count, lanes), jnp.float32)
        for inner in range(per_tile):
            g = tile * groups_per_tile + inner // query_local
            q = inner % query_local
            mine = owned_rows(arrived, tokens, query_local, candidates, g, q, me)
            at = tile * per_tile + inner
            picked = jnp.where(passage_index == mine, grad[at : at + 1], 0.0)
            total = jnp.sum(picked, axis=1, keepdims=True)
            spread_out = jnp.where(lane_query == inner, total, spread_out)
        factors[tile, 0:passage_count, :] = spread_out / summed[tile, 0:passage_count, :]
        factors[tile, passage_count:, :] = jnp.zeros((slots - passage_count, lanes), jnp.float32)
    multiplier[...] = factors[...]

    for one in sums:
        one[...] = jnp.zeros_like(one)

    fetch_rows.wait()

    def step(s, carry):
        chunk_copy(s).wait()
        for u in range(2 * UNROLL):
            b = s * 2 * UNROLL + u
            slot, tile = decode(block_code, b, tiles)
            p = jnp.minimum(slot, passage_count - 1)
            part = powers[b].astype(jnp.float32) * factors[tile, pl.ds(slot, 1), :]
            part = part.astype(jnp.bfloat16)
            sums[u % len(sums)][tile] += lax.dot_general(
                passages[p], part, (((0,), (0,)), ((), ())), preferred_element_type=jnp.float32
            )
        return carry

    lax.fori_loop(0, steps, step, 0)
    for tile in range(tiles):
        back = pair_sums([one[tile] for one in sums]).T.astype(jnp.bfloat16)
        for inner in range(groups_per_tile):
            g = tile * groups_per_tile + inner
            grads_out[g] = back[inner * tokens : (inner + 1) * tokens]


def passage_kernel(
    dims,
    arrived,
    multiplier,
    block_code,
    block_count,
    powers_hbm,
    out_hbm,
    out,
    powers,
    sums,
    queries_all,
    powers_done,
    out_done,
):
    tokens, per_tile_groups = dims
    token_len, passage_count, feature = out.shape
    tiles = queries_all.shape[0]
    padded = powers.shape[1]
    pitch = sums.shape[0] // (passage_count + 1)
    steps = block_count[0, 0]

    def chunk_copy(s):
        at = pl.ds(s * 2 * UNROLL, 2 * UNROLL)
        return pltpu.make_async_copy(powers_hbm.at[at], powers.at[at], powers_done.at[s])

    def fetch(s, carry):
        chunk_copy(s).start()
        return carry

    lax.fori_loop(0, steps, fetch, 0)
    for tile in range(tiles):
        for inner in range(per_tile_groups):
            g = tile * per_tile_groups + inner
            queries_all[tile, inner * tokens : (inner + 1) * tokens, :] = arrived[g, 0:tokens, :]

    def clear(p, carry):
        sums[pl.ds(p * pitch, pitch), :] = jnp.zeros((pitch, feature), jnp.float32)
        return carry

    lax.fori_loop(0, passage_count, clear, 0)

    def step(s, carry):
        chunk_copy(s).wait()
        for u in range(2 * UNROLL):
            b = s * 2 * UNROLL + u
            slot, tile = decode(block_code, b, tiles)
            part = powers[b].astype(jnp.float32) * multiplier[tile, pl.ds(slot, 1), :]
            at = pl.ds(slot * pitch, padded)
            sums[at, :] += jnp.dot(
                part.astype(jnp.bfloat16), queries_all[tile], preferred_element_type=jnp.float32
            )
        return carry

    lax.fori_loop(0, steps, step, 0)

    pieces = out_done.shape[0]
    piece = token_len // pieces
    copies = []
    for k in range(pieces):
        first = k * piece
        last = token_len if k == pieces - 1 else first + piece

        def store(j, carry, first=first):
            for u in range(STORE):
                at = first + j * STORE + u
                out[at] = sums[pl.ds(at, passage_count, stride=pitch), :].astype(out.dtype)
            return carry

        whole = (last - first) // STORE
        lax.fori_loop(0, whole, store, 0)
        for at in range(first + whole * STORE, last):
            out[at] = sums[pl.ds(at, passage_count, stride=pitch), :].astype(out.dtype)
        rows = pl.ds(first, last - first)
        copies.append(pltpu.make_async_copy(out.at[rows], out_hbm.at[rows], out_done.at[k]))
        copies[-1].start()
    for copy in copies:
        copy.wait()


def vmem(count):
    return [pl.BlockSpec(memory_space=VMEM)] * count


def smem(count):
    return [pl.BlockSpec(memory_space=SMEM)] * count


def from_replicas(values, replicas):
    rings = [[(r, r ^ hop) for r in range(replicas)] for hop in range(1, replicas)]
    return [values] + [lax.ppermute(values, "rep", ring) for ring in rings]


def hbm(count):
    return [pl.BlockSpec(memory_space=pltpu.HBM)] * count


def on_device(queries, passages, lengths, cand_ids, owner_map, teacher, weights):
    groups = lax.axis_size("grp")
    replicas = lax.axis_size("rep")
    query_local, _, query_len, feature = queries.shape
    passage_local, _, token_len, _ = passages.shape
    candidates = cand_ids.shape[2]
    tokens = query_local * query_len
    lanes = 128
    per_tile = lanes // query_len
    tiles = groups * tokens // lanes
    padded = round_up(token_len, 16)
    pitch = padded + 9
    ref_count = query_local * candidates
    capacity = groups * (2 * ref_count // groups)
    limit = min(passage_local * tiles, capacity)
    blocks = limit + 3 * UNROLL
    chunks = -(-limit // (2 * UNROLL))
    aux_rows = round_up(KINDS * query_local, 16)
    slots = round_up(passage_local + 1, 8)
    score_rows = round_up(groups * query_local, 8)
    shape = jax.ShapeDtypeStruct
    alone = pltpu.CompilerParams(vmem_limit_bytes=62 * 2**20)
    params = pltpu.CompilerParams(vmem_limit_bytes=52 * 2**20)

    share = pl.pallas_call(
        functools.partial(pack_kernel, passage_local),
        out_shape=shape((groups, tokens + aux_rows, feature), jnp.bfloat16),
        in_specs=vmem(5),
        out_specs=pl.BlockSpec(memory_space=VMEM),
        scratch_shapes=[VMEM((aux_rows, feature), jnp.float32)],
        name="pack",
        compiler_params=alone,
    )(queries.reshape(tokens, feature), cand_ids, owner_map, teacher, weights.T)
    arrived = lax.all_to_all(share, "grp", split_axis=0, concat_axis=0, tiled=True)

    replica_weights = from_replicas(weights.T, replicas)

    rows = pl.pallas_call(
        prepare_kernel,
        out_shape=shape((passage_local, padded, feature), jnp.bfloat16),
        in_specs=hbm(1),
        out_specs=pl.BlockSpec(memory_space=pltpu.HBM),
        scratch_shapes=[
            VMEM((token_len, passage_local, feature), jnp.bfloat16),
            VMEM((passage_local * pitch, feature), jnp.float32),
            VMEM((passage_local, padded, feature), jnp.bfloat16),
            pltpu.SemaphoreType.DMA((PIECES,)),
            pltpu.SemaphoreType.DMA((math.gcd(passage_local, PIECES),)),
        ],
        name="prepare",
        compiler_params=params,
    )(passages[:, 0].transpose(1, 0, 2))

    dims = (tokens, query_local, candidates, per_tile)
    scores, summed, block_code, block_count, powers = (
        pl.pallas_call(
            functools.partial(score_kernel, dims + (replicas,), "grp"),
            out_shape=(
                shape((groups, score_rows, 128), jnp.float32),
                shape((tiles, slots, lanes), jnp.float32),
                shape((1, blocks), jnp.int32),
                shape((1, 1), jnp.int32),
                shape((chunks * 2 * UNROLL, padded, lanes), jnp.bfloat16),
            ),
            in_specs=vmem(1) + smem(1) + vmem(replicas) + hbm(1),
            out_specs=tuple(vmem(2) + smem(2) + hbm(1)),
            scratch_shapes=[
                VMEM((tiles, slots, lanes), jnp.float32),
                VMEM((passage_local, padded, feature), jnp.bfloat16),
                VMEM((tiles, feature, lanes), jnp.bfloat16),
                VMEM((passage_local, 128), jnp.int32),
                SMEM((passage_local, 128), jnp.int32),
                VMEM((2 * padded, lanes), jnp.float32),
                VMEM((UNROLL, padded, lanes), jnp.float32),
                VMEM((UNROLL, padded, lanes), jnp.float32),
                VMEM((UNROLL, lanes), jnp.float32),
                VMEM((UNROLL, lanes), jnp.float32),
                VMEM((chunks * 2 * UNROLL, padded, lanes), jnp.bfloat16),
                pltpu.SemaphoreType.DMA,
                pltpu.SemaphoreType.DMA,
                pltpu.SemaphoreType.DMA((chunks,)),
            ],
            name="score",
            compiler_params=params,
        )(arrived, lengths.T, *replica_weights, rows)
    )
    all_scores = lax.all_to_all(scores, "grp", split_axis=0, concat_axis=0, tiled=True)

    query_total = query_local * groups * replicas
    grads, multiplier, numerator, weight_sum = pl.pallas_call(
        functools.partial(query_kernel, dims + (query_total,), "grp"),
        out_shape=(
            shape((groups, tokens, feature), jnp.bfloat16),
            shape((tiles, slots, lanes), jnp.float32),
            shape((1, 128), jnp.float32),
            shape((1, 128), jnp.float32),
        ),
        in_specs=vmem(3) + smem(2) + hbm(2),
        out_specs=tuple(vmem(4)),
        scratch_shapes=[
            VMEM(rows.shape, jnp.bfloat16),
            VMEM(powers.shape, jnp.bfloat16),
            VMEM((tiles, slots, lanes), jnp.float32),
            pltpu.SemaphoreType.DMA,
            pltpu.SemaphoreType.DMA((chunks,)),
        ]
        + [VMEM((tiles, feature, lanes), jnp.float32)] * SUMS,
        name="query_grad",
        compiler_params=params,
    )(arrived, all_scores, summed, block_code, block_count, rows, powers)
    returned = lax.all_to_all(grads, "grp", split_axis=0, concat_axis=0, tiled=True)

    passage_grad = pl.pallas_call(
        functools.partial(passage_kernel, (tokens, per_tile // query_local)),
        out_shape=shape((token_len, passage_local, feature), jnp.bfloat16),
        in_specs=vmem(2) + smem(2) + hbm(1),
        out_specs=pl.BlockSpec(memory_space=pltpu.HBM),
        scratch_shapes=[
            VMEM((token_len, passage_local, feature), jnp.bfloat16),
            VMEM(powers.shape, jnp.bfloat16),
            VMEM(((passage_local + 1) * pitch, feature), jnp.float32),
            VMEM((tiles, lanes, feature), jnp.bfloat16),
            pltpu.SemaphoreType.DMA((chunks,)),
            pltpu.SemaphoreType.DMA((PIECES,)),
        ],
        name="passage_grad",
        compiler_params=params,
        cost_estimate=pl.CostEstimate(
            flops=2 * limit * padded * lanes * feature,
            bytes_accessed=2 * limit * padded * lanes,
            transcendentals=0,
        ),
    )(arrived, multiplier, block_code, block_count, powers)
    numerators = from_replicas(numerator, replicas)

    loss = pair_sums(numerators)[0, 0] / weight_sum[0, 0]
    query_grad = jnp.sum(returned.astype(jnp.float32), axis=0)
    query_grad = query_grad.reshape(query_local, 1, query_len, feature)
    return (loss, query_grad, passage_grad.transpose(1, 0, 2)[:, None])


def solution(mesh):
    return jax.shard_map(
        on_device,
        mesh=mesh,
        in_specs=(
            P("grp", "rep", None, None),
            P("grp", "rep", None, None),
            P("grp", "rep"),
            P("grp", "rep", None),
            P("rep", None),
            P("grp", "rep", None),
            P("grp", "rep"),
        ),
        out_specs=(P(), P("grp", "rep", None, None), P("grp", "rep", None, None)),
        check_vma=False,
    )
```

```python
import functools
import math

import jax
import jax.numpy as jnp
from jax import lax
from jax.experimental import pallas as pl
from jax.experimental.pallas import tpu as pltpu
from jax.sharding import PartitionSpec as P


TEMPER = 0.05
LOG2E = math.log2(math.e)
MASKED = -1e30
KINDS = 8
HALF = 7
UNROLL = 2 * HALF
SPREAD = 5
SUMS = 4
STORE = 5
PIECES = 4
HIGHEST = lax.Precision.HIGHEST
VMEM = pltpu.VMEM
SMEM = pltpu.SMEM


def round_up(value, multiple):
    return -(-value // multiple) * multiple


def iota(shape, dim):
    return lax.broadcasted_iota(jnp.int32, shape, dim)


def three_parts(values):
    first = values.astype(jnp.bfloat16).astype(jnp.float32)
    rest = values - first
    second = rest.astype(jnp.bfloat16).astype(jnp.float32)
    third = (rest - second).astype(jnp.bfloat16).astype(jnp.float32)
    return first, second, third


def pack_kernel(passage_local, queries, cand_ids, owner_map, teacher, weights, out, aux):
    groups = out.shape[0]
    tokens = queries.shape[0]
    query_local, _, candidates = cand_ids.shape
    entries = owner_map.shape[1]
    table = owner_map[...].astype(jnp.float32)
    owner = jnp.floor((table + 0.5) * (1.0 / passage_local))
    local = table - owner * passage_local
    which = iota((8, entries), 0)
    tables = jnp.where(which == 0, owner, jnp.where(which == 1, local, 0.0)).astype(jnp.bfloat16)
    aux[...] = jnp.zeros_like(aux)
    for q in range(query_local):
        hot = (iota((entries, candidates), 0) == cand_ids[q]).astype(jnp.bfloat16)
        found = jnp.dot(tables, hot, preferred_element_type=jnp.float32)
        scores = teacher[q]
        shifted = scores - jnp.max(scores, axis=1, keepdims=True)
        log_teacher = shifted - jnp.log(jnp.sum(jnp.exp(shifted), axis=1, keepdims=True))
        weight = jnp.broadcast_to(weights[:, q : q + 1], (1, candidates))
        rows = (found[0:1], found[1:2], *three_parts(log_teacher), *three_parts(weight))
        for kind, row in enumerate(rows):
            at = kind * query_local + q
            aux[at : at + 1, 0:candidates] = row
    packed = aux[...].astype(jnp.bfloat16)
    for g in range(groups):
        out[g, 0:tokens, :] = queries[...]
        out[g, tokens:, :] = packed


def owned_rows(arrived, tokens, query_local, candidates, g, q, me):
    at = tokens + q
    owner = arrived[g, at : at + 1, 0:candidates].astype(jnp.float32)
    at = tokens + query_local + q
    local = arrived[g, at : at + 1, 0:candidates].astype(jnp.float32)
    return jnp.where(owner == me.astype(jnp.float32), local, -1.0).astype(jnp.int32)


def prepare_kernel(stored_hbm, rows_hbm, stored, gathered, rows, stored_done, rows_done):
    token_len, chunk, feature = stored.shape
    padded = rows.shape[1]
    pitch = gathered.shape[0] // chunk
    pieces = stored_done.shape[0]
    piece = token_len // pieces
    spans = [(k * piece, token_len if k == pieces - 1 else (k + 1) * piece) for k in range(pieces)]
    copies = []
    for k, (first, last) in enumerate(spans):
        at = pl.ds(first, last - first)
        copies.append(pltpu.make_async_copy(stored_hbm.at[at], stored.at[at], stored_done.at[k]))
        copies[-1].start()

    def clear(p, carry):
        at = pl.ds(p * pitch + token_len, padded - token_len)
        gathered[at, :] = jnp.zeros((padded - token_len, feature), jnp.float32)
        return carry

    lax.fori_loop(0, chunk, clear, 0)
    for copy, (first, last) in zip(copies, spans):
        copy.wait()

        def spread(j, carry, first=first):
            for u in range(SPREAD):
                at = first + j * SPREAD + u
                gathered[pl.ds(at, chunk, stride=pitch), :] = stored[at].astype(jnp.float32)
            return carry

        whole = (last - first) // SPREAD
        lax.fori_loop(0, whole, spread, 0)
        for at in range(first + whole * SPREAD, last):
            gathered[pl.ds(at, chunk, stride=pitch), :] = stored[at].astype(jnp.float32)

    parts = rows_done.shape[0]
    part = chunk // parts
    ahead = math.gcd(part, 4)
    copies = []
    for k in range(parts):

        def collect(step, carry, first=k * part):
            for inner in range(ahead):
                p = first + step * ahead + inner
                rows[p] = gathered[pl.ds(p * pitch, padded), :].astype(jnp.bfloat16)
            return carry

        lax.fori_loop(0, part // ahead, collect, 0)
        at = pl.ds(k * part, part)
        copies.append(pltpu.make_async_copy(rows.at[at], rows_hbm.at[at], rows_done.at[k]))
        copies[-1].start()
    for copy in copies:
        copy.wait()


def list_blocks(flags_scalar, block_code, block_count, passage_count, tiles):
    base = code_base(tiles)
    ahead = math.gcd(passage_count, 4)

    def list_passages(step, count):
        for inner in range(ahead):
            p = step * ahead + inner
            for tile in range(tiles):
                block_code[0, count] = p * base + tile
                count = count + flags_scalar[p, tile]
        return count

    count = lax.fori_loop(0, passage_count // ahead, list_passages, jnp.int32(0))
    for extra in range(3 * UNROLL):
        block_code[0, count + extra] = passage_count * base
    steps = (count + 2 * UNROLL - 1) // (2 * UNROLL)
    block_count[0, 0] = steps
    return steps


def code_base(tiles):
    return 1 << (tiles - 1).bit_length()


def decode(block_code, block, tiles):
    code = block_code[0, block]
    base = code_base(tiles)
    return code >> (base.bit_length() - 1), code & (base - 1)


def score_kernel(
    dims,
    axis,
    arrived,
    lengths,
    *refs,
):
    tokens, query_local, candidates, per_tile, replicas = dims
    weights, refs = refs[:replicas], refs[replicas:]
    passages_hbm, scores_out, summed, block_code, block_count, powers_hbm, *scratch = refs
    score_body(
        (tokens, query_local, candidates, per_tile),
        lax.axis_index(axis),
        arrived,
        lengths,
        pair_sums([one[...] for one in weights]),
        passages_hbm,
        scores_out,
        summed,
        block_code,
        block_count,
        powers_hbm,
        *scratch,
    )


def score_body(
    dims,
    me,
    arrived,
    lengths,
    weights,
    passages_hbm,
    scores_out,
    summed,
    block_code,
    block_count,
    powers_hbm,
    highest,
    passages,
    turned,
    flags,
    flags_scalar,
    penalty,
    even,
    odd,
    even_top,
    odd_top,
    powers,
    flags_done,
    rows_done,
    powers_done,
):
    tokens, query_local, candidates, per_tile = dims
    groups = arrived.shape[0]
    passage_count, padded, _ = passages.shape
    tiles, _, lanes = highest.shape
    groups_per_tile = per_tile // query_local
    fetch_rows = pltpu.make_async_copy(passages_hbm, passages, rows_done)
    fetch_rows.start()

    column = iota(flags.shape, 1)
    passage_index = iota((passage_count, candidates), 0)
    marks = jnp.zeros(flags.shape, jnp.int32)
    for tile in range(tiles):
        hit = jnp.zeros((passage_count, candidates), jnp.int32)
        for g in range(tile * groups_per_tile, (tile + 1) * groups_per_tile):
            for q in range(query_local):
                mine = owned_rows(arrived, tokens, query_local, candidates, g, q, me)
                hit = jnp.where(passage_index == mine, 1, hit)
        any_hit = jnp.max(hit, axis=1, keepdims=True)
        marks = jnp.where(column == tile, any_hit, marks)
    flags[...] = marks
    to_scalar = pltpu.make_async_copy(flags, flags_scalar, flags_done)
    to_scalar.start()

    for tile in range(tiles):
        parts = [
            arrived[g, 0:tokens, :]
            for g in range(tile * groups_per_tile, (tile + 1) * groups_per_tile)
        ]
        block = jnp.concatenate(parts, axis=0).astype(jnp.float32)
        turned[tile] = block.T.astype(jnp.bfloat16)
    highest[...] = jnp.zeros_like(highest)
    summed[...] = jnp.ones_like(summed)
    penalty[...] = jnp.where(iota(penalty.shape, 0) < padded, 0.0, MASKED)
    to_scalar.wait()
    steps = (UNROLL // HALF) * list_blocks(flags_scalar, block_code, block_count, passage_count, tiles)
    fetch_rows.wait()

    factor = LOG2E / TEMPER

    def multiply(first, into, tops):
        for u in range(HALF):
            slot, tile = decode(block_code, first + u, tiles)
            p = jnp.minimum(slot, passage_count - 1)
            products = jnp.dot(passages[p], turned[tile], preferred_element_type=jnp.float32)
            products = products + penalty[pl.ds(padded - lengths[0, p], padded), :]
            into[u] = products
            tops[u : u + 1, :] = jnp.max(products, axis=0, keepdims=True)

    def soften(first, held, tops):
        for u in range(HALF):
            slot, tile = decode(block_code, first + u, tiles)
            top = tops[u : u + 1, :]
            raised = jnp.exp2((held[u] - top) * factor)
            powers[first + u] = raised.astype(jnp.bfloat16)
            highest[tile, pl.ds(slot, 1), :] = top
            summed[tile, pl.ds(slot, 1), :] = jnp.sum(raised, axis=0, keepdims=True)

    def chunk_copy(s):
        at = pl.ds(s * 2 * HALF, 2 * HALF)
        return pltpu.make_async_copy(powers.at[at], powers_hbm.at[at], powers_done.at[s])

    multiply(0, even, even_top)

    def step(s, carry):
        first = s * 2 * HALF
        multiply(first + HALF, odd, odd_top)
        soften(first, even, even_top)
        multiply(first + 2 * HALF, even, even_top)
        soften(first + HALF, odd, odd_top)
        chunk_copy(s).start()
        return carry

    lax.fori_loop(0, steps, step, 0)

    query_len = lanes // per_tile
    member = iota((lanes, 128), 0) // query_len == iota((lanes, 128), 1)
    member = member.astype(jnp.float32)
    weight_part = jnp.sum(weights, axis=1, keepdims=True)
    scores_out[0] = jnp.broadcast_to(weight_part, scores_out.shape[1:])
    for tile in range(tiles):
        matched = highest[tile, 0:passage_count, :] + TEMPER * jnp.log(
            summed[tile, 0:passage_count, :]
        )
        sums = jnp.dot(matched, member, precision=HIGHEST, preferred_element_type=jnp.float32)
        for inner in range(per_tile):
            g = tile * groups_per_tile + inner // query_local
            q = inner % query_local
            mine = owned_rows(arrived, tokens, query_local, candidates, g, q, me)
            picked = jnp.where(passage_index == mine, sums[:, inner : inner + 1], 0.0)
            at = tile * per_tile + inner
            scores_out[0, at : at + 1, 0:candidates] = jnp.sum(picked, axis=0, keepdims=True)
    for g in range(1, groups):
        scores_out[g] = scores_out[0]

    def finish(s, carry):
        chunk_copy(s).wait()
        return carry

    lax.fori_loop(0, steps, finish, 0)


def pair_sums(values):
    while len(values) > 1:
        values = [values[i] + values[i + 1] for i in range(0, len(values), 2)]
    return values[0]


def query_kernel(
    dims,
    axis,
    arrived,
    scores,
    summed,
    block_code,
    block_count,
    passages_hbm,
    powers_hbm,
    grads_out,
    multiplier,
    numerator_out,
    weight_sum_out,
    passages,
    powers,
    factors,
    rows_done,
    powers_done,
    *sums,
):
    tokens, query_local, candidates, per_tile, query_total = dims
    groups = arrived.shape[0]
    tiles, slots, lanes = summed.shape
    passage_count = passages.shape[0]
    groups_per_tile = per_tile // query_local
    queries_all = tiles * per_tile
    query_len = lanes // per_tile
    me = lax.axis_index(axis)
    steps = block_count[0, 0]
    fetch_rows = pltpu.make_async_copy(passages_hbm, passages, rows_done)
    fetch_rows.start()

    def chunk_copy(s):
        at = pl.ds(s * 2 * UNROLL, 2 * UNROLL)
        return pltpu.make_async_copy(powers_hbm.at[at], powers.at[at], powers_done.at[s])

    def fetch(s, carry):
        chunk_copy(s).start()
        return carry

    lax.fori_loop(0, steps, fetch, 0)

    got = scores[0]
    for g in range(1, groups):
        got = got + scores[g]
    student = got[0:queries_all, 0:candidates]

    def gather_parts(kind):
        rows = []
        for g in range(groups):
            parts = []
            for part in range(3):
                at = tokens + (kind + part) * query_local
                block = arrived[g, at : at + query_local, 0:candidates]
                parts.append(block.astype(jnp.float32))
            rows.append((parts[0] + parts[1]) + parts[2])
        return jnp.concatenate(rows, axis=0)

    log_teacher = gather_parts(2)
    weight = gather_parts(5)
    shifted = student - jnp.max(student, axis=1, keepdims=True)
    log_student = shifted - jnp.log(jnp.sum(jnp.exp(shifted), axis=1, keepdims=True))
    teacher_prob = jnp.exp(log_teacher)
    spread = jnp.sum(weight * teacher_prob * (log_teacher - log_student), axis=1, keepdims=True)
    numerator = jnp.sum(spread, axis=0, keepdims=True)
    numerator_out[...] = jnp.broadcast_to(numerator, numerator_out.shape)
    weight_sum = got[0:1, candidates : candidates + 1]
    weight_sum_out[...] = jnp.broadcast_to(weight_sum, weight_sum_out.shape)
    scale = query_total / weight_sum
    grad = (weight * scale) * (jnp.exp(log_student) - teacher_prob)

    passage_index = iota((passage_count, candidates), 0)
    lane_query = iota((passage_count, lanes), 1) // query_len
    for tile in range(tiles):
        spread_out = jnp.zeros((passage_count, lanes), jnp.float32)
        for inner in range(per_tile):
            g = tile * groups_per_tile + inner // query_local
            q = inner % query_local
            mine = owned_rows(arrived, tokens, query_local, candidates, g, q, me)
            at = tile * per_tile + inner
            picked = jnp.where(passage_index == mine, grad[at : at + 1], 0.0)
            total = jnp.sum(picked, axis=1, keepdims=True)
            spread_out = jnp.where(lane_query == inner, total, spread_out)
        factors[tile, 0:passage_count, :] = spread_out / summed[tile, 0:passage_count, :]
        factors[tile, passage_count:, :] = jnp.zeros((slots - passage_count, lanes), jnp.float32)
    multiplier[...] = factors[...]

    for one in sums:
        one[...] = jnp.zeros_like(one)

    fetch_rows.wait()

    def step(s, carry):
        chunk_copy(s).wait()
        for u in range(2 * UNROLL):
            b = s * 2 * UNROLL + u
            slot, tile = decode(block_code, b, tiles)
            p = jnp.minimum(slot, passage_count - 1)
            part = powers[b].astype(jnp.float32) * factors[tile, pl.ds(slot, 1), :]
            part = part.astype(jnp.bfloat16)
            sums[u % len(sums)][tile] += lax.dot_general(
                passages[p], part, (((0,), (0,)), ((), ())), preferred_element_type=jnp.float32
            )
        return carry

    lax.fori_loop(0, steps, step, 0)
    for tile in range(tiles):
        back = pair_sums([one[tile] for one in sums]).T.astype(jnp.bfloat16)
        for inner in range(groups_per_tile):
            g = tile * groups_per_tile + inner
            grads_out[g] = back[inner * tokens : (inner + 1) * tokens]


def passage_kernel(
    dims,
    arrived,
    multiplier,
    block_code,
    block_count,
    powers_hbm,
    out_hbm,
    out,
    powers,
    sums,
    queries_all,
    powers_done,
    out_done,
):
    tokens, per_tile_groups = dims
    token_len, passage_count, feature = out.shape
    tiles = queries_all.shape[0]
    padded = powers.shape[1]
    pitch = sums.shape[0] // (passage_count + 1)
    steps = block_count[0, 0]

    def chunk_copy(s):
        at = pl.ds(s * 2 * UNROLL, 2 * UNROLL)
        return pltpu.make_async_copy(powers_hbm.at[at], powers.at[at], powers_done.at[s])

    def fetch(s, carry):
        chunk_copy(s).start()
        return carry

    lax.fori_loop(0, steps, fetch, 0)
    for tile in range(tiles):
        for inner in range(per_tile_groups):
            g = tile * per_tile_groups + inner
            queries_all[tile, inner * tokens : (inner + 1) * tokens, :] = arrived[g, 0:tokens, :]

    def clear(p, carry):
        sums[pl.ds(p * pitch, pitch), :] = jnp.zeros((pitch, feature), jnp.float32)
        return carry

    lax.fori_loop(0, passage_count, clear, 0)

    def step(s, carry):
        chunk_copy(s).wait()
        for u in range(2 * UNROLL):
            b = s * 2 * UNROLL + u
            slot, tile = decode(block_code, b, tiles)
            part = powers[b].astype(jnp.float32) * multiplier[tile, pl.ds(slot, 1), :]
            at = pl.ds(slot * pitch, padded)
            sums[at, :] += jnp.dot(
                part.astype(jnp.bfloat16), queries_all[tile], preferred_element_type=jnp.float32
            )
        return carry

    lax.fori_loop(0, steps, step, 0)

    pieces = out_done.shape[0]
    piece = token_len // pieces
    copies = []
    for k in range(pieces):
        first = k * piece
        last = token_len if k == pieces - 1 else first + piece

        def store(j, carry, first=first):
            for u in range(STORE):
                at = first + j * STORE + u
                out[at] = sums[pl.ds(at, passage_count, stride=pitch), :].astype(out.dtype)
            return carry

        whole = (last - first) // STORE
        lax.fori_loop(0, whole, store, 0)
        for at in range(first + whole * STORE, last):
            out[at] = sums[pl.ds(at, passage_count, stride=pitch), :].astype(out.dtype)
        rows = pl.ds(first, last - first)
        copies.append(pltpu.make_async_copy(out.at[rows], out_hbm.at[rows], out_done.at[k]))
        copies[-1].start()
    for copy in copies:
        copy.wait()


def vmem(count):
    return [pl.BlockSpec(memory_space=VMEM)] * count


def smem(count):
    return [pl.BlockSpec(memory_space=SMEM)] * count


def from_replicas(values, replicas):
    rings = [[(r, r ^ hop) for r in range(replicas)] for hop in range(1, replicas)]
    return [values] + [lax.ppermute(values, "rep", ring) for ring in rings]


def hbm(count):
    return [pl.BlockSpec(memory_space=pltpu.HBM)] * count


def on_device(queries, passages, lengths, cand_ids, owner_map, teacher, weights):
    groups = lax.axis_size("grp")
    replicas = lax.axis_size("rep")
    query_local, _, query_len, feature = queries.shape
    passage_local, _, token_len, _ = passages.shape
    candidates = cand_ids.shape[2]
    tokens = query_local * query_len
    lanes = 128
    per_tile = lanes // query_len
    tiles = groups * tokens // lanes
    padded = round_up(token_len, 16)
    pitch = padded + 9
    ref_count = query_local * candidates
    capacity = groups * (2 * ref_count // groups)
    limit = min(passage_local * tiles, capacity)
    blocks = limit + 3 * UNROLL
    chunks = -(-limit // (2 * UNROLL))
    aux_rows = round_up(KINDS * query_local, 16)
    slots = round_up(passage_local + 1, 8)
    score_rows = round_up(groups * query_local, 8)
    shape = jax.ShapeDtypeStruct
    alone = pltpu.CompilerParams(vmem_limit_bytes=62 * 2**20)
    params = pltpu.CompilerParams(vmem_limit_bytes=52 * 2**20)

    share = pl.pallas_call(
        functools.partial(pack_kernel, passage_local),
        out_shape=shape((groups, tokens + aux_rows, feature), jnp.bfloat16),
        in_specs=vmem(5),
        out_specs=pl.BlockSpec(memory_space=VMEM),
        scratch_shapes=[VMEM((aux_rows, feature), jnp.float32)],
        name="pack",
        compiler_params=alone,
    )(queries.reshape(tokens, feature), cand_ids, owner_map, teacher, weights.T)
    arrived = lax.all_to_all(share, "grp", split_axis=0, concat_axis=0, tiled=True)

    replica_weights = from_replicas(weights.T, replicas)

    rows = pl.pallas_call(
        prepare_kernel,
        out_shape=shape((passage_local, padded, feature), jnp.bfloat16),
        in_specs=hbm(1),
        out_specs=pl.BlockSpec(memory_space=pltpu.HBM),
        scratch_shapes=[
            VMEM((token_len, passage_local, feature), jnp.bfloat16),
            VMEM((passage_local * pitch, feature), jnp.float32),
            VMEM((passage_local, padded, feature), jnp.bfloat16),
            pltpu.SemaphoreType.DMA((PIECES,)),
            pltpu.SemaphoreType.DMA((math.gcd(passage_local, PIECES),)),
        ],
        name="prepare",
        compiler_params=params,
    )(passages[:, 0].transpose(1, 0, 2))

    dims = (tokens, query_local, candidates, per_tile)
    scores, summed, block_code, block_count, powers = (
        pl.pallas_call(
            functools.partial(score_kernel, dims + (replicas,), "grp"),
            out_shape=(
                shape((groups, score_rows, 128), jnp.float32),
                shape((tiles, slots, lanes), jnp.float32),
                shape((1, blocks), jnp.int32),
                shape((1, 1), jnp.int32),
                shape((chunks * 2 * UNROLL, padded, lanes), jnp.bfloat16),
            ),
            in_specs=vmem(1) + smem(1) + vmem(replicas) + hbm(1),
            out_specs=tuple(vmem(2) + smem(2) + hbm(1)),
            scratch_shapes=[
                VMEM((tiles, slots, lanes), jnp.float32),
                VMEM((passage_local, padded, feature), jnp.bfloat16),
                VMEM((tiles, feature, lanes), jnp.bfloat16),
                VMEM((passage_local, 128), jnp.int32),
                SMEM((passage_local, 128), jnp.int32),
                VMEM((2 * padded, lanes), jnp.float32),
                VMEM((HALF, padded, lanes), jnp.float32),
                VMEM((HALF, padded, lanes), jnp.float32),
                VMEM((HALF, lanes), jnp.float32),
                VMEM((HALF, lanes), jnp.float32),
                VMEM((chunks * 2 * UNROLL, padded, lanes), jnp.bfloat16),
                pltpu.SemaphoreType.DMA,
                pltpu.SemaphoreType.DMA,
                pltpu.SemaphoreType.DMA((chunks * UNROLL // HALF,)),
            ],
            name="score",
            compiler_params=params,
        )(arrived, lengths.T, *replica_weights, rows)
    )
    all_scores = lax.all_to_all(scores, "grp", split_axis=0, concat_axis=0, tiled=True)

    query_total = query_local * groups * replicas
    grads, multiplier, numerator, weight_sum = pl.pallas_call(
        functools.partial(query_kernel, dims + (query_total,), "grp"),
        out_shape=(
            shape((groups, tokens, feature), jnp.bfloat16),
            shape((tiles, slots, lanes), jnp.float32),
            shape((1, 128), jnp.float32),
            shape((1, 128), jnp.float32),
        ),
        in_specs=vmem(3) + smem(2) + hbm(2),
        out_specs=tuple(vmem(4)),
        scratch_shapes=[
            VMEM(rows.shape, jnp.bfloat16),
            VMEM(powers.shape, jnp.bfloat16),
            VMEM((tiles, slots, lanes), jnp.float32),
            pltpu.SemaphoreType.DMA,
            pltpu.SemaphoreType.DMA((chunks,)),
        ]
        + [VMEM((tiles, feature, lanes), jnp.float32)] * SUMS,
        name="query_grad",
        compiler_params=params,
    )(arrived, all_scores, summed, block_code, block_count, rows, powers)
    returned = lax.all_to_all(grads, "grp", split_axis=0, concat_axis=0, tiled=True)

    passage_grad = pl.pallas_call(
        functools.partial(passage_kernel, (tokens, per_tile // query_local)),
        out_shape=shape((token_len, passage_local, feature), jnp.bfloat16),
        in_specs=vmem(2) + smem(2) + hbm(1),
        out_specs=pl.BlockSpec(memory_space=pltpu.HBM),
        scratch_shapes=[
            VMEM((token_len, passage_local, feature), jnp.bfloat16),
            VMEM(powers.shape, jnp.bfloat16),
            VMEM(((passage_local + 1) * pitch, feature), jnp.float32),
            VMEM((tiles, lanes, feature), jnp.bfloat16),
            pltpu.SemaphoreType.DMA((chunks,)),
            pltpu.SemaphoreType.DMA((PIECES,)),
        ],
        name="passage_grad",
        compiler_params=params,
        cost_estimate=pl.CostEstimate(
            flops=2 * limit * padded * lanes * feature,
            bytes_accessed=2 * limit * padded * lanes,
            transcendentals=0,
        ),
    )(arrived, multiplier, block_code, block_count, powers)
    numerators = from_replicas(numerator, replicas)

    loss = pair_sums(numerators)[0, 0] / weight_sum[0, 0]
    query_grad = jnp.sum(returned.astype(jnp.float32), axis=0)
    query_grad = query_grad.reshape(query_local, 1, query_len, feature)
    return (loss, query_grad, passage_grad.transpose(1, 0, 2)[:, None])


def solution(mesh):
    return jax.shard_map(
        on_device,
        mesh=mesh,
        in_specs=(
            P("grp", "rep", None, None),
            P("grp", "rep", None, None),
            P("grp", "rep"),
            P("grp", "rep", None),
            P("rep", None),
            P("grp", "rep", None),
            P("grp", "rep"),
        ),
        out_specs=(P(), P("grp", "rep", None, None), P("grp", "rep", None, None)),
        check_vma=False,
    )
```
